32 devices in a mesh: dp: 8 (over z, core), tensor: 4 (over y, x).
Axes of the slice: x: 2, y: 2, z: 4, core: 2. Of those that a mesh axis runs over, the one named last changes fastest.
Arguments:
- block_input: bfloat16 [16, 736, 1152], P('dp', 'tensor'), may hold values from -40 to 40
- key_mask: int32 [16, 736], P('dp'), may hold values from 0 to 1, as said below
- attn_norm_gain: float32 [1152], replicated, may hold values from 0.5 to 1.5
- attn_norm_bias: float32 [1152], replicated, may hold values from -1.5 to 1.5
- qkv_weight: bfloat16 [1152, 3, 1152], P('dp', None, 'tensor'), may hold values from -1.5 to 1.5
- qv_bias: float32 [2, 1152], P(None, 'tensor'), may hold values from -2.5 to 2.5
- out_weight: bfloat16 [1152, 1152], P('tensor', 'dp'), may hold values from -0.5 to 0.5
- out_bias: float32 [1152], replicated, may hold values from -2.5 to 2.5
- mlp_norm_gain: float32 [1152], replicated, may hold values from 0.5 to 1.5
- mlp_norm_bias: float32 [1152], replicated, may hold values from -1.5 to 1.5
- hidden_weight: bfloat16 [1152, 4304], P('dp', 'tensor'), may hold values from -0.1875 to 0.1875
- hidden_bias: float32 [4304], P('tensor'), may hold values from -2.5 to 2.5
- down_weight: bfloat16 [4304, 1152], P('tensor', 'dp'), may hold values from -0.125 to 0.125
- down_bias: float32 [1152], replicated, may hold values from -2.5 to 2.5
- grad_out: bfloat16 [16, 736, 1152], P('dp', 'tensor'), may hold values from -6 to 6
Outputs:
- block_output: bfloat16 [16, 736, 1152], P('dp', 'tensor')
- grad_input: float32 [16, 736, 1152], P('dp', 'tensor')
- grad_attn_norm_gain: float32 [1152], replicated
- grad_attn_norm_bias: float32 [1152], replicated
- grad_qkv_weight: float32 [1152, 3, 1152], P('dp', None, 'tensor')
- grad_qv_bias: float32 [2, 1152], P(None, 'tensor')
- grad_out_weight: float32 [1152, 1152], P('tensor', 'dp')
- grad_out_bias: float32 [1152], replicated
- grad_mlp_norm_gain: float32 [1152], replicated
- grad_mlp_norm_bias: float32 [1152], replicated
- grad_hidden_weight: float32 [1152, 4304], P('dp', 'tensor')
- grad_hidden_bias: float32 [4304], P('tensor')
- grad_down_weight: float32 [4304, 1152], P('tensor', 'dp')
- grad_down_bias: float32 [1152], replicated
The draws below stay inside these ranges and needn't reach their ends.
Inputs may be any that keep to these rules, and one draw needn't show every extreme that they name: `key_mask`: each image's mask is 1 on its first L positions and 0 after them, with L from 368 to 729; some image has L = 729.
All inputs are finite; a program needn't handle non-finite values.
Results may differ from the reference program's by a relative error of at most 0.0095.
The reference program's roundings to bfloat16 on the way count: a program that leaves them out, or rounds other values in their place, can miss the bound.
Values may be sent and summed in bfloat16 or wider, within the bound.
A program may use at most 192 MiB of HBM per device.

```python
import math
import jax
import jax.numpy as jnp
from jax import lax

D = 1152
HEADS = 16
FF = 4304
HD = 72
SEQ = 736
VALID = 729
IMAGES = 16


def draw_block_input(key, part):
    streams = jax.random.split(jax.random.fold_in(key, 11), 3)
    row_scale = jnp.exp(jax.random.uniform(streams[0], (IMAGES, SEQ, 1), jnp.float32, math.log(0.3), math.log(3.0)))
    col_scale = jnp.exp(jax.random.uniform(streams[1], (1, 1, D), jnp.float32, math.log(0.3), math.log(3.0)))
    noise = jax.random.truncated_normal(streams[2], -3.0, 3.0, (IMAGES, SEQ, D), jnp.float32)
    values = noise * row_scale * col_scale
    return values.astype(jnp.bfloat16)


def draw_qkv_weight(key, part):
    streams = jax.random.split(jax.random.fold_in(key, 23), 1)
    base = jax.random.truncated_normal(streams[0], -4.0, 4.0, (D, 3, D), jnp.float32) / math.sqrt(D)
    return base.astype(jnp.bfloat16)


def draw_key_mask(key, part):
    streams = jax.random.split(jax.random.fold_in(key, 37), 2)
    lengths = jax.random.randint(streams[0], (IMAGES,), SEQ // 2, VALID + 1)
    if IMAGES >= 4:
        chosen = jax.random.randint(streams[1], (), 0, IMAGES)
    else:
        chosen = jnp.array(IMAGES - 1, jnp.int32)
    index = jnp.arange(IMAGES)
    lengths = jnp.where(index == chosen, VALID, lengths)
    return (jnp.arange(SEQ)[None, :] < lengths[:, None]).astype(jnp.int32)


def steps_of(stream_key, extent, cuts, smallest, high):
    def one(axis_at, blocks):
        draws = jax.random.uniform(jax.random.fold_in(jax.random.fold_in(stream_key, 6), axis_at), (blocks,), jnp.float32, smallest / len(cuts), high / len(cuts))
        return jnp.repeat(jnp.exp(draws), extent[axis_at] // blocks).reshape((-1,) + (1,) * (len(extent) - axis_at - 1))

    level = one(*cuts[0])
    for cut in cuts[1:]:
        level = level * one(*cut)
    return level


def scatter_about(stream_key, extent, width, most, pieces=(), held_as=jnp.bfloat16):
    result = width * jax.random.normal(stream_key, extent, jnp.float32)
    if pieces:
        result = result * steps_of(stream_key, extent, pieces, -0.22, 0.18)
    return jnp.clip(result, -most, most).astype(held_as)


def setup_inputs(seed: int = 0) -> dict:
    arg_keys = jax.random.split(jax.random.key(seed), 16)
    block_input = draw_block_input(jax.random.fold_in(arg_keys[15], 71), 0)
    key_mask = draw_key_mask(jax.random.fold_in(arg_keys[15], 71), 0)
    attn_norm_gain = jnp.clip(1.0 + 0.1 * jax.random.normal(arg_keys[2], (D,), jnp.float32), 0.5, 1.5)
    attn_norm_bias = scatter_about(arg_keys[3], (D,), 0.3, 1.5, (), jnp.float32)
    qkv_weight = draw_qkv_weight(jax.random.fold_in(arg_keys[15], 71), 0)
    qv_bias = scatter_about(arg_keys[5], (2, D), 0.5, 2.5, ((1, 4),), jnp.float32)
    out_weight = scatter_about(arg_keys[6], (D, D), (D // 8) ** -0.5, 0.5, ((0, 4), (1, 8)))
    out_bias = scatter_about(arg_keys[7], (D,), 0.5, 2.5, (), jnp.float32)
    mlp_norm_gain = jnp.clip(1.0 + 0.1 * jax.random.normal(arg_keys[8], (D,), jnp.float32), 0.5, 1.5)
    mlp_norm_bias = scatter_about(arg_keys[9], (D,), 0.3, 1.5, (), jnp.float32)
    hidden_weight = scatter_about(arg_keys[10], (D, FF), D ** -0.5, 0.1875, ((0, 8), (1, 4)))
    hidden_bias = scatter_about(arg_keys[11], (FF,), 0.5, 2.5, ((0, 4),), jnp.float32)
    down_weight = scatter_about(arg_keys[12], (FF, D), (FF // 2) ** -0.5, 0.125, ((0, 4), (1, 8)))
    down_bias = scatter_about(arg_keys[13], (D,), 0.5, 2.5, (), jnp.float32)
    grad_out = scatter_about(arg_keys[14], (IMAGES, SEQ, D), 1.0, 6.0, ((0, 8), (1, 4)))
    return dict(block_input=block_input, key_mask=key_mask, attn_norm_gain=attn_norm_gain, attn_norm_bias=attn_norm_bias, qkv_weight=qkv_weight, qv_bias=qv_bias, out_weight=out_weight, out_bias=out_bias, mlp_norm_gain=mlp_norm_gain, mlp_norm_bias=mlp_norm_bias, hidden_weight=hidden_weight, hidden_bias=hidden_bias, down_weight=down_weight, down_bias=down_bias, grad_out=grad_out)


layer_eps = 1e-06
gelu_root = math.sqrt(2.0 / math.pi)
gelu_cubic = 0.044715

def norm_forward(rows, gain, shift):
    center = rows - lax.optimization_barrier(jnp.mean(rows, axis=-1, keepdims=True))
    inv_std = lax.rsqrt(lax.optimization_barrier(jnp.mean(center * center, axis=-1, keepdims=True)) + layer_eps)
    unit = center * inv_std
    return ((unit * gain + shift).astype(jnp.bfloat16), unit, inv_std)

def norm_backward(grad_normed, unit, inv_std, gain):
    scaled = grad_normed * gain
    return inv_std * (scaled - lax.optimization_barrier(jnp.mean(scaled, axis=-1, keepdims=True)) - unit * lax.optimization_barrier(jnp.mean(scaled * unit, axis=-1, keepdims=True)))

def gelu_forward(pre):
    inner = gelu_root * (pre + gelu_cubic * pre * pre * pre)
    return 0.5 * pre * (1.0 + jnp.tanh(inner))

def gelu_slope(pre):
    tangent = jnp.tanh(gelu_root * (pre + gelu_cubic * pre * pre * pre))
    return 0.5 * (1.0 + tangent) + 0.5 * pre * (1.0 - tangent * tangent) * gelu_root * (1.0 + 3.0 * gelu_cubic * pre * pre)

def score_block(queries, keys_in, valid):
    scale = HD ** (-0.5)
    scores = jnp.einsum('qhd,khd->hqk', queries.astype(jnp.float32), keys_in.astype(jnp.float32)) * scale
    return jnp.where(valid[None, None, :] > 0, scores, -1e+30)

def attend_forward(queries, keys_in, values, valid):
    scores = score_block(queries, keys_in, valid)
    top = lax.optimization_barrier(jnp.max(scores, axis=-1, keepdims=True))
    log_total = top + jnp.log(lax.optimization_barrier(jnp.sum(jnp.exp(scores - top), axis=-1, keepdims=True)))
    weights = jnp.exp(scores - log_total).astype(jnp.bfloat16)
    mixed = jnp.einsum('hqk,khd->qhd', weights.astype(jnp.float32), values.astype(jnp.float32)).astype(jnp.bfloat16)
    return (mixed, log_total)

def attend_backward(queries, keys_in, values, grad_mixed, log_total, valid):
    scale = HD ** (-0.5)
    probs = jnp.exp(score_block(queries, keys_in, valid) - log_total)
    weights = probs.astype(jnp.bfloat16)
    grad_probs = jnp.einsum('qhd,khd->hqk', grad_mixed.astype(jnp.float32), values.astype(jnp.float32))
    delta = lax.optimization_barrier(jnp.sum(probs * grad_probs, axis=-1, keepdims=True))
    grad_scores = (probs * (grad_probs - delta) * scale).astype(jnp.bfloat16).astype(jnp.float32)
    grad_queries = jnp.einsum('hqk,khd->qhd', grad_scores, keys_in.astype(jnp.float32))
    grad_keys = jnp.einsum('hqk,qhd->khd', grad_scores, queries.astype(jnp.float32))
    grad_values = jnp.einsum('hqk,qhd->khd', weights.astype(jnp.float32), grad_mixed.astype(jnp.float32))
    return (grad_queries, grad_keys, grad_values)

def reference(block_input, key_mask, attn_norm_gain, attn_norm_bias, qkv_weight, qv_bias, out_weight, out_bias, mlp_norm_gain, mlp_norm_bias, hidden_weight, hidden_bias, down_weight, down_bias, grad_out):
    qkv_flat = qkv_weight.reshape(D, 3 * D)

    def image_step(carry, item):
        image_in, valid, image_grad = item
        in_float = image_in.astype(jnp.float32)
        normed_one, unit_one, inv_one = norm_forward(in_float, attn_norm_gain, attn_norm_bias)
        projected = jnp.dot(normed_one, qkv_flat, preferred_element_type=jnp.float32).reshape(SEQ, 3, D)
        queries = (projected[:, 0] + qv_bias[0]).astype(jnp.bfloat16).reshape(SEQ, HEADS, HD)
        keys_in = projected[:, 1].astype(jnp.bfloat16).reshape(SEQ, HEADS, HD)
        values = (projected[:, 2] + qv_bias[1]).astype(jnp.bfloat16).reshape(SEQ, HEADS, HD)
        mixed, log_total = attend_forward(queries, keys_in, values, valid)
        mixed_flat = mixed.reshape(SEQ, D)
        hidden_res = in_float + jnp.dot(mixed_flat, out_weight, preferred_element_type=jnp.float32) + out_bias
        normed_two, unit_two, inv_two = norm_forward(hidden_res, mlp_norm_gain, mlp_norm_bias)
        pre_act = jnp.dot(normed_two, hidden_weight, preferred_element_type=jnp.float32) + hidden_bias
        activated = gelu_forward(pre_act).astype(jnp.bfloat16)
        image_out = (hidden_res + jnp.dot(activated, down_weight, preferred_element_type=jnp.float32) + down_bias).astype(jnp.bfloat16)
        grad_float = image_grad.astype(jnp.float32)
        grad_down_w = jnp.dot(activated.T, image_grad, preferred_element_type=jnp.float32)
        grad_down_b = lax.optimization_barrier(jnp.sum(grad_float, axis=0))
        grad_pre = jnp.dot(image_grad, down_weight.T, preferred_element_type=jnp.float32) * gelu_slope(pre_act)
        grad_hidden_b = lax.optimization_barrier(jnp.sum(grad_pre, axis=0))
        grad_pre_low = grad_pre.astype(jnp.bfloat16)
        grad_hidden_w = jnp.dot(normed_two.T, grad_pre_low, preferred_element_type=jnp.float32)
        grad_normed_two = jnp.dot(grad_pre_low, hidden_weight.T, preferred_element_type=jnp.float32)
        grad_mlp_gain = lax.optimization_barrier(jnp.sum(grad_normed_two * unit_two, axis=0))
        grad_mlp_shift = lax.optimization_barrier(jnp.sum(grad_normed_two, axis=0))
        grad_hidden = grad_float + norm_backward(grad_normed_two, unit_two, inv_two, mlp_norm_gain)
        grad_out_b = lax.optimization_barrier(jnp.sum(grad_hidden, axis=0))
        grad_hidden_low = grad_hidden.astype(jnp.bfloat16)
        grad_out_w = jnp.dot(mixed_flat.T, grad_hidden_low, preferred_element_type=jnp.float32)
        grad_mixed = jnp.dot(grad_hidden_low, out_weight.T, preferred_element_type=jnp.float32).astype(jnp.bfloat16).reshape(SEQ, HEADS, HD)
        grad_queries, grad_keys, grad_values = attend_backward(queries, keys_in, values, grad_mixed, log_total, valid)
        grad_queries = grad_queries.reshape(SEQ, D)
        grad_keys = grad_keys.reshape(SEQ, D)
        grad_values = grad_values.reshape(SEQ, D)
        grad_qv_b = jnp.stack([lax.optimization_barrier(jnp.sum(grad_queries, axis=0)), lax.optimization_barrier(jnp.sum(grad_values, axis=0))])
        grad_projected = jnp.stack([grad_queries, grad_keys, grad_values], axis=1).astype(jnp.bfloat16).reshape(SEQ, 3 * D)
        grad_qkv_w = jnp.dot(normed_one.T, grad_projected, preferred_element_type=jnp.float32).reshape(D, 3, D)
        grad_normed_one = jnp.dot(grad_projected, qkv_flat.T, preferred_element_type=jnp.float32)
        grad_attn_gain = lax.optimization_barrier(jnp.sum(grad_normed_one * unit_one, axis=0))
        grad_attn_shift = lax.optimization_barrier(jnp.sum(grad_normed_one, axis=0))
        image_grad_in = grad_hidden + norm_backward(grad_normed_one, unit_one, inv_one, attn_norm_gain)
        terms = (grad_attn_gain, grad_attn_shift, grad_qkv_w, grad_qv_b, grad_out_w, grad_out_b, grad_mlp_gain, grad_mlp_shift, grad_hidden_w, grad_hidden_b, grad_down_w, grad_down_b)
        carry = jax.tree.map(lambda total, term: total + term, carry, terms)
        return (carry, (image_out, image_grad_in))
    start = (jnp.zeros((D,), jnp.float32), jnp.zeros((D,), jnp.float32), jnp.zeros((D, 3, D), jnp.float32), jnp.zeros((2, D), jnp.float32), jnp.zeros((D, D), jnp.float32), jnp.zeros((D,), jnp.float32), jnp.zeros((D,), jnp.float32), jnp.zeros((D,), jnp.float32), jnp.zeros((D, FF), jnp.float32), jnp.zeros((FF,), jnp.float32), jnp.zeros((FF, D), jnp.float32), jnp.zeros((D,), jnp.float32))
    totals, (block_output, grad_input) = lax.scan(image_step, start, (block_input, key_mask, grad_out))
    return (block_output, grad_input, totals[0], totals[1], totals[2], totals[3], totals[4], totals[5], totals[6], totals[7], totals[8], totals[9], totals[10], totals[11])
```

```python
import functools
import math

import jax
import jax.numpy as jnp
from jax import lax
from jax.experimental import pallas as pl
from jax.experimental.pallas import tpu as pltpu
from jax.sharding import PartitionSpec as P

HD = 72
CHUNK = 768
F32 = jnp.float32
BF16 = jnp.bfloat16
LOG2E = math.log2(math.e)
NN = (((1,), (0,)), ((), ()))
NT = (((1,), (1,)), ((), ()))
MESH = pl.DeviceIdType.MESH
ANY = pl.BlockSpec(memory_space=pl.ANY)
VMEM = pl.BlockSpec(memory_space=pltpu.VMEM)
SMEM = pl.BlockSpec(memory_space=pltpu.SMEM)


layer_eps = 1e-06
gelu_root = math.sqrt(2.0 / math.pi)
gelu_cubic = 0.044715


def norm_stats(rows):
    center = rows - jnp.mean(rows, axis=-1, keepdims=True)
    inv_std = lax.rsqrt(jnp.mean(center * center, axis=-1, keepdims=True) + layer_eps)
    return (center * inv_std, inv_std)


def norm_forward(rows, gain, shift):
    unit, _ = norm_stats(rows)
    return (unit * gain + shift).astype(BF16)


def norm_backward(grad_normed, unit, inv_std, gain):
    scaled = grad_normed * gain
    return inv_std * (
        scaled
        - jnp.mean(scaled, axis=-1, keepdims=True)
        - unit * jnp.mean(scaled * unit, axis=-1, keepdims=True)
    )


def gelu_both(pre):
    tangent = jnp.tanh(gelu_root * (pre + gelu_cubic * pre * pre * pre))
    value = 0.5 * pre * (1.0 + tangent)
    slope = 0.5 * (1.0 + tangent) + 0.5 * pre * (1.0 - tangent * tangent) * gelu_root * (
        1.0 + 3.0 * gelu_cubic * pre * pre
    )
    return (value, slope)


def dot(a, b, dims=NN):
    return lax.dot_general(a, b, dims, preferred_element_type=F32)


def soft_columns(keys_in, queries, row_ok, factor):
    raw = jnp.where(row_ok, dot(keys_in, queries, NT), -1e30)
    top = jnp.max(raw, axis=0, keepdims=True)
    grown = jnp.exp2((raw - top) * factor)
    total = jnp.sum(grown, axis=0, keepdims=True)
    return grown * (1.0 / total)


def attend_forward_body(seq, heads, lens_ref, proj_ref, mixed_ref, qh, kh, vh, oh):
    width = heads * HD
    padded = qh.shape[1]
    for h in range(heads):
        qh[h, :seq] = proj_ref[0, :, h * HD : (h + 1) * HD]
        qh[h, seq:] = jnp.zeros((padded - seq, HD), BF16)
        kh[h] = proj_ref[0, :, width + h * HD : width + (h + 1) * HD]
        vh[h] = proj_ref[0, :, 2 * width + h * HD : 2 * width + (h + 1) * HD].T
    length = lens_ref[pl.program_id(0)]
    factor = HD**-0.5 * LOG2E

    def head(h, _):
        def chunk(c, _):
            row_ok = lax.broadcasted_iota(jnp.int32, (seq, CHUNK), 0) < length
            at = pl.ds(pl.multiple_of(c * CHUNK, CHUNK), CHUNK)
            probs = soft_columns(kh[h], qh[h, at], row_ok, factor)
            oh[h, at] = dot(vh[h], probs.astype(BF16)).T.astype(BF16)
            return 0

        return lax.fori_loop(0, padded // CHUNK, chunk, 0)

    lax.fori_loop(0, heads, head, 0)
    for h in range(heads):
        mixed_ref[0, :, h * HD : (h + 1) * HD] = oh[h, :seq]


def attend_forward(lens, proj):
    images, seq, triple = proj.shape
    heads = triple // (3 * HD)
    padded = -(-seq // CHUNK) * CHUNK
    return pl.pallas_call(
        functools.partial(attend_forward_body, seq, heads),
        out_shape=jax.ShapeDtypeStruct((images, seq, heads * HD), BF16),
        grid=(images,),
        in_specs=[SMEM, pl.BlockSpec((1, seq, triple), lambda i: (i, 0, 0))],
        out_specs=pl.BlockSpec((1, seq, heads * HD), lambda i: (i, 0, 0)),
        scratch_shapes=[
            pltpu.VMEM((heads, padded, HD), BF16),
            pltpu.VMEM((heads, seq, HD), BF16),
            pltpu.VMEM((heads, HD, seq), BF16),
            pltpu.VMEM((heads, padded, HD), BF16),
        ],
        name="attend_forward",
    )(lens, proj)


def attend_backward_body(
    seq, heads, lens_ref, proj_ref, gmix_ref, gproj_ref, gbias_ref, qh, kh, kt, vh, gh, gq, gk, gv
):
    width = heads * HD
    padded = qh.shape[1]
    for h in range(heads):
        qh[h, :seq] = proj_ref[0, :, h * HD : (h + 1) * HD]
        qh[h, seq:] = jnp.zeros((padded - seq, HD), BF16)
        gh[h, :seq] = gmix_ref[0, :, h * HD : (h + 1) * HD]
        gh[h, seq:] = jnp.zeros((padded - seq, HD), BF16)
        keys_in = proj_ref[0, :, width + h * HD : width + (h + 1) * HD]
        kh[h] = keys_in
        kt[h] = keys_in.T
        vh[h] = proj_ref[0, :, 2 * width + h * HD : 2 * width + (h + 1) * HD]
    length = lens_ref[pl.program_id(0)]
    scale = HD**-0.5
    factor = scale * LOG2E

    def head(h, _):
        gk[h] = jnp.zeros((seq, HD), F32)
        gv[h] = jnp.zeros((seq, HD), F32)

        def chunk(c, _):
            row_ok = lax.broadcasted_iota(jnp.int32, (seq, CHUNK), 0) < length
            at = pl.ds(pl.multiple_of(c * CHUNK, CHUNK), CHUNK)
            queries = qh[h, at]
            grads = gh[h, at]
            probs = soft_columns(kh[h], queries, row_ok, factor)
            grad_probs = dot(vh[h], grads, NT)
            gv[h] += dot(probs.astype(BF16), grads)
            delta = jnp.sum(probs * grad_probs, axis=0, keepdims=True)
            grad_scores = (probs * (grad_probs - delta) * scale).astype(BF16)
            gk[h] += dot(grad_scores, queries)
            gq[h, at] = dot(kt[h], grad_scores).T
            return 0

        return lax.fori_loop(0, padded // CHUNK, chunk, 0)

    lax.fori_loop(0, heads, head, 0)
    for h in range(heads):
        for c, held in enumerate((gq, gk, gv)):
            value = held[h, :seq]
            at = slice(c * width + h * HD, c * width + (h + 1) * HD)
            gproj_ref[0, :, at] = value.astype(BF16)
            gbias_ref[0, :, at] = jnp.sum(value, axis=0, keepdims=True)


def attend_backward(lens, proj, gmix):
    images, seq, triple = proj.shape
    heads = triple // (3 * HD)
    padded = -(-seq // CHUNK) * CHUNK
    return pl.pallas_call(
        functools.partial(attend_backward_body, seq, heads),
        out_shape=(
            jax.ShapeDtypeStruct((images, seq, triple), BF16),
            jax.ShapeDtypeStruct((images, 1, triple), F32),
        ),
        grid=(images,),
        in_specs=[
            SMEM,
            pl.BlockSpec((1, seq, triple), lambda i: (i, 0, 0)),
            pl.BlockSpec((1, seq, heads * HD), lambda i: (i, 0, 0)),
        ],
        out_specs=(
            pl.BlockSpec((1, seq, triple), lambda i: (i, 0, 0)),
            pl.BlockSpec((1, 1, triple), lambda i: (i, 0, 0)),
        ),
        scratch_shapes=[
            pltpu.VMEM((heads, padded, HD), BF16),
            pltpu.VMEM((heads, seq, HD), BF16),
            pltpu.VMEM((heads, HD, seq), BF16),
            pltpu.VMEM((heads, seq, HD), BF16),
            pltpu.VMEM((heads, padded, HD), BF16),
            pltpu.VMEM((heads, padded, HD), F32),
            pltpu.VMEM((heads, seq, HD), F32),
            pltpu.VMEM((heads, seq, HD), F32),
        ],
        name="attend_backward",
    )(lens, proj, gmix)


def plane():
    me = lax.axis_index("tensor")
    side = me + 1 - 2 * lax.rem(me, 2)
    over = lax.rem(me + 2, 4)
    return (me, side, over, lax.rem(side + 2, 4))


def greet(peers):
    barrier = pltpu.get_barrier_semaphore()
    for peer in peers:
        pl.semaphore_signal(barrier, inc=1, device_id={"tensor": peer}, device_id_type=MESH)
    pl.semaphore_wait(barrier, len(peers))


def remote(src, dst, send, recv, peer):
    return pltpu.make_async_remote_copy(
        src_ref=src,
        dst_ref=dst,
        send_sem=send,
        recv_sem=recv,
        device_id={"tensor": peer},
        device_id_type=MESH,
    )


def halves_of(rows):
    first = -(-rows // 32) * 16
    return (pl.ds(0, first), pl.ds(first, rows - first))


class Gather:
    def __init__(self, all_ref, send, recv):
        self.me, self.side, self.over, _ = plane()
        self.all_ref, self.send, self.recv = all_ref, send, recv
        self.low, self.high = halves_of(all_ref.shape[1])
        self.done = []

    def copy(self, k, block, rows, peer):
        part = self.all_ref.at[block, rows]
        made = remote(part, part, self.send.at[k], self.recv.at[k], peer)
        made.start()
        self.done.append(made)
        return made

    def start(self):
        self.first = self.copy(0, self.me, self.low, self.side)
        self.second = self.copy(1, self.me, self.high, self.over)
        self.copy(2, self.me, self.high, self.side)
        self.copy(3, self.me, self.low, self.over)

    def forward(self):
        self.first.wait_recv()
        self.copy(4, self.side, self.low, self.over)
        self.second.wait_recv()
        self.copy(5, self.over, self.high, self.side)

    def finish(self):
        for made in self.done:
            if made is not self.first and made is not self.second:
                made.wait_recv()
            made.wait_send()


class Scatter:
    def __init__(self, part_ref, near_ref, far_ref, pass_ref, send, recv):
        self.me, self.side, self.over, self.cross = plane()
        self.part_ref, self.near_ref, self.far_ref, self.pass_ref = part_ref, near_ref, far_ref, pass_ref
        self.send, self.recv = send, recv
        self.halves = halves_of(part_ref.shape[1])
        self.done = []

    def copy(self, k, src, dst, peer):
        made = remote(src, dst, self.send.at[k], self.recv.at[k], peer)
        made.start()
        self.done.append(made)
        return made

    def near(self, half, slot):
        return self.near_ref.at[slot, self.halves[half]]

    def start(self):
        low, high = self.halves
        part = self.part_ref
        self.first = self.copy(0, part.at[self.cross, low], self.near(0, 1), self.side)
        self.second = self.copy(1, part.at[self.cross, high], self.near(1, 1), self.over)
        self.third = self.copy(2, part.at[self.side, low], self.near(0, 0), self.side)
        self.fourth = self.copy(3, part.at[self.over, high], self.near(1, 0), self.over)

    def forward(self):
        low, high = self.halves
        self.first.wait_recv()
        self.pass_ref[low] = (
            self.part_ref[self.over, low].astype(F32) + self.near_ref[1, low].astype(F32)
        ).astype(BF16)
        self.fifth = self.copy(4, self.pass_ref.at[low], self.far_ref.at[low], self.over)
        self.second.wait_recv()
        self.pass_ref[high] = (
            self.part_ref[self.side, high].astype(F32) + self.near_ref[1, high].astype(F32)
        ).astype(BF16)
        self.sixth = self.copy(5, self.pass_ref.at[high], self.far_ref.at[high], self.side)

    def arrive(self):
        for made in (self.third, self.fourth, self.fifth, self.sixth):
            made.wait_recv()

    def total(self, rows):
        return (
            self.part_ref[self.me, rows].astype(F32)
            + self.near_ref[0, rows].astype(F32)
            + self.far_ref[rows].astype(F32)
        )

    def finish(self):
        for made in self.done:
            made.wait_send()


STEPS = 6


def sems(*shape):
    return [pltpu.SemaphoreType.DMA(shape), pltpu.SemaphoreType.DMA(shape)]


def scatter_scratch(images, rows, width):
    return [
        pltpu.VMEM((images, 2, rows, width), BF16),
        pltpu.VMEM((images, rows, width), BF16),
        pltpu.VMEM((images, rows, width), BF16),
    ]


def params(cid):
    return pltpu.CompilerParams(collective_id=cid, has_side_effects=True, vmem_limit_bytes=60 << 20)


def open_body(x_ref, gain_ref, shift_ref, grad_ref, normed_ref, gfull_ref, send, recv):
    images, rows, _ = x_ref.shape
    me, side, over, _ = plane()
    greet((side, over))
    gathers = []
    for i in range(images):
        normed_ref[i, me] = norm_forward(x_ref[i].astype(F32), gain_ref[...], shift_ref[...])
        step = Gather(normed_ref.at[i], send.at[0, i], recv.at[0, i])
        step.start()
        gathers.append(step)
    for i in range(images):
        gfull_ref[i, me] = grad_ref[i]
        gathers[i].forward()
    more = []
    for i in range(images):
        step = Gather(gfull_ref.at[i], send.at[1, i], recv.at[1, i])
        step.start()
        more.append(step)
    for step in more:
        step.forward()
    for step in gathers + more:
        step.finish()


def open_plane(block_input, gain, shift, grad_out):
    images, rows, width = block_input.shape
    full = jax.ShapeDtypeStruct((images, 4, rows, width), BF16)
    return pl.pallas_call(
        open_body,
        out_shape=(full, full),
        in_specs=[VMEM] * 4,
        out_specs=(VMEM, VMEM),
        scratch_shapes=sems(2, images, STEPS),
        compiler_params=params(0),
        name="open_plane",
    )(block_input, gain, shift, grad_out)


def middle_body(
    part_ref, x_ref, bias_ref, gain_ref, shift_ref, hidden_ref, normed_ref, near, far, passing, ssend, srecv, gsend, grecv
):
    images, rows, _ = x_ref.shape
    me, side, over, _ = plane()
    greet((side, over))
    sums = []
    for i in range(images):
        step = Scatter(part_ref.at[i], near.at[i], far.at[i], passing.at[i], ssend.at[i], srecv.at[i])
        step.start()
        sums.append(step)
    for step in sums:
        step.forward()
    gathers = []
    for i in range(images):
        sums[i].arrive()
        hidden = x_ref[i].astype(F32) + sums[i].total(pl.ds(0, rows)) + bias_ref[...]
        hidden_ref[i] = hidden
        normed_ref[i, me] = norm_forward(hidden, gain_ref[...], shift_ref[...])
        step = Gather(normed_ref.at[i], gsend.at[i], grecv.at[i])
        step.start()
        gathers.append(step)
    for step in gathers:
        step.forward()
    for step in sums + gathers:
        step.finish()


def middle_plane(part, block_input, bias, gain, shift):
    images, rows, width = block_input.shape
    return pl.pallas_call(
        middle_body,
        out_shape=(
            jax.ShapeDtypeStruct((images, rows, width), F32),
            jax.ShapeDtypeStruct((images, 4, rows, width), BF16),
        ),
        in_specs=[VMEM] * 5,
        out_specs=(VMEM, VMEM),
        scratch_shapes=scatter_scratch(images, rows, width) + sems(images, STEPS) + sems(images, STEPS),
        compiler_params=params(1),
        name="middle_plane",
    )(part, block_input, bias, gain, shift)


def turn_body(
    gpart_ref, mpart_ref, hidden_ref, grad_ref, gain_ref, dbias_ref,
    out_ref, ghid_ref, glow_ref, sums_ref,
    near, far, passing, near2, far2, passing2, ssend, srecv, msend, mrecv, gsend, grecv,
):
    images, rows, _ = hidden_ref.shape
    me, side, over, _ = plane()
    greet((side, over))
    sums, outs = [], []
    for i in range(images):
        step = Scatter(gpart_ref.at[i], near.at[i], far.at[i], passing.at[i], ssend.at[i], srecv.at[i])
        step.start()
        sums.append(step)
    for step in sums:
        step.forward()
    for i in range(images):
        step = Scatter(mpart_ref.at[i], near2.at[i], far2.at[i], passing2.at[i], msend.at[i], mrecv.at[i])
        outs.append(step)
    outs[0].start()
    gathers = []
    totals = [0.0, 0.0, 0.0, 0.0]
    for i in range(images):
        sums[i].arrive()
        grad_normed = sums[i].total(pl.ds(0, rows))
        unit, inv_std = norm_stats(hidden_ref[i])
        upper = grad_ref[i].astype(F32)
        grad_hidden = upper + norm_backward(grad_normed, unit, inv_std, gain_ref[...])
        ghid_ref[i] = grad_hidden
        glow_ref[i, me] = grad_hidden.astype(BF16)
        step = Gather(glow_ref.at[i], gsend.at[i], grecv.at[i])
        step.start()
        gathers.append(step)
        for k, term in enumerate((grad_normed * unit, grad_normed, grad_hidden, upper)):
            totals[k] = totals[k] + jnp.sum(term, axis=0, keepdims=True)
    for k in range(4):
        sums_ref[k : k + 1] = totals[k]
    outs[0].forward()
    for step in gathers:
        step.forward()
    for step in outs[1:]:
        step.start()
    for step in outs[1:]:
        step.forward()
    for i in range(images):
        outs[i].arrive()
        out_ref[i] = (hidden_ref[i] + outs[i].total(pl.ds(0, rows)) + dbias_ref[...]).astype(BF16)
    for step in sums + outs + gathers:
        step.finish()


def turn_plane(gpart, mpart, hidden, grad_out, gain, dbias):
    images, rows, width = hidden.shape
    return pl.pallas_call(
        turn_body,
        out_shape=(
            jax.ShapeDtypeStruct((images, rows, width), BF16),
            jax.ShapeDtypeStruct((images, rows, width), F32),
            jax.ShapeDtypeStruct((images, 4, rows, width), BF16),
            jax.ShapeDtypeStruct((4, width), F32),
        ),
        in_specs=[VMEM] * 6,
        out_specs=(VMEM,) * 4,
        scratch_shapes=scatter_scratch(images, rows, width) * 2 + sems(images, STEPS) * 3,
        compiler_params=params(2),
        name="turn_plane",
    )(gpart, mpart, hidden, grad_out, gain, dbias)


def close_body(
    part_ref, x_ref, ghid_ref, gain_ref, out_ref, sums_ref, near, far, passing, ssend, srecv
):
    images, rows, _ = x_ref.shape
    me, side, over, _ = plane()
    greet((side, over))
    sums = []
    for i in range(images):
        step = Scatter(part_ref.at[i], near.at[i], far.at[i], passing.at[i], ssend.at[i], srecv.at[i])
        step.start()
        sums.append(step)
    for step in sums:
        step.forward()
    totals = [0.0, 0.0]
    for i in range(images):
        sums[i].arrive()
        grad_normed = sums[i].total(pl.ds(0, rows))
        unit, inv_std = norm_stats(x_ref[i].astype(F32))
        out_ref[i] = ghid_ref[i] + norm_backward(grad_normed, unit, inv_std, gain_ref[...])
        for k, term in enumerate((grad_normed * unit, grad_normed)):
            totals[k] = totals[k] + jnp.sum(term, axis=0, keepdims=True)
    for k in range(2):
        sums_ref[k : k + 1] = totals[k]
    for step in sums:
        step.finish()


def close_plane(part, block_input, ghid, gain):
    images, rows, width = block_input.shape
    return pl.pallas_call(
        close_body,
        out_shape=(
            jax.ShapeDtypeStruct((images, rows, width), F32),
            jax.ShapeDtypeStruct((2, width), F32),
        ),
        in_specs=[VMEM] * 4,
        out_specs=(VMEM, VMEM),
        scratch_shapes=scatter_scratch(images, rows, width) + sems(images, STEPS),
        compiler_params=params(3),
        name="close_plane",
    )(part, block_input, ghid, gain)


def small_body(groups, both_ref, own_ref, both_out, own_out, both_in, own_in, side_in, over_in, held, send, recv, psend, precv):
    row = lax.axis_index("dp")
    me, side, over, _ = plane()
    barrier = pltpu.get_barrier_semaphore()
    for k in range(1, groups):
        pl.semaphore_signal(
            barrier, inc=1, device_id={"dp": lax.rem(row + k, groups)}, device_id_type=MESH
        )
    for peer in (side, over):
        pl.semaphore_signal(barrier, inc=1, device_id={"tensor": peer}, device_id_type=MESH)
    pl.semaphore_wait(barrier, groups + 1)
    copies = []
    for k in range(1, groups):
        for j, (src, dst) in enumerate(((both_ref, both_in), (own_ref, own_in))):
            made = pltpu.make_async_remote_copy(
                src_ref=src,
                dst_ref=dst.at[row],
                send_sem=send.at[j, k],
                recv_sem=recv.at[j, k],
                device_id={"dp": lax.rem(row + k, groups)},
                device_id_type=MESH,
            )
            made.start()
            copies.append(made)
    both_in[row] = both_ref[...]
    own_in[row] = own_ref[...]
    for made in copies:
        made.wait()
    held[0] = jnp.sum(both_in[...], axis=0)
    own_out[...] = jnp.sum(own_in[...], axis=0)
    first = remote(held.at[0], side_in, psend.at[0], precv.at[0], side)
    first.start()
    first.wait()
    held[1] = held[0] + side_in[...]
    second = remote(held.at[1], over_in, psend.at[1], precv.at[1], over)
    second.start()
    second.wait()
    both_out[...] = held[1] + over_in[...]


def small_sums(groups, both, own):
    return pl.pallas_call(
        functools.partial(small_body, groups),
        out_shape=(
            jax.ShapeDtypeStruct(both.shape, F32),
            jax.ShapeDtypeStruct(own.shape, F32),
        ),
        in_specs=[VMEM] * 2,
        out_specs=(VMEM, VMEM),
        scratch_shapes=[
            pltpu.VMEM((groups,) + both.shape, F32),
            pltpu.VMEM((groups,) + own.shape, F32),
            pltpu.VMEM(both.shape, F32),
            pltpu.VMEM(both.shape, F32),
            pltpu.VMEM((2,) + both.shape, F32),
        ]
        + sems(2, groups)
        + sems(2),
        compiler_params=params(4),
        name="small_sums",
    )(both, own)


def gather_rows(rows):
    return lax.all_gather(rows, "tensor", axis=1, tiled=True)


def scatter_rows(part):
    return lax.psum_scatter(part, "tensor", scatter_dimension=1, tiled=True).astype(F32)


def shards(
    groups,
    ranks,
    block_input,
    key_mask,
    attn_norm_gain,
    attn_norm_bias,
    qkv_weight,
    qv_bias,
    out_weight,
    out_bias,
    mlp_norm_gain,
    mlp_norm_bias,
    hidden_weight,
    hidden_bias,
    down_weight,
    down_bias,
    grad_out,
):
    flat = ranks == 4
    images, rows, model = block_input.shape
    seq = key_mask.shape[1]
    width = qkv_weight.shape[2]
    units = hidden_weight.shape[1]
    row = lambda v: v.reshape(1, -1)
    whole = lambda v: v.reshape(images, seq, model)
    split = lambda v: v.reshape(images, ranks, rows, model)

    def weight(shard):
        return lax.all_gather(shard, "dp", axis=0, tiled=True)

    def owned(grad):
        return lax.psum_scatter(grad.astype(BF16), "dp", scatter_dimension=0, tiled=True).astype(F32)

    qkv_all = weight(qkv_weight.reshape(-1, 3 * width))
    out_all = weight(out_weight.T)
    hidden_all = weight(hidden_weight)
    down_all = weight(down_weight.T)

    lens = jnp.sum(key_mask, axis=1)
    if flat:
        normed_one, grad_full = open_plane(
            block_input, row(attn_norm_gain), row(attn_norm_bias), grad_out
        )
        normed_one, grad_full = whole(normed_one), whole(grad_full)
    else:
        in_float = block_input.astype(F32)
        normed_one = gather_rows(norm_forward(in_float, attn_norm_gain, attn_norm_bias))
        grad_full = gather_rows(grad_out)

    shift = jnp.concatenate([qv_bias[0], jnp.zeros_like(qv_bias[0]), qv_bias[1]])
    proj = jnp.einsum("isd,df->isf", normed_one, qkv_all, preferred_element_type=F32) + shift
    proj = proj.astype(BF16)
    mixed = attend_forward(lens, proj)
    attn_part = jnp.einsum("isf,df->isd", mixed, out_all, preferred_element_type=F32).astype(BF16)
    if flat:
        hidden_res, normed_two = middle_plane(
            split(attn_part), block_input, row(out_bias), row(mlp_norm_gain), row(mlp_norm_bias)
        )
        normed_two = whole(normed_two)
    else:
        hidden_res = in_float + scatter_rows(attn_part) + out_bias
        normed_two = gather_rows(norm_forward(hidden_res, mlp_norm_gain, mlp_norm_bias))

    pre_act = jnp.einsum("isd,df->isf", normed_two, hidden_all, preferred_element_type=F32) + hidden_bias
    value, slope = gelu_both(pre_act)
    activated = value.astype(BF16)
    grad_act = jnp.einsum("isd,df->isf", grad_full, down_all, preferred_element_type=F32)
    grad_pre = grad_act * slope
    grad_hidden_b = jnp.sum(grad_pre, axis=(0, 1))
    grad_pre_low = grad_pre.astype(BF16)
    gpart = jnp.einsum("isf,df->isd", grad_pre_low, hidden_all, preferred_element_type=F32).astype(BF16)
    mpart = jnp.einsum("isf,df->isd", activated, down_all, preferred_element_type=F32).astype(BF16)
    if flat:
        block_output, grad_hidden, hidden_full, mlp_sums = turn_plane(
            split(gpart), split(mpart), hidden_res, grad_out, row(mlp_norm_gain), row(down_bias)
        )
        hidden_full = whole(hidden_full)
    else:
        block_output = (hidden_res + scatter_rows(mpart) + down_bias).astype(BF16)
        grad_float = grad_out.astype(F32)
        grad_normed = scatter_rows(gpart)
        unit, inv_std = norm_stats(hidden_res)
        grad_hidden = grad_float + norm_backward(grad_normed, unit, inv_std, mlp_norm_gain)
        hidden_full = gather_rows(grad_hidden.astype(BF16))
        mlp_sums = jnp.stack(
            [jnp.sum(v, axis=(0, 1)) for v in (grad_normed * unit, grad_normed, grad_hidden, grad_float)]
        )
    grad_hidden_w = owned(jnp.einsum("isd,isf->df", normed_two, grad_pre_low, preferred_element_type=F32))
    grad_down_w = owned(jnp.einsum("isd,isf->df", grad_full, activated, preferred_element_type=F32))

    grad_mixed = jnp.einsum("isd,df->isf", hidden_full, out_all, preferred_element_type=F32).astype(BF16)
    grad_proj, proj_sums = attend_backward(lens, proj, grad_mixed)
    npart = jnp.einsum("isf,df->isd", grad_proj, qkv_all, preferred_element_type=F32).astype(BF16)
    grad_out_w = owned(jnp.einsum("isd,isf->df", hidden_full, mixed, preferred_element_type=F32))
    grad_qkv_w = owned(jnp.einsum("isd,isf->df", normed_one, grad_proj, preferred_element_type=F32))
    if flat:
        grad_input, attn_sums = close_plane(split(npart), block_input, grad_hidden, row(attn_norm_gain))
    else:
        grad_normed = scatter_rows(npart)
        unit, inv_std = norm_stats(in_float)
        grad_input = grad_hidden + norm_backward(grad_normed, unit, inv_std, attn_norm_gain)
        attn_sums = jnp.stack([jnp.sum(v, axis=(0, 1)) for v in (grad_normed * unit, grad_normed)])

    both = jnp.concatenate([mlp_sums, attn_sums])
    proj_sums = jnp.sum(proj_sums, axis=(0, 1))
    own = jnp.concatenate([proj_sums[:width], proj_sums[2 * width :], grad_hidden_b])
    if flat:
        pad = -own.shape[0] % 1024
        both, own = small_sums(
            groups, jnp.pad(both, ((0, 2), (0, 0))), jnp.pad(own, (0, pad)).reshape(8, -1)
        )
        own = own.reshape(-1)
    else:
        both = lax.psum(both, ("dp", "tensor"))
        own = lax.psum(own, "dp")
    return (
        block_output,
        grad_input,
        both[4],
        both[5],
        grad_qkv_w.reshape(-1, 3, width),
        own[: 2 * width].reshape(2, width),
        grad_out_w.T,
        both[2],
        both[0],
        both[1],
        grad_hidden_w,
        own[2 * width : 2 * width + units],
        grad_down_w.T,
        both[3],
    )


def solution(mesh):
    return jax.shard_map(
        functools.partial(shards, mesh.shape["dp"], mesh.shape["tensor"]),
        mesh=mesh,
        in_specs=(
            P("dp", "tensor", None),
            P("dp", None),
            P(),
            P(),
            P("dp", None, "tensor"),
            P(None, "tensor"),
            P("tensor", "dp"),
            P(),
            P(),
            P(),
            P("dp", "tensor"),
            P("tensor"),
            P("tensor", "dp"),
            P(),
            P("dp", "tensor", None),
        ),
        out_specs=(
            P("dp", "tensor", None),
            P("dp", "tensor", None),
            P(),
            P(),
            P("dp", None, "tensor"),
            P(None, "tensor"),
            P("tensor", "dp"),
            P(),
            P(),
            P(),
            P("dp", "tensor"),
            P("tensor"),
            P("tensor", "dp"),
            P(),
        ),
        check_vma=False,
    )
```

```python
import functools
import math

import jax
import jax.numpy as jnp
from jax import lax
from jax.experimental import pallas as pl
from jax.experimental.pallas import tpu as pltpu
from jax.sharding import PartitionSpec as P

HD = 72
CHUNK = 768
F32 = jnp.float32
BF16 = jnp.bfloat16
LOG2E = math.log2(math.e)
NN = (((1,), (0,)), ((), ()))
NT = (((1,), (1,)), ((), ()))
TN = (((0,), (0,)), ((), ()))
MESH = pl.DeviceIdType.MESH
ANY = pl.BlockSpec(memory_space=pl.ANY)
VMEM = pl.BlockSpec(memory_space=pltpu.VMEM)
SMEM = pl.BlockSpec(memory_space=pltpu.SMEM)


layer_eps = 1e-06
gelu_root = math.sqrt(2.0 / math.pi)
gelu_cubic = 0.044715


def norm_stats(rows):
    center = rows - jnp.mean(rows, axis=-1, keepdims=True)
    inv_std = lax.rsqrt(jnp.mean(center * center, axis=-1, keepdims=True) + layer_eps)
    return (center * inv_std, inv_std)


def norm_forward(rows, gain, shift):
    unit, _ = norm_stats(rows)
    return (unit * gain + shift).astype(BF16)


def norm_backward(grad_normed, unit, inv_std, gain):
    scaled = grad_normed * gain
    return inv_std * (
        scaled
        - jnp.mean(scaled, axis=-1, keepdims=True)
        - unit * jnp.mean(scaled * unit, axis=-1, keepdims=True)
    )


def gelu_both(pre):
    tangent = jnp.tanh(gelu_root * (pre + gelu_cubic * pre * pre * pre))
    value = 0.5 * pre * (1.0 + tangent)
    slope = 0.5 * (1.0 + tangent) + 0.5 * pre * (1.0 - tangent * tangent) * gelu_root * (
        1.0 + 3.0 * gelu_cubic * pre * pre
    )
    return (value, slope)


def dot(a, b, dims=NN):
    return lax.dot_general(a, b, dims, preferred_element_type=F32)


def soft_columns(keys_in, queries, row_ok, factor):
    raw = jnp.where(row_ok, dot(keys_in, queries, NT), -1e30)
    top = jnp.max(raw, axis=0, keepdims=True)
    grown = jnp.exp2((raw - top) * factor)
    total = jnp.sum(grown, axis=0, keepdims=True)
    return grown * (1.0 / total)


def attend_forward_body(seq, heads, lens_ref, proj_ref, mixed_ref, qh, kh, vh, oh):
    width = heads * HD
    padded = qh.shape[1]
    for h in range(heads):
        qh[h, :seq] = proj_ref[0, :, h * HD : (h + 1) * HD]
        qh[h, seq:] = jnp.zeros((padded - seq, HD), BF16)
        kh[h] = proj_ref[0, :, width + h * HD : width + (h + 1) * HD]
        vh[h] = proj_ref[0, :, 2 * width + h * HD : 2 * width + (h + 1) * HD].T
    length = lens_ref[pl.program_id(0)]
    factor = HD**-0.5 * LOG2E

    def head(h, _):
        def chunk(c, _):
            row_ok = lax.broadcasted_iota(jnp.int32, (seq, CHUNK), 0) < length
            at = pl.ds(pl.multiple_of(c * CHUNK, CHUNK), CHUNK)
            probs = soft_columns(kh[h], qh[h, at], row_ok, factor)
            oh[h, at] = dot(vh[h], probs.astype(BF16)).T.astype(BF16)
            return 0

        return lax.fori_loop(0, padded // CHUNK, chunk, 0)

    lax.fori_loop(0, heads, head, 0)
    for h in range(heads):
        mixed_ref[0, :, h * HD : (h + 1) * HD] = oh[h, :seq]


def attend_forward(lens, proj):
    images, seq, triple = proj.shape
    heads = triple // (3 * HD)
    padded = -(-seq // CHUNK) * CHUNK
    return pl.pallas_call(
        functools.partial(attend_forward_body, seq, heads),
        out_shape=jax.ShapeDtypeStruct((images, seq, heads * HD), BF16),
        grid=(images,),
        in_specs=[SMEM, pl.BlockSpec((1, seq, triple), lambda i: (i, 0, 0))],
        out_specs=pl.BlockSpec((1, seq, heads * HD), lambda i: (i, 0, 0)),
        scratch_shapes=[
            pltpu.VMEM((heads, padded, HD), BF16),
            pltpu.VMEM((heads, seq, HD), BF16),
            pltpu.VMEM((heads, HD, seq), BF16),
            pltpu.VMEM((heads, padded, HD), BF16),
        ],
        name="attend_forward",
    )(lens, proj)


def attend_backward_body(
    seq, heads, lens_ref, proj_ref, gmix_ref, gproj_ref, gbias_ref, qh, kh, kt, vh, gh, gq, gk, gv
):
    width = heads * HD
    padded = qh.shape[1]
    for h in range(heads):
        qh[h, :seq] = proj_ref[0, :, h * HD : (h + 1) * HD]
        qh[h, seq:] = jnp.zeros((padded - seq, HD), BF16)
        gh[h, :seq] = gmix_ref[0, :, h * HD : (h + 1) * HD]
        gh[h, seq:] = jnp.zeros((padded - seq, HD), BF16)
        keys_in = proj_ref[0, :, width + h * HD : width + (h + 1) * HD]
        kh[h] = keys_in
        kt[h] = keys_in.T
        vh[h] = proj_ref[0, :, 2 * width + h * HD : 2 * width + (h + 1) * HD]
    length = lens_ref[pl.program_id(0)]
    scale = HD**-0.5
    factor = scale * LOG2E

    def head(h, _):
        gk[h] = jnp.zeros((seq, HD), F32)
        gv[h] = jnp.zeros((seq, HD), F32)

        def chunk(c, _):
            row_ok = lax.broadcasted_iota(jnp.int32, (seq, CHUNK), 0) < length
            at = pl.ds(pl.multiple_of(c * CHUNK, CHUNK), CHUNK)
            queries = qh[h, at]
            grads = gh[h, at]
            probs = soft_columns(kh[h], queries, row_ok, factor)
            grad_probs = dot(vh[h], grads, NT)
            gv[h] += dot(probs.astype(BF16), grads)
            delta = jnp.sum(probs * grad_probs, axis=0, keepdims=True)
            grad_scores = (probs * (grad_probs - delta) * scale).astype(BF16)
            gk[h] += dot(grad_scores, queries)
            gq[h, at] = dot(kt[h], grad_scores).T
            return 0

        return lax.fori_loop(0, padded // CHUNK, chunk, 0)

    lax.fori_loop(0, heads, head, 0)
    for h in range(heads):
        for c, held in enumerate((gq, gk, gv)):
            value = held[h, :seq]
            at = slice(c * width + h * HD, c * width + (h + 1) * HD)
            gproj_ref[0, :, at] = value.astype(BF16)
            gbias_ref[0, :, at] = jnp.sum(value, axis=0, keepdims=True)


def attend_backward(lens, proj, gmix):
    images, seq, triple = proj.shape
    heads = triple // (3 * HD)
    padded = -(-seq // CHUNK) * CHUNK
    return pl.pallas_call(
        functools.partial(attend_backward_body, seq, heads),
        out_shape=(
            jax.ShapeDtypeStruct((images, seq, triple), BF16),
            jax.ShapeDtypeStruct((images, 1, triple), F32),
        ),
        grid=(images,),
        in_specs=[
            SMEM,
            pl.BlockSpec((1, seq, triple), lambda i: (i, 0, 0)),
            pl.BlockSpec((1, seq, heads * HD), lambda i: (i, 0, 0)),
        ],
        out_specs=(
            pl.BlockSpec((1, seq, triple), lambda i: (i, 0, 0)),
            pl.BlockSpec((1, 1, triple), lambda i: (i, 0, 0)),
        ),
        scratch_shapes=[
            pltpu.VMEM((heads, padded, HD), BF16),
            pltpu.VMEM((heads, seq, HD), BF16),
            pltpu.VMEM((heads, HD, seq), BF16),
            pltpu.VMEM((heads, seq, HD), BF16),
            pltpu.VMEM((heads, padded, HD), BF16),
            pltpu.VMEM((heads, padded, HD), F32),
            pltpu.VMEM((heads, seq, HD), F32),
            pltpu.VMEM((heads, seq, HD), F32),
        ],
        name="attend_backward",
    )(lens, proj, gmix)


def plane():
    me = lax.axis_index("tensor")
    side = me + 1 - 2 * lax.rem(me, 2)
    over = lax.rem(me + 2, 4)
    return (me, side, over, lax.rem(side + 2, 4))


def greet(peers):
    barrier = pltpu.get_barrier_semaphore()
    for peer in peers:
        pl.semaphore_signal(barrier, inc=1, device_id={"tensor": peer}, device_id_type=MESH)
    pl.semaphore_wait(barrier, len(peers))


def greet_both(groups, side, over):
    row = lax.axis_index("dp")
    barrier = pltpu.get_barrier_semaphore()
    peers = [{"tensor": side}, {"tensor": over}, {"dp": row + 1 - 2 * lax.rem(row, 2)}]
    peers += [{"dp": lax.rem(row + 2 * k, groups)} for k in range(1, groups // 2)]
    for peer in peers:
        pl.semaphore_signal(barrier, inc=1, device_id=peer, device_id_type=MESH)
    pl.semaphore_wait(barrier, len(peers))


def remote(src, dst, send, recv, peer):
    return pltpu.make_async_remote_copy(
        src_ref=src,
        dst_ref=dst,
        send_sem=send,
        recv_sem=recv,
        device_id={"tensor": peer},
        device_id_type=MESH,
    )


def halves_of(rows):
    first = -(-rows // 32) * 16
    return (pl.ds(0, first), pl.ds(first, rows - first))


class Gather:
    def __init__(self, all_ref, rows, send, recv):
        self.me, self.side, self.over, _ = plane()
        self.all_ref, self.send, self.recv = all_ref, send, recv
        self.low, self.high = halves_of(rows)
        self.done = []

    def copy(self, k, block, rows, peer):
        part = self.all_ref.at[block, rows]
        made = remote(part, part, self.send.at[k], self.recv.at[k], peer)
        made.start()
        self.done.append(made)
        return made

    def start(self):
        self.first = self.copy(0, self.me, self.low, self.side)
        self.second = self.copy(1, self.me, self.high, self.over)
        self.copy(2, self.me, self.high, self.side)
        self.copy(3, self.me, self.low, self.over)

    def forward(self):
        self.first.wait_recv()
        self.copy(4, self.side, self.low, self.over)
        self.second.wait_recv()
        self.copy(5, self.over, self.high, self.side)

    def arrive(self):
        for made in self.done[2:]:
            made.wait_recv()

    def finish(self):
        for made in self.done:
            made.wait_send()


class Scatter:
    def __init__(self, part_ref, rows, near_ref, far_ref, pass_ref, send, recv):
        self.me, self.side, self.over, self.cross = plane()
        self.part_ref, self.near_ref, self.far_ref, self.pass_ref = part_ref, near_ref, far_ref, pass_ref
        self.send, self.recv = send, recv
        self.halves = halves_of(rows)
        self.done = []

    def copy(self, k, src, dst, peer):
        made = remote(src, dst, self.send.at[k], self.recv.at[k], peer)
        made.start()
        self.done.append(made)
        return made

    def near(self, half, slot):
        return self.near_ref.at[slot, self.halves[half]]

    def start(self):
        low, high = self.halves
        part = self.part_ref
        self.first = self.copy(0, part.at[self.cross, low], self.near(0, 1), self.side)
        self.second = self.copy(1, part.at[self.cross, high], self.near(1, 1), self.over)
        self.third = self.copy(2, part.at[self.side, low], self.near(0, 0), self.side)
        self.fourth = self.copy(3, part.at[self.over, high], self.near(1, 0), self.over)

    def forward(self):
        low, high = self.halves
        self.first.wait_recv()
        self.pass_ref[low] = (
            self.part_ref[self.over, low].astype(F32) + self.near_ref[1, low].astype(F32)
        ).astype(BF16)
        self.fifth = self.copy(4, self.pass_ref.at[low], self.far_ref.at[low], self.over)
        self.second.wait_recv()
        self.pass_ref[high] = (
            self.part_ref[self.side, high].astype(F32) + self.near_ref[1, high].astype(F32)
        ).astype(BF16)
        self.sixth = self.copy(5, self.pass_ref.at[high], self.far_ref.at[high], self.side)

    def arrive(self):
        for made in (self.third, self.fourth, self.fifth, self.sixth):
            made.wait_recv()

    def total(self, rows):
        return (
            self.part_ref[self.me, rows].astype(F32)
            + self.near_ref[0, rows].astype(F32)
            + self.far_ref[rows].astype(F32)
        )

    def finish(self):
        for made in self.done:
            made.wait_send()


STEPS = 6


def sems(*shape):
    return [pltpu.SemaphoreType.DMA(shape), pltpu.SemaphoreType.DMA(shape)]


def scatter_scratch(images, rows, width):
    return [
        pltpu.VMEM((images, 2, rows, width), BF16),
        pltpu.VMEM((images, rows, width), BF16),
        pltpu.VMEM((images, rows, width), BF16),
    ]


def params(cid):
    return pltpu.CompilerParams(collective_id=cid, has_side_effects=True, vmem_limit_bytes=60 << 20)


def pad_rows(rows):
    return -(-rows // 16) * 16


def clear_pads(ref, rows):
    full = ref.shape[-2]
    for i in range(ref.shape[0]):
        for b in range(ref.shape[1]):
            ref[i, b, rows:full] = jnp.zeros((full - rows, ref.shape[-1]), ref.dtype)


def key_bias(mask, rows, full, seq):
    length = jnp.sum(mask.astype(F32), axis=1, keepdims=True).astype(jnp.int32)
    at = lax.broadcasted_iota(jnp.int32, (seq, 128 - HD), 0)
    lane = lax.broadcasted_iota(jnp.int32, (seq, 128 - HD), 1)
    block = sum((at >= b * full).astype(jnp.int32) for b in range(1, seq // full))
    inner = at - block * full
    good = (inner < rows) & (inner + block * rows < length)
    bias = jnp.where(good, 0.0, -1e30)
    ones = jnp.where(lane == 0, 1.0, 0.0)
    return (jnp.where(lane == 0, bias, 0.0).astype(BF16), ones.astype(BF16))


def soft_open(keys_in, queries, factor):
    raw = dot(keys_in, queries, NT)
    top = jnp.max(raw, axis=0, keepdims=True)
    grown = jnp.exp2((raw - top) * factor)
    total = jnp.sum(grown, axis=0, keepdims=True)
    return grown * (1.0 / total)


class Spread:
    def __init__(self, groups, all_ref, send, recv):
        self.groups, self.all_ref, self.send, self.recv = groups, all_ref, send, recv
        self.row = lax.axis_index("dp")
        self.twin = self.row + 1 - 2 * lax.rem(self.row, 2)
        self.done = []

    def copy(self, k, block, peer):
        part = self.all_ref.at[block]
        made = pltpu.make_async_remote_copy(
            src_ref=part,
            dst_ref=part,
            send_sem=self.send.at[k],
            recv_sem=self.recv.at[k],
            device_id={"dp": peer},
            device_id_type=MESH,
        )
        made.start()
        self.done.append(made)

    def far(self, k):
        return lax.rem(self.row + 2 * k, self.groups)

    def start(self):
        for k in range(1, self.groups // 2):
            self.copy(k, self.row, self.far(k))
        self.copy(0, self.row, self.twin)

    def forward(self):
        for k in range(1, self.groups // 2):
            self.done[k - 1].wait_recv()
            came = lax.rem(self.row + self.groups - 2 * k, self.groups)
            self.copy(self.groups // 2 + k - 1, came, self.twin)

    def arrive(self):
        for made in self.done[self.groups // 2 - 1 :]:
            made.wait_recv()

    def finish(self):
        for made in self.done:
            made.wait_send()


class Moves:
    def __init__(self, sem):
        self.sem, self.made = sem, []

    def start(self, src, dst):
        made = pltpu.make_async_copy(src, dst, self.sem.at[len(self.made)])
        made.start()
        self.made.append(made)
        return made

    def finish(self):
        for made in self.made:
            made.wait()


def front_body(
    groups, rows, heads,
    x_ref, grad_ref, mask_ref, vec_ref, shift_ref, wq_ref, wo_ref, wh_ref, wd_ref,
    one_out, full_out, two_out, hidden_out, qh_out, kh_out, vh_out, mixed_out, wq_out, wo_out, wh_out, wd_out,
    one_ref, full_ref, two_ref, hidden_ref, qh, kh, vh, mixed_ref, wq_all, wo_all, wh_all, wd_all,
    oh, part_ref, near, far, passing, osem,
    asend, arecv, fsend, frecv, ssend, srecv, gsend, grecv, wsend, wrecv,
):
    images = x_ref.shape[0]
    full = one_ref.shape[2]
    seq = 4 * full
    width = heads * HD
    me, side, over, _ = plane()
    mine = lax.axis_index("dp")
    stores = Moves(osem)
    for ref in (one_ref, full_ref, two_ref):
        clear_pads(ref, rows)
    weights = []
    for k, (own, everyone) in enumerate(((wq_ref, wq_all), (wo_ref, wo_all), (wh_ref, wh_all), (wd_ref, wd_all))):
        everyone[mine] = own[...]
        weights.append(Spread(groups, everyone, wsend.at[k], wrecv.at[k]))
    wq, wo, wh, wd = weights
    one_ref[0, me, :rows] = norm_forward(x_ref[0].astype(F32), vec_ref[0:1], vec_ref[1:2])
    greet_both(groups, side, over)
    ones, fulls, sums, twos = [], [], [], []
    for i in range(images):
        ones.append(Gather(one_ref.at[i], rows, asend.at[i], arecv.at[i]))
        fulls.append(Gather(full_ref.at[i], rows, fsend.at[i], frecv.at[i]))
        sums.append(Scatter(part_ref.at[i], rows, near.at[i], far.at[i], passing.at[i], ssend.at[i], srecv.at[i]))
        twos.append(Gather(two_ref.at[i], rows, gsend.at[i], grecv.at[i]))
    ones[0].start()
    wq.start()
    for i in range(1, images):
        one_ref[i, me, :rows] = norm_forward(x_ref[i].astype(F32), vec_ref[0:1], vec_ref[1:2])
        ones[i].start()
    wo.start()
    for i in range(images):
        full_ref[i, me, :rows] = grad_ref[i]
        bias, tail = key_bias(mask_ref[i : i + 1], rows, full, seq)
        for h in range(heads):
            kh[i, h, :, HD:] = bias
            qh[i, h, :, HD:] = tail
    for step in ones:
        step.forward()
    for step in fulls:
        step.start()
    wq.forward()
    wo.forward()
    wh.start()
    wd.start()
    factor = HD**-0.5 * LOG2E

    def project(i):
        weight = wq_all[...].reshape(-1, 3 * width)

        def block(b, _):
            at = pl.ds(pl.multiple_of(b * full, 16), full)
            value = (dot(one_ref[i, b], weight) + shift_ref[...]).astype(BF16)
            for h in range(heads):
                qh[i, h, at, :HD] = value[:, h * HD : (h + 1) * HD]
                kh[i, h, at, :HD] = value[:, width + h * HD : width + (h + 1) * HD]
                vh[i, h, at] = value[:, 2 * width + h * HD : 2 * width + (h + 1) * HD]
            return 0

        lax.fori_loop(0, 4, block, 0)

    def attend(i):
        def head(h, _):
            probs = soft_open(kh[i, h], qh[i, h], factor)
            oh[h] = dot(vh[i, h].T, probs.astype(BF16)).T.astype(BF16)
            return 0

        lax.fori_loop(0, heads, head, 0, unroll=2)
        for h in range(heads):
            for b in range(4):
                mixed_ref[i, b, :, h * HD : (h + 1) * HD] = oh[h, b * full : (b + 1) * full]

    def combine(i):
        weight = wo_all[...].reshape(-1, width)

        def block(b, _):
            part_ref[i, b] = dot(mixed_ref[i, b], weight, NT).astype(BF16)
            return 0

        lax.fori_loop(0, 4, block, 0)
        sums[i].start()

    for i in range(images):
        ones[i].arrive()
        stores.start(one_ref.at[i], one_out.at[i])
        if i == 0:
            wq.arrive()
            stores.start(wq_all, wq_out)
        project(i)
        for src, dst in ((qh, qh_out), (kh, kh_out), (vh, vh_out)):
            stores.start(src.at[i], dst.at[i])
        attend(i)
        stores.start(mixed_ref.at[i], mixed_out.at[i])
        fulls[i].forward()
        if i == 0:
            wo.arrive()
            stores.start(wo_all, wo_out)
        combine(i)
    for step in sums:
        step.forward()
    wh.forward()
    for i in range(images):
        sums[i].arrive()
        hidden = x_ref[i].astype(F32) + sums[i].total(pl.ds(0, rows)) + vec_ref[2:3]
        hidden_ref[i] = hidden
        two_ref[i, me, :rows] = norm_forward(hidden, vec_ref[3:4], vec_ref[4:5])
        twos[i].start()
        stores.start(hidden_ref.at[i], hidden_out.at[i])
        fulls[i].arrive()
        stores.start(full_ref.at[i], full_out.at[i])
    for step in twos:
        step.forward()
    wd.forward()
    wh.arrive()
    stores.start(wh_all, wh_out)
    wd.arrive()
    stores.start(wd_all, wd_out)
    for i in range(images):
        twos[i].arrive()
        stores.start(two_ref.at[i], two_out.at[i])
    for step in ones + fulls + sums + twos + weights:
        step.finish()
    stores.finish()


def front(groups, block_input, grad_out, key_mask, vectors, shift, wq, wo, wh, wd):
    images, rows, model = block_input.shape
    full = pad_rows(rows)
    width = wo.shape[1]
    units = wh.shape[1]
    heads = width // HD
    seq = 4 * full
    depth = wq.shape[0]
    held = [
        ((images, 4, full, model), BF16),
        ((images, 4, full, model), BF16),
        ((images, 4, full, model), BF16),
        ((images, rows, model), F32),
        ((images, heads, seq, 128), BF16),
        ((images, heads, seq, 128), BF16),
        ((images, heads, seq, HD), BF16),
        ((images, 4, full, width), BF16),
        ((groups, depth, 3 * width), BF16),
        ((groups, depth, width), BF16),
        ((groups, depth, units), BF16),
        ((groups, depth, units), BF16),
    ]
    return pl.pallas_call(
        functools.partial(front_body, groups, rows, heads),
        out_shape=tuple(jax.ShapeDtypeStruct(*h) for h in held),
        in_specs=[VMEM] * 9,
        out_specs=(ANY,) * len(held),
        scratch_shapes=[pltpu.VMEM(*h) for h in held]
        + [pltpu.VMEM((heads, seq, HD), BF16), pltpu.VMEM((images, 4, full, model), BF16)]
        + scatter_scratch(images, full, model)
        + [pltpu.SemaphoreType.DMA((8 * images + 4,))]
        + sems(images, STEPS) * 4
        + sems(4, groups),
        compiler_params=params(0),
        name="front",
    )(block_input, grad_out, key_mask, vectors, shift, wq, wo, wh, wd)


class Reduce:
    def __init__(self, groups, grad_ref, twin_ref, far_ref, tsend, trecv, fsend, frecv):
        self.groups, self.grad_ref, self.twin_ref, self.far_ref = groups, grad_ref, twin_ref, far_ref
        self.sems = (tsend, trecv, fsend, frecv)
        self.row = lax.axis_index("dp")
        self.core = lax.rem(self.row, 2)
        self.twin = self.row + 1 - 2 * self.core
        self.near, self.away = [], []

    def rows(self, block):
        depth = self.grad_ref.shape[0] // self.groups
        return pl.ds(pl.multiple_of(block * depth, 16), depth)

    def copy(self, src, dst, send, recv, peer, held):
        made = pltpu.make_async_remote_copy(
            src_ref=src, dst_ref=dst, send_sem=send, recv_sem=recv, device_id={"dp": peer}, device_id_type=MESH
        )
        made.start()
        held.append(made)

    def start(self):
        send, recv, _, _ = self.sems
        for k in range(self.groups // 2):
            theirs = self.grad_ref.at[self.rows(2 * k + 1 - self.core)]
            self.copy(theirs, self.twin_ref.at[k], send.at[k], recv.at[k], self.twin, self.near)

    def pair(self):
        _, _, send, recv = self.sems
        for made in self.near:
            made.wait_recv()
        for k in range(1, self.groups // 2):
            peer = lax.rem(self.row + 2 * k, self.groups)
            slot = lax.div(peer, 2)
            mine = self.grad_ref[self.rows(peer)].astype(F32)
            self.twin_ref[slot] = (self.twin_ref[slot].astype(F32) + mine).astype(BF16)
            self.copy(self.twin_ref.at[slot], self.far_ref.at[k], send.at[k], recv.at[k], peer, self.away)

    def total(self):
        value = self.twin_ref[lax.div(self.row, 2)].astype(F32) + self.grad_ref[self.rows(self.row)].astype(F32)
        for k, made in enumerate(self.away):
            made.wait_recv()
            value = value + self.far_ref[k + 1].astype(F32)
        return value

    def finish(self):
        for made in self.near + self.away:
            made.wait_send()


def reduce_scratch(groups, depth, width):
    half = groups // 2
    return [pltpu.VMEM((half, depth, width), BF16)] * 2 + sems(half) * 2


def outer(out_ref, left_ref, right_ref):
    images, blocks, full, model = left_ref.shape
    count = images * blocks * full
    width = right_ref.shape[-1]
    tile = 384

    def part(c, _):
        at = pl.ds(pl.multiple_of(c * tile, tile), tile)
        left = left_ref[:, :, :, at].reshape(count, tile)
        out_ref[at] = dot(left, right_ref[...].reshape(count, width), TN).astype(BF16)
        return 0

    lax.fori_loop(0, model // tile, part, 0)


def turn_body(
    groups, rows,
    two_hbm, full_hbm, wh_hbm, wd_hbm, hidden_hbm, vec_ref, hb_ref,
    glow_hbm, ghid_hbm, gwh_hbm, mpart_hbm, gwd_ref, sums_ref, hsum_ref,
    two_ref, full_ref, wh_ref, wd_ref, hidden_ref, glow_ref, ghid_ref, gwh_ref, mpart_ref,
    act_ref, gpl_ref, gpart_ref, gwd_part, lsem, osem,
    near, far, passing, twin, away, tsend, trecv, fsend, frecv, ssend, srecv, gsend, grecv,
):
    images, _, full, model = two_ref.shape
    units = wh_ref.shape[-1]
    me, side, over, _ = plane()
    loads, stores = Moves(lsem), Moves(osem)
    got = [[loads.start(two_hbm.at[0], two_ref.at[0])]]
    got[0].append(loads.start(wh_hbm, wh_ref))
    got[0].append(loads.start(full_hbm.at[0], full_ref.at[0]))
    got[0].append(loads.start(wd_hbm, wd_ref))
    for i in range(1, images):
        got.append([loads.start(two_hbm.at[i], two_ref.at[i]), loads.start(full_hbm.at[i], full_ref.at[i])])
    got_hidden = loads.start(hidden_hbm, hidden_ref)
    clear_pads(glow_ref, rows)
    hsum_ref[...] = jnp.zeros_like(hsum_ref)
    greet_both(groups, side, over)
    sums, gathers = [], []
    for i in range(images):
        sums.append(Scatter(gpart_ref.at[i], rows, near.at[i], far.at[i], passing.at[i], ssend.at[i], srecv.at[i]))
        gathers.append(Gather(glow_ref.at[i], rows, gsend.at[i], grecv.at[i]))
    down = Reduce(groups, gwd_part, twin, away, tsend, trecv, fsend, frecv)
    wide = lambda ref: ref[...].reshape(model, units)

    def ascend(i):
        def pair(c, _):
            at = pl.ds(2 * c, 2)
            pre = dot(two_ref[i, at].reshape(2 * full, model), wide(wh_ref)) + hb_ref[...]
            value, slope = gelu_both(pre)
            act_ref[i, at] = value.astype(BF16).reshape(2, full, units)
            grad_pre = dot(full_ref[i, at].reshape(2 * full, model), wide(wd_ref)) * slope
            hsum_ref[...] += jnp.sum(grad_pre, axis=0, keepdims=True)
            low = grad_pre.astype(BF16)
            gpl_ref[i, at] = low.reshape(2, full, units)
            gpart_ref[i, at] = dot(low, wide(wh_ref), NT).astype(BF16).reshape(2, full, model)
            return 0

        lax.fori_loop(0, 2, pair, 0)

    def descend(i):
        def pair(c, _):
            at = pl.ds(2 * c, 2)
            part = dot(act_ref[i, at].reshape(2 * full, units), wide(wd_ref), NT)
            mpart_ref[i, at] = part.astype(BF16).reshape(2, full, model)
            return 0

        lax.fori_loop(0, 2, pair, 0)
        stores.start(mpart_ref.at[i], mpart_hbm.at[i])

    totals = [0.0, 0.0, 0.0, 0.0]

    def settle(i):
        sums[i].arrive()
        grad_normed = sums[i].total(pl.ds(0, rows))
        unit, inv_std = norm_stats(hidden_ref[i])
        upper = full_ref[i, me, :rows].astype(F32)
        grad_hidden = upper + norm_backward(grad_normed, unit, inv_std, vec_ref[3:4])
        ghid_ref[i] = grad_hidden
        glow_ref[i, me, :rows] = grad_hidden.astype(BF16)
        gathers[i].start()
        stores.start(ghid_ref.at[i], ghid_hbm.at[i])
        for k, term in enumerate((grad_normed * unit, grad_normed, grad_hidden, upper)):
            totals[k] = totals[k] + jnp.sum(term, axis=0, keepdims=True)

    for i in range(images):
        for made in got[i]:
            made.wait()
        ascend(i)
        if i > 0:
            sums[i - 1].forward()
        sums[i].start()
    outer(gwd_part, full_ref, act_ref)
    down.start()
    got_hidden.wait()
    settle(0)
    down.pair()
    sums[-1].forward()
    outer(gwh_ref, two_ref, gpl_ref)
    stores.start(gwh_ref, gwh_hbm)
    gathers[0].forward()
    for i in range(1, images):
        settle(i)
    for i in range(images):
        descend(i)
    for k in range(4):
        sums_ref[k : k + 1] = totals[k]
    for step in gathers[1:]:
        step.forward()
    gwd_ref[...] = down.total().T
    for i in range(images):
        gathers[i].arrive()
        stores.start(glow_ref.at[i], glow_hbm.at[i])
    for step in sums + gathers + [down]:
        step.finish()
    stores.finish()


def turn(groups, rows, two, full_grad, wh, wd, hidden, vectors, bias):
    images, _, full, model = two.shape
    units = wh.shape[-1]
    depth = model // groups
    blocks = ((images, 4, full, model), BF16)
    wide = ((images, 4, full, units), BF16)
    outs = [blocks, ((images, rows, model), F32), ((model, units), BF16), blocks]
    ins = [blocks, blocks, (wh.shape, BF16), (wh.shape, BF16), (hidden.shape, F32)]
    more = [((units, depth), F32), ((4, model), F32), ((1, units), F32)]
    return pl.pallas_call(
        functools.partial(turn_body, groups, rows),
        out_shape=tuple(jax.ShapeDtypeStruct(*h) for h in outs + more),
        in_specs=[ANY] * 5 + [VMEM] * 2,
        out_specs=(ANY,) * 4 + (VMEM,) * 3,
        scratch_shapes=[pltpu.VMEM(*h) for h in ins + outs + [wide, wide, blocks, ((model, units), BF16)]]
        + [pltpu.SemaphoreType.DMA((2 * images + 3,)), pltpu.SemaphoreType.DMA((3 * images + 1,))]
        + scatter_scratch(images, full, model)
        + reduce_scratch(groups, depth, units)
        + sems(images, STEPS) * 2,
        compiler_params=params(1),
        name="turn",
    )(two, full_grad, wh, wd, hidden, vectors, bias)


def close_body(
    groups, rows, heads,
    glow_hbm, wo_hbm, mpart_hbm, gwh_hbm, qh_hbm, kh_hbm, vh_hbm, wq_hbm, mixed_hbm, hidden_hbm, ghid_hbm, x_hbm, one_hbm,
    vec_ref, tsum_ref, hsum_ref,
    out_ref, gin_ref, gwq_ref, gwo_ref, gwh_ref, both_ref,
    tok, wo_ref, mpart_ref, gwh_part, qh, kh, vh, wq_ref, mixed_ref, hidden_ref, ghid_ref, x_ref,
    gh, gq, gk, gv, bsum, gproj, npart, gwq_part, gwo_part, lsem,
    near, far, passing, near2, far2, passing2,
    htwin, haway, htsend, htrecv, hfsend, hfrecv,
    otwin, oaway, otsend, otrecv, ofsend, ofrecv,
    qtwin, qaway, qtsend, qtrecv, qfsend, qfrecv,
    mid, msend, mrecv, ssend, srecv, vsend, vrecv, twin_in, far_in, side_in, over_in,
):
    images, _, full, model = tok.shape
    width = heads * HD
    seq = 4 * full
    me, side, over, _ = plane()
    mine = lax.axis_index("dp")
    loads = Moves(lsem)
    got_tok = loads.start(glow_hbm, tok)
    got_wo = loads.start(wo_hbm, wo_ref)
    got_qkv = [loads.start(a, b) for a, b in ((qh_hbm, qh), (kh_hbm, kh), (vh_hbm, vh))]
    got_mpart = loads.start(mpart_hbm, mpart_ref)
    got_gwh = loads.start(gwh_hbm, gwh_part)
    got_wq = loads.start(wq_hbm, wq_ref)
    got_late = [loads.start(a, b) for a, b in ((mixed_hbm, mixed_ref), (hidden_hbm, hidden_ref), (ghid_hbm, ghid_ref), (x_hbm, x_ref))]
    bsum[...] = jnp.zeros_like(bsum)
    greet_both(groups, side, over)
    outs, sums = [], []
    for i in range(images):
        outs.append(Scatter(mpart_ref.at[i], rows, near2.at[i], far2.at[i], passing2.at[i], msend.at[i], mrecv.at[i]))
        sums.append(Scatter(npart.at[i], rows, near.at[i], far.at[i], passing.at[i], ssend.at[i], srecv.at[i]))
    red_h = Reduce(groups, gwh_part, htwin, haway, htsend, htrecv, hfsend, hfrecv)
    red_o = Reduce(groups, gwo_part, otwin, oaway, otsend, otrecv, ofsend, ofrecv)
    red_q = Reduce(groups, gwq_part, qtwin, qaway, qtsend, qtrecv, qfsend, qfrecv)
    got_mpart.wait()
    for step in outs:
        step.start()
    got_gwh.wait()
    red_h.start()
    scale = HD**-0.5

    def attend(i):
        value = dot(tok[i].reshape(seq, model), wo_ref[...].reshape(model, width)).astype(BF16)
        for h in range(heads):
            gh[h] = value[:, h * HD : (h + 1) * HD]

        def head(h, _):
            queries = qh[i, h]
            grads = gh[h]
            keys_in = kh[i, h]
            probs = soft_open(keys_in, queries, scale * LOG2E)
            grad_probs = dot(vh[i, h], grads, NT)
            grad_values = dot(probs.astype(BF16), grads)
            delta = jnp.sum(probs * grad_probs, axis=0, keepdims=True)
            grad_scores = (probs * (grad_probs - delta) * scale).astype(BF16)
            grad_keys = dot(grad_scores, queries[:, :HD])
            grad_queries = dot(keys_in[:, :HD].T, grad_scores).T
            for c, (held, value) in enumerate(((gq, grad_queries), (gk, grad_keys), (gv, grad_values))):
                held[h] = value.astype(BF16)
                bsum[h, c : c + 1] += jnp.sum(value, axis=0, keepdims=True)
            return 0

        lax.fori_loop(0, heads, head, 0, unroll=2)
        for h in range(heads):
            for c, held in enumerate((gq, gk, gv)):
                at = slice(c * width + h * HD, c * width + (h + 1) * HD)
                for b in range(4):
                    gproj[i, b, :, at] = held[h, b * full : (b + 1) * full]

    def spread(i):
        def pair(c, _):
            at = pl.ds(2 * c, 2)
            part = dot(gproj[i, at].reshape(2 * full, 3 * width), wq_ref[...].reshape(model, 3 * width), NT)
            npart[i, at] = part.astype(BF16).reshape(2, full, model)
            return 0

        lax.fori_loop(0, 2, pair, 0)

    totals = [0.0, 0.0]

    def settle(i):
        sums[i].arrive()
        grad_normed = sums[i].total(pl.ds(0, rows))
        unit, inv_std = norm_stats(x_ref[i].astype(F32))
        gin_ref[i] = ghid_ref[i] + norm_backward(grad_normed, unit, inv_std, vec_ref[0:1])
        for k, term in enumerate((grad_normed * unit, grad_normed)):
            totals[k] = totals[k] + jnp.sum(term, axis=0, keepdims=True)

    got_tok.wait()
    got_wo.wait()
    for made in got_qkv:
        made.wait()
    for i in range(images):
        attend(i)
        if i == 0:
            red_h.pair()
            for step in outs:
                step.forward()
            got_wq.wait()
        spread(i)
        if i > 0:
            sums[i - 1].forward()
        sums[i].start()
    for made in got_late:
        made.wait()
    outer(gwo_part, tok, mixed_ref)
    red_o.start()
    got_one = loads.start(one_hbm, tok)
    for i in range(images):
        outs[i].arrive()
        out_ref[i] = (hidden_ref[i] + outs[i].total(pl.ds(0, rows)) + vec_ref[5:6]).astype(BF16)
    sums[-1].forward()
    red_o.pair()
    got_one.wait()
    outer(gwq_part, tok, gproj)
    red_q.start()
    settle(0)
    red_q.pair()
    for i in range(1, images):
        settle(i)

    mid[0] = jnp.zeros_like(mid[0])
    mid[0, 0:4] = tsum_ref[...]
    for k in range(2):
        mid[0, 4 + k : 5 + k] = totals[k]
    for h in range(heads):
        for c in range(3):
            mid[0, 6:7, c * width + h * HD : c * width + (h + 1) * HD] = bsum[h, c : c + 1]
    mid[0, 7:8, : hsum_ref.shape[1]] = hsum_ref[...]

    def small(k, src, dst, peer):
        made = pltpu.make_async_remote_copy(
            src_ref=src, dst_ref=dst, send_sem=vsend.at[k], recv_sem=vrecv.at[k], device_id=peer, device_id_type=MESH
        )
        made.start()
        return made

    half = groups // 2
    place = lax.div(mine, 2)
    twin = small(0, mid.at[0], twin_in, {"dp": mine + 1 - 2 * lax.rem(mine, 2)})
    gwh_ref[...] = red_h.total()
    twin.wait()
    mid[1] = mid[0] + twin_in[...]
    far_in[place] = mid[1]
    aways = [
        small(k, mid.at[1], far_in.at[place], {"dp": lax.rem(mine + 2 * k, groups)}) for k in range(1, half)
    ]
    gwo_ref[...] = red_o.total().T
    for made in aways:
        made.wait()
    held = far_in[0]
    for k in range(1, half):
        held = held + far_in[k]
    mid[2] = held
    near_sum = small(half, mid.at[2], side_in, {"tensor": side})
    near_sum.wait()
    mid[3] = mid[2] + side_in[...]
    over_sum = small(half + 1, mid.at[3], over_in, {"tensor": over})
    over_sum.wait()
    both_ref[0:6] = mid[3, 0:6] + over_in[0:6]
    both_ref[6:8] = mid[2, 6:8]
    gwq_ref[...] = red_q.total()
    for step in sums + outs + [red_h, red_o, red_q]:
        step.finish()


def close(groups, rows, heads, glow, wo, mpart, gwh, qh, kh, vh, wq, mixed, hidden, ghid, x, one, vectors, tsum, hsum):
    images, _, full, model = glow.shape
    width = heads * HD
    units = gwh.shape[-1]
    depth = model // groups
    seq = 4 * full
    held = [glow, wo, mpart, gwh, qh, kh, vh, wq, mixed, hidden, ghid, x]
    piece = pltpu.VMEM((heads, seq, HD), BF16)
    small = pltpu.VMEM((8, model), F32)
    return pl.pallas_call(
        functools.partial(close_body, groups, rows, heads),
        out_shape=(
            jax.ShapeDtypeStruct((images, rows, model), BF16),
            jax.ShapeDtypeStruct((images, rows, model), F32),
            jax.ShapeDtypeStruct((depth, 3 * width), F32),
            jax.ShapeDtypeStruct((width, depth), F32),
            jax.ShapeDtypeStruct((depth, units), F32),
            jax.ShapeDtypeStruct((8, model), F32),
        ),
        in_specs=[ANY] * 13 + [VMEM] * 3,
        out_specs=(VMEM,) * 6,
        scratch_shapes=[pltpu.VMEM(h.shape, h.dtype) for h in held]
        + [piece] * 4
        + [
            pltpu.VMEM((heads, 3, HD), F32),
            pltpu.VMEM((images, 4, full, 3 * width), BF16),
            pltpu.VMEM((images, 4, full, model), BF16),
            pltpu.VMEM((model, 3 * width), BF16),
            pltpu.VMEM((model, width), BF16),
            pltpu.SemaphoreType.DMA((13,)),
        ]
        + scatter_scratch(images, full, model) * 2
        + reduce_scratch(groups, depth, units)
        + reduce_scratch(groups, depth, width)
        + reduce_scratch(groups, depth, 3 * width)
        + [pltpu.VMEM((4, 8, model), F32)]
        + sems(images, STEPS) * 2
        + sems(groups // 2 + 2)
        + [small, pltpu.VMEM((groups // 2, 8, model), F32), small, small],
        compiler_params=params(2),
        name="close",
    )(glow, wo, mpart, gwh, qh, kh, vh, wq, mixed, hidden, ghid, x, one, vectors, tsum, hsum)


def gather_rows(rows):
    return lax.all_gather(rows, "tensor", axis=1, tiled=True)


def scatter_rows(part):
    return lax.psum_scatter(part, "tensor", scatter_dimension=1, tiled=True).astype(F32)


def shards(
    groups,
    ranks,
    block_input,
    key_mask,
    attn_norm_gain,
    attn_norm_bias,
    qkv_weight,
    qv_bias,
    out_weight,
    out_bias,
    mlp_norm_gain,
    mlp_norm_bias,
    hidden_weight,
    hidden_bias,
    down_weight,
    down_bias,
    grad_out,
):
    flat = ranks == 4
    images, rows, model = block_input.shape
    seq = key_mask.shape[1]
    width = qkv_weight.shape[2]
    units = hidden_weight.shape[1]
    row = lambda v: v.reshape(1, -1)

    def weight(shard):
        return lax.all_gather(shard, "dp", axis=0, tiled=True)

    def owned(grad):
        return lax.psum_scatter(grad.astype(BF16), "dp", scatter_dimension=0, tiled=True).astype(F32)

    shift = jnp.concatenate([qv_bias[0], jnp.zeros_like(qv_bias[0]), qv_bias[1]])
    qkv_rows, out_rows, down_rows = qkv_weight.reshape(-1, 3 * width), out_weight.T, down_weight.T
    if flat:
        vectors = jnp.stack(
            [attn_norm_gain, attn_norm_bias, out_bias, mlp_norm_gain, mlp_norm_bias, down_bias] + [out_bias] * 2
        )
        (
            normed_one, grad_full, normed_two, hidden_res, qh, kh, vh, mixed, qkv_all, out_all, hidden_all, down_all
        ) = front(
            groups, block_input, grad_out, key_mask, vectors, row(shift), qkv_rows, out_rows, hidden_weight, down_rows
        )
        hidden_full, grad_hidden, hidden_part, mpart, grad_down_w, mlp_sums, unit_sums = turn(
            groups, rows, normed_two, grad_full, hidden_all, down_all, hidden_res, vectors, row(hidden_bias)
        )
        block_output, grad_input, grad_qkv_w, grad_out_w, grad_hidden_w, both = close(
            groups, rows, width // HD, hidden_full, out_all, mpart, hidden_part, qh, kh, vh, qkv_all, mixed,
            hidden_res, grad_hidden, block_input, normed_one, vectors, mlp_sums, unit_sums,
        )
        proj_sums = both[6, : 3 * width]
        grad_hidden_b = both[7, :units]
    else:
        hidden_all, down_all = weight(hidden_weight), weight(down_rows)
        qkv_all, out_all = weight(qkv_rows), weight(out_rows)
        lens = jnp.sum(key_mask, axis=1)
        in_float = block_input.astype(F32)
        normed_one = gather_rows(norm_forward(in_float, attn_norm_gain, attn_norm_bias))
        grad_full = gather_rows(grad_out)
        proj = jnp.einsum("isd,df->isf", normed_one, qkv_all, preferred_element_type=F32) + shift
        proj = proj.astype(BF16)
        mixed = attend_forward(lens, proj)
        attn_part = jnp.einsum("isf,df->isd", mixed, out_all, preferred_element_type=F32).astype(BF16)
        hidden_res = in_float + scatter_rows(attn_part) + out_bias
        normed_two = gather_rows(norm_forward(hidden_res, mlp_norm_gain, mlp_norm_bias))
        pre_act = jnp.einsum("isd,df->isf", normed_two, hidden_all, preferred_element_type=F32) + hidden_bias
        value, slope = gelu_both(pre_act)
        activated = value.astype(BF16)
        grad_act = jnp.einsum("isd,df->isf", grad_full, down_all, preferred_element_type=F32)
        grad_pre = grad_act * slope
        grad_hidden_b = jnp.sum(grad_pre, axis=(0, 1))
        grad_pre_low = grad_pre.astype(BF16)
        gpart = jnp.einsum("isf,df->isd", grad_pre_low, hidden_all, preferred_element_type=F32).astype(BF16)
        mpart = jnp.einsum("isf,df->isd", activated, down_all, preferred_element_type=F32).astype(BF16)
        block_output = (hidden_res + scatter_rows(mpart) + down_bias).astype(BF16)
        grad_float = grad_out.astype(F32)
        grad_normed = scatter_rows(gpart)
        unit, inv_std = norm_stats(hidden_res)
        grad_hidden = grad_float + norm_backward(grad_normed, unit, inv_std, mlp_norm_gain)
        hidden_full = gather_rows(grad_hidden.astype(BF16))
        mlp_sums = jnp.stack(
            [jnp.sum(v, axis=(0, 1)) for v in (grad_normed * unit, grad_normed, grad_hidden, grad_float)]
        )
        grad_hidden_w = owned(jnp.einsum("isd,isf->df", normed_two, grad_pre_low, preferred_element_type=F32))
        grad_down_w = owned(jnp.einsum("isd,isf->df", grad_full, activated, preferred_element_type=F32)).T
        grad_mixed = jnp.einsum("isd,df->isf", hidden_full, out_all, preferred_element_type=F32).astype(BF16)
        grad_proj, proj_sums = attend_backward(lens, proj, grad_mixed)
        proj_sums = jnp.sum(proj_sums, axis=(0, 1))
        npart = jnp.einsum("isf,df->isd", grad_proj, qkv_all, preferred_element_type=F32).astype(BF16)
        grad_out_w = owned(jnp.einsum("isd,isf->df", hidden_full, mixed, preferred_element_type=F32)).T
        grad_qkv_w = owned(jnp.einsum("isd,isf->df", normed_one, grad_proj, preferred_element_type=F32))
        grad_normed = scatter_rows(npart)
        unit, inv_std = norm_stats(in_float)
        grad_input = grad_hidden + norm_backward(grad_normed, unit, inv_std, attn_norm_gain)
        attn_sums = jnp.stack([jnp.sum(v, axis=(0, 1)) for v in (grad_normed * unit, grad_normed)])
        both = lax.psum(jnp.concatenate([mlp_sums, attn_sums]), ("dp", "tensor"))
        proj_sums, grad_hidden_b = lax.psum((proj_sums, grad_hidden_b), "dp")
    return (
        block_output,
        grad_input,
        both[4],
        both[5],
        grad_qkv_w.reshape(-1, 3, width),
        jnp.stack([proj_sums[:width], proj_sums[2 * width :]]),
        grad_out_w,
        both[2],
        both[0],
        both[1],
        grad_hidden_w,
        grad_hidden_b,
        grad_down_w,
        both[3],
    )


def solution(mesh):
    return jax.shard_map(
        functools.partial(shards, mesh.shape["dp"], mesh.shape["tensor"]),
        mesh=mesh,
        in_specs=(
            P("dp", "tensor", None),
            P("dp", None),
            P(),
            P(),
            P("dp", None, "tensor"),
            P(None, "tensor"),
            P("tensor", "dp"),
            P(),
            P(),
            P(),
            P("dp", "tensor"),
            P("tensor"),
            P("tensor", "dp"),
            P(),
            P("dp", "tensor", None),
        ),
        out_specs=(
            P("dp", "tensor", None),
            P("dp", "tensor", None),
            P(),
            P(),
            P("dp", None, "tensor"),
            P(None, "tensor"),
            P("tensor", "dp"),
            P(),
            P(),
            P(),
            P("dp", "tensor"),
            P("tensor"),
            P("tensor", "dp"),
            P(),
        ),
        check_vma=False,
    )
```

```python
import functools
import math

import jax
import jax.numpy as jnp
from jax import lax
from jax.experimental import pallas as pl
from jax.experimental.pallas import tpu as pltpu
from jax.sharding import PartitionSpec as P

HD = 72
CHUNK = 768
F32 = jnp.float32
BF16 = jnp.bfloat16
LOG2E = math.log2(math.e)
NN = (((1,), (0,)), ((), ()))
NT = (((1,), (1,)), ((), ()))
TN = (((0,), (0,)), ((), ()))
MESH = pl.DeviceIdType.MESH
ANY = pl.BlockSpec(memory_space=pl.ANY)
VMEM = pl.BlockSpec(memory_space=pltpu.VMEM)
SMEM = pl.BlockSpec(memory_space=pltpu.SMEM)


layer_eps = 1e-06
gelu_root = math.sqrt(2.0 / math.pi)
gelu_cubic = 0.044715


def norm_stats(rows):
    center = rows - jnp.mean(rows, axis=-1, keepdims=True)
    inv_std = lax.rsqrt(jnp.mean(center * center, axis=-1, keepdims=True) + layer_eps)
    return (center * inv_std, inv_std)


def norm_forward(rows, gain, shift):
    unit, _ = norm_stats(rows)
    return (unit * gain + shift).astype(BF16)


def norm_backward(grad_normed, unit, inv_std, gain):
    scaled = grad_normed * gain
    return inv_std * (
        scaled
        - jnp.mean(scaled, axis=-1, keepdims=True)
        - unit * jnp.mean(scaled * unit, axis=-1, keepdims=True)
    )


def gelu_both(pre):
    tangent = jnp.tanh(gelu_root * (pre + gelu_cubic * pre * pre * pre))
    value = 0.5 * pre * (1.0 + tangent)
    slope = 0.5 * (1.0 + tangent) + 0.5 * pre * (1.0 - tangent * tangent) * gelu_root * (
        1.0 + 3.0 * gelu_cubic * pre * pre
    )
    return (value, slope)


def dot(a, b, dims=NN):
    return lax.dot_general(a, b, dims, preferred_element_type=F32)


def soft_columns(keys_in, queries, row_ok, factor):
    raw = jnp.where(row_ok, dot(keys_in, queries, NT), -1e30)
    top = jnp.max(raw, axis=0, keepdims=True)
    grown = jnp.exp2((raw - top) * factor)
    total = jnp.sum(grown, axis=0, keepdims=True)
    return grown * (1.0 / total)


def attend_forward_body(seq, heads, lens_ref, proj_ref, mixed_ref, qh, kh, vh, oh):
    width = heads * HD
    padded = qh.shape[1]
    for h in range(heads):
        qh[h, :seq] = proj_ref[0, :, h * HD : (h + 1) * HD]
        qh[h, seq:] = jnp.zeros((padded - seq, HD), BF16)
        kh[h] = proj_ref[0, :, width + h * HD : width + (h + 1) * HD]
        vh[h] = proj_ref[0, :, 2 * width + h * HD : 2 * width + (h + 1) * HD].T
    length = lens_ref[pl.program_id(0)]
    factor = HD**-0.5 * LOG2E

    def head(h, _):
        def chunk(c, _):
            row_ok = lax.broadcasted_iota(jnp.int32, (seq, CHUNK), 0) < length
            at = pl.ds(pl.multiple_of(c * CHUNK, CHUNK), CHUNK)
            probs = soft_columns(kh[h], qh[h, at], row_ok, factor)
            oh[h, at] = dot(vh[h], probs.astype(BF16)).T.astype(BF16)
            return 0

        return lax.fori_loop(0, padded // CHUNK, chunk, 0)

    lax.fori_loop(0, heads, head, 0)
    for h in range(heads):
        mixed_ref[0, :, h * HD : (h + 1) * HD] = oh[h, :seq]


def attend_forward(lens, proj):
    images, seq, triple = proj.shape
    heads = triple // (3 * HD)
    padded = -(-seq // CHUNK) * CHUNK
    return pl.pallas_call(
        functools.partial(attend_forward_body, seq, heads),
        out_shape=jax.ShapeDtypeStruct((images, seq, heads * HD), BF16),
        grid=(images,),
        in_specs=[SMEM, pl.BlockSpec((1, seq, triple), lambda i: (i, 0, 0))],
        out_specs=pl.BlockSpec((1, seq, heads * HD), lambda i: (i, 0, 0)),
        scratch_shapes=[
            pltpu.VMEM((heads, padded, HD), BF16),
            pltpu.VMEM((heads, seq, HD), BF16),
            pltpu.VMEM((heads, HD, seq), BF16),
            pltpu.VMEM((heads, padded, HD), BF16),
        ],
        name="attend_forward",
    )(lens, proj)


def attend_backward_body(
    seq, heads, lens_ref, proj_ref, gmix_ref, gproj_ref, gbias_ref, qh, kh, kt, vh, gh, gq, gk, gv
):
    width = heads * HD
    padded = qh.shape[1]
    for h in range(heads):
        qh[h, :seq] = proj_ref[0, :, h * HD : (h + 1) * HD]
        qh[h, seq:] = jnp.zeros((padded - seq, HD), BF16)
        gh[h, :seq] = gmix_ref[0, :, h * HD : (h + 1) * HD]
        gh[h, seq:] = jnp.zeros((padded - seq, HD), BF16)
        keys_in = proj_ref[0, :, width + h * HD : width + (h + 1) * HD]
        kh[h] = keys_in
        kt[h] = keys_in.T
        vh[h] = proj_ref[0, :, 2 * width + h * HD : 2 * width + (h + 1) * HD]
    length = lens_ref[pl.program_id(0)]
    scale = HD**-0.5
    factor = scale * LOG2E

    def head(h, _):
        gk[h] = jnp.zeros((seq, HD), F32)
        gv[h] = jnp.zeros((seq, HD), F32)

        def chunk(c, _):
            row_ok = lax.broadcasted_iota(jnp.int32, (seq, CHUNK), 0) < length
            at = pl.ds(pl.multiple_of(c * CHUNK, CHUNK), CHUNK)
            queries = qh[h, at]
            grads = gh[h, at]
            probs = soft_columns(kh[h], queries, row_ok, factor)
            grad_probs = dot(vh[h], grads, NT)
            gv[h] += dot(probs.astype(BF16), grads)
            delta = jnp.sum(probs * grad_probs, axis=0, keepdims=True)
            grad_scores = (probs * (grad_probs - delta) * scale).astype(BF16)
            gk[h] += dot(grad_scores, queries)
            gq[h, at] = dot(kt[h], grad_scores).T
            return 0

        return lax.fori_loop(0, padded // CHUNK, chunk, 0)

    lax.fori_loop(0, heads, head, 0)
    for h in range(heads):
        for c, held in enumerate((gq, gk, gv)):
            value = held[h, :seq]
            at = slice(c * width + h * HD, c * width + (h + 1) * HD)
            gproj_ref[0, :, at] = value.astype(BF16)
            gbias_ref[0, :, at] = jnp.sum(value, axis=0, keepdims=True)


def attend_backward(lens, proj, gmix):
    images, seq, triple = proj.shape
    heads = triple // (3 * HD)
    padded = -(-seq // CHUNK) * CHUNK
    return pl.pallas_call(
        functools.partial(attend_backward_body, seq, heads),
        out_shape=(
            jax.ShapeDtypeStruct((images, seq, triple), BF16),
            jax.ShapeDtypeStruct((images, 1, triple), F32),
        ),
        grid=(images,),
        in_specs=[
            SMEM,
            pl.BlockSpec((1, seq, triple), lambda i: (i, 0, 0)),
            pl.BlockSpec((1, seq, heads * HD), lambda i: (i, 0, 0)),
        ],
        out_specs=(
            pl.BlockSpec((1, seq, triple), lambda i: (i, 0, 0)),
            pl.BlockSpec((1, 1, triple), lambda i: (i, 0, 0)),
        ),
        scratch_shapes=[
            pltpu.VMEM((heads, padded, HD), BF16),
            pltpu.VMEM((heads, seq, HD), BF16),
            pltpu.VMEM((heads, HD, seq), BF16),
            pltpu.VMEM((heads, seq, HD), BF16),
            pltpu.VMEM((heads, padded, HD), BF16),
            pltpu.VMEM((heads, padded, HD), F32),
            pltpu.VMEM((heads, seq, HD), F32),
            pltpu.VMEM((heads, seq, HD), F32),
        ],
        name="attend_backward",
    )(lens, proj, gmix)


def plane():
    me = lax.axis_index("tensor")
    side = me + 1 - 2 * lax.rem(me, 2)
    over = lax.rem(me + 2, 4)
    return (me, side, over, lax.rem(side + 2, 4))


def greet(peers):
    barrier = pltpu.get_barrier_semaphore()
    for peer in peers:
        pl.semaphore_signal(barrier, inc=1, device_id={"tensor": peer}, device_id_type=MESH)
    pl.semaphore_wait(barrier, len(peers))


def greet_both(groups, side, over):
    row = lax.axis_index("dp")
    barrier = pltpu.get_barrier_semaphore()
    peers = [{"tensor": side}, {"tensor": over}, {"dp": row + 1 - 2 * lax.rem(row, 2)}]
    peers += [{"dp": lax.rem(row + 2 * k, groups)} for k in range(1, groups // 2)]
    for peer in peers:
        pl.semaphore_signal(barrier, inc=1, device_id=peer, device_id_type=MESH)
    pl.semaphore_wait(barrier, len(peers))


def remote(src, dst, send, recv, peer):
    return pltpu.make_async_remote_copy(
        src_ref=src,
        dst_ref=dst,
        send_sem=send,
        recv_sem=recv,
        device_id={"tensor": peer},
        device_id_type=MESH,
    )


def halves_of(rows):
    first = -(-rows // 32) * 16
    return (pl.ds(0, first), pl.ds(first, rows - first))


class Gather:
    def __init__(self, all_ref, rows, send, recv):
        me, side, over, _ = plane()
        low, high = halves_of(rows)
        plan = (
            (me, low, side),
            (me, high, over),
            (me, high, side),
            (me, low, over),
            (side, low, over),
            (over, high, side),
        )
        self.copies = []
        for k, (block, part, peer) in enumerate(plan):
            ref = all_ref.at[block, part]
            self.copies.append(remote(ref, ref, send.at[k], recv.at[k], peer))

    def start(self):
        for made in self.copies[:4]:
            made.start()

    def forward(self):
        for k in range(2):
            self.copies[k].wait_recv()
            self.copies[4 + k].start()

    def arrive(self):
        for made in self.copies[2:]:
            made.wait_recv()

    def finish(self):
        for made in self.copies:
            made.wait_send()


class Scatter:
    def __init__(self, part_ref, rows, near_ref, far_ref, pass_ref, send, recv):
        self.me, self.side, self.over, cross = plane()
        self.part_ref, self.near_ref, self.far_ref, self.pass_ref = part_ref, near_ref, far_ref, pass_ref
        self.halves = low, high = halves_of(rows)
        plan = (
            (part_ref.at[cross, low], near_ref.at[1, low], self.side),
            (part_ref.at[cross, high], near_ref.at[1, high], self.over),
            (part_ref.at[self.side, low], near_ref.at[0, low], self.side),
            (part_ref.at[self.over, high], near_ref.at[0, high], self.over),
            (pass_ref.at[low], far_ref.at[low], self.over),
            (pass_ref.at[high], far_ref.at[high], self.side),
        )
        self.copies = [remote(src, dst, send.at[k], recv.at[k], peer) for k, (src, dst, peer) in enumerate(plan)]

    def start(self):
        for made in self.copies[:4]:
            made.start()

    def forward(self):
        for k, (part, block) in enumerate(zip(self.halves, (self.over, self.side))):
            self.copies[k].wait_recv()
            mine = self.part_ref[block, part].astype(F32)
            self.pass_ref[part] = (mine + self.near_ref[1, part].astype(F32)).astype(BF16)
            self.copies[4 + k].start()

    def arrive(self):
        for made in self.copies[2:]:
            made.wait_recv()

    def total(self, rows):
        return (
            self.part_ref[self.me, rows].astype(F32)
            + self.near_ref[0, rows].astype(F32)
            + self.far_ref[rows].astype(F32)
        )

    def finish(self):
        for made in self.copies:
            made.wait_send()


STEPS = 6


def sems(*shape):
    return [pltpu.SemaphoreType.DMA(shape), pltpu.SemaphoreType.DMA(shape)]


def scatter_scratch(images, rows, width):
    return [
        pltpu.VMEM((images, 2, rows, width), BF16),
        pltpu.VMEM((images, rows, width), BF16),
        pltpu.VMEM((images, rows, width), BF16),
    ]


def params(cid):
    return pltpu.CompilerParams(collective_id=cid, has_side_effects=True, vmem_limit_bytes=60 << 20)


def lanes(width):
    return -(-width // 128) * 128


def pad_rows(rows):
    return -(-rows // 16) * 16


def clear_pads(ref, rows):
    full = ref.shape[1]
    for b in range(ref.shape[0]):
        ref[b, rows:full] = jnp.zeros((full - rows, ref.shape[2]), ref.dtype)


def at_row(ref):
    return ref[...].reshape(1, -1)


def for_image(i, images, act):
    for k in range(images):
        pl.when(i == k)(functools.partial(act, k))


def key_bias(mask, rows, full, seq):
    length = jnp.sum(mask.astype(F32), axis=1, keepdims=True).astype(jnp.int32)
    at = lax.broadcasted_iota(jnp.int32, (seq, 128 - HD), 0)
    lane = lax.broadcasted_iota(jnp.int32, (seq, 128 - HD), 1)
    block = sum((at >= b * full).astype(jnp.int32) for b in range(1, seq // full))
    inner = at - block * full
    good = (inner < rows) & (inner + block * rows < length)
    bias = jnp.where(good, 0.0, -1e30)
    ones = jnp.where(lane == 0, 1.0, 0.0)
    return (jnp.where(lane == 0, bias, 0.0).astype(BF16), ones.astype(BF16))


def soft_open(keys_in, queries, factor):
    raw = dot(keys_in, queries, NT)
    top = jnp.max(raw, axis=0, keepdims=True)
    grown = jnp.exp2((raw - top) * factor)
    total = jnp.sum(grown, axis=0, keepdims=True)
    return grown * (1.0 / total)


def over_dp(src, dst, send, recv, peer):
    return pltpu.make_async_remote_copy(
        src_ref=src, dst_ref=dst, send_sem=send, recv_sem=recv, device_id={"dp": peer}, device_id_type=MESH
    )


class Spread:
    def __init__(self, groups, all_ref, send, recv):
        row = lax.axis_index("dp")
        twin = row + 1 - 2 * lax.rem(row, 2)
        half = groups // 2
        chip = lax.div(row, 2)
        self.relayed = half == 4
        self.out, self.back = [], []
        for k in range(half):
            came = all_ref.at[lax.rem(row + groups - 2 * k, groups)]
            self.back.append(over_dp(came, came, send.at[half + k], recv.at[half + k], twin))
            if k > 0:
                mine = all_ref.at[row]
                self.out.append(over_dp(mine, mine, send.at[k], recv.at[k], lax.rem(row + 2 * k, groups)))
        self.asked = {}
        if self.relayed:
            self.asked = {0: chip != 3, 2: chip != 0}
            self.inner = (chip == 1) | (chip == 2)
            up = lax.div(chip, 2)
            came = all_ref.at[lax.rem(row + 4, groups)]
            self.relay = over_dp(came, came, send.at[0], recv.at[1 + 2 * up], row + 4 * up - 2)

    def where(self, k, act):
        if k in self.asked:
            pl.when(self.asked[k])(act)
        else:
            act()

    def start(self):
        for k in (1, 0, 2) if self.relayed else range(len(self.out)):
            self.where(k, self.out[k].start)
        self.back[0].start()

    def hop(self):
        if self.relayed:
            self.out[1].wait_recv()
            pl.when(self.inner)(self.relay.start)
            self.back[2].start()

    def forward(self):
        for k, (far, near) in enumerate(zip(self.out, self.back[1:])):
            if k != 1 or not self.relayed:
                far.wait_recv()
                near.start()

    def arrive(self):
        for made in self.back:
            made.wait_recv()

    def finish(self):
        for k, made in enumerate(self.out):
            self.where(k, made.wait_send)
        for made in self.back:
            made.wait_send()
        if self.relayed:
            pl.when(self.inner)(self.relay.wait_send)


class Moves:
    def __init__(self, sem):
        self.sem, self.made = sem, []

    def plan(self, src, dst):
        made = pltpu.make_async_copy(src, dst, self.sem.at[len(self.made)])
        self.made.append(made)
        return made

    def start(self, src, dst):
        made = self.plan(src, dst)
        made.start()
        return made

    def finish(self):
        for made in self.made:
            made.wait()


def front_body(
    groups, rows, heads,
    x_ref, grad_ref, mask_ref, gain_one, bias_one, bias_out, gain_two, bias_two, qv_ref, wq_ref, wo_ref, wh_ref, wd_ref,
    one_out, full_out, two_out, hidden_out, qh_out, kh_out, vh_out, mixed_out, wq_out, wo_out, wh_out, wd_out,
    one_ref, full_ref, two_ref, hidden_ref, qh, kh, vh, mixed_ref, wq_all, wo_all, wh_all, wd_all,
    oh, part_ref, near, far, passing, osem,
    asend, arecv, fsend, frecv, ssend, srecv, gsend, grecv, wsend, wrecv,
):
    images = x_ref.shape[0]
    full = one_ref.shape[2]
    seq = 4 * full
    width = heads * HD
    me, side, over, _ = plane()
    mine = lax.axis_index("dp")
    wq_all[mine, :, 3 * width :] = jnp.zeros_like(wq_all[mine, :, 3 * width :])
    for c in range(3):
        wq_all[mine, :, c * width : (c + 1) * width] = wq_ref[c]
    weights = [Spread(groups, wq_all, wsend.at[0], wrecv.at[0])]
    for k, (own, everyone) in enumerate(((wo_ref, wo_all), (wh_ref, wh_all), (wd_ref, wd_all))):
        count = own.shape[1]
        everyone[mine, :, count:] = jnp.zeros_like(everyone[mine, :, count:])
        everyone[mine, :, :count] = own[...]
        weights.append(Spread(groups, everyone, wsend.at[k + 1], wrecv.at[k + 1]))
    wq, wo, wh, wd = weights
    ones, sums, twos = [], [], []
    for i in range(images):
        clear_pads(one_ref.at[i], rows)
        clear_pads(two_ref.at[i], rows)
        ones.append(Gather(one_ref.at[i], rows, asend.at[i], arecv.at[i]))
        sums.append(Scatter(part_ref.at[i], rows, near.at[i], far.at[i], passing.at[i], ssend.at[i], srecv.at[i]))
        twos.append(Gather(two_ref.at[i], rows, gsend.at[i], grecv.at[i]))
    mixed_ref[:, :, :, width:] = jnp.zeros_like(mixed_ref[:, :, :, width:])
    clear_pads(full_ref, rows)
    grads = Gather(full_ref, rows, fsend, frecv)
    stores = Moves(osem)
    put_weight = [stores.plan(a, b) for a, b in ((wq_all, wq_out), (wo_all, wo_out), (wh_all, wh_out), (wd_all, wd_out))]
    put_full = stores.plan(full_ref, full_out)
    pairs = (
        (one_ref, one_out), (two_ref, two_out), (hidden_ref, hidden_out), (qh, qh_out), (kh, kh_out), (vh, vh_out),
        (mixed_ref, mixed_out),
    )
    put = [[stores.plan(a.at[i], b.at[i]) for a, b in pairs] for i in range(images)]

    def enter(i):
        one_ref[i, me, :rows] = norm_forward(x_ref[i].astype(F32), at_row(gain_one), at_row(bias_one))

    enter(0)
    greet_both(groups, side, over)
    ones[0].start()
    wq.start()
    for i in range(1, images):
        enter(i)
        ones[i].start()
    wo.start()
    wh.start()
    wd.start()
    full_ref[me, :rows] = grad_ref[0]
    for i in range(images):
        bias, tail = key_bias(mask_ref[i : i + 1], rows, full, seq)
        for h in range(heads):
            kh[i, h, :, HD:] = bias
            vh[i, h, :, HD:] = jnp.zeros_like(bias)
            qh[i, h, :, HD:] = tail
    for step in ones:
        step.forward()
    grads.start()
    wq.hop()
    wq.forward()
    factor = HD**-0.5 * LOG2E
    shift_q, shift_v = qv_ref[0:1], qv_ref[1:2]

    def project(i):
        weight = wq_all[:, :, : 3 * width].reshape(-1, 3 * width)

        def block(b, _):
            at = pl.ds(pl.multiple_of(b * full, 16), full)
            value = dot(one_ref[i, b], weight)
            queries = (value[:, :width] + shift_q).astype(BF16)
            keys_in = value[:, width : 2 * width].astype(BF16)
            values = (value[:, 2 * width :] + shift_v).astype(BF16)
            for h in range(heads):
                here = slice(h * HD, (h + 1) * HD)
                qh[i, h, at, :HD] = queries[:, here]
                kh[i, h, at, :HD] = keys_in[:, here]
                vh[i, h, at, :HD] = values[:, here]
            return 0

        lax.fori_loop(0, 4, block, 0)

    def attend(i):
        def head(h, _):
            probs = soft_open(kh[i, h], qh[i, h], factor)
            oh[h] = dot(vh[i, h, :, :HD].T, probs.astype(BF16)).T.astype(BF16)
            return 0

        lax.fori_loop(0, heads, head, 0, unroll=2)
        for h in range(heads):
            for b in range(4):
                mixed_ref[i, b, :, h * HD : (h + 1) * HD] = oh[h, b * full : (b + 1) * full]

    def combine(i):
        weight = wo_all[:, :, :width].reshape(-1, width)

        def block(b, _):
            part_ref[i, b] = dot(mixed_ref[i, b, :, :width], weight, NT).astype(BF16)
            return 0

        lax.fori_loop(0, 4, block, 0)

    def ready(k):
        ones[k].arrive()
        put[k][0].start()
        if k == 0:
            wq.arrive()
            put_weight[0].start()

    def between(k):
        for made in put[k][3:]:
            made.start()
        if k == 0:
            grads.forward()
            wo.hop()
            wo.forward()
            wh.hop()
            wo.arrive()
            put_weight[1].start()

    def send(k):
        if k > 0:
            sums[k - 1].forward()
        sums[k].start()

    def image(i, _):
        for_image(i, images, ready)
        project(i)
        attend(i)
        for_image(i, images, between)
        combine(i)
        for_image(i, images, send)
        return 0

    lax.fori_loop(0, images, image, 0)

    def settle(i):
        sums[i].arrive()
        hidden = x_ref[i].astype(F32) + sums[i].total(pl.ds(0, rows)) + at_row(bias_out)
        hidden_ref[i] = hidden
        two_ref[i, me, :rows] = norm_forward(hidden, at_row(gain_two), at_row(bias_two))
        twos[i].start()
        put[i][2].start()

    for i in range(images - 1):
        settle(i)
    sums[-1].forward()
    wd.hop()
    for i in range(images - 1):
        twos[i].forward()
    settle(images - 1)
    grads.arrive()
    put_full.start()
    wh.forward()
    twos[-1].forward()
    wh.arrive()
    put_weight[2].start()
    wd.forward()
    for i in range(images):
        twos[i].arrive()
        put[i][1].start()
    wd.arrive()
    put_weight[3].start()
    for step in ones + sums + twos + weights + [grads]:
        step.finish()
    stores.finish()


def front(groups, block_input, grad_out, key_mask, vectors, qv_bias, wq, wo, wh, wd):
    images, rows, model = block_input.shape
    full = pad_rows(rows)
    width = wo.shape[1]
    units = wh.shape[1]
    heads = width // HD
    seq = 4 * full
    depth = wo.shape[0]
    held = [
        ((images, 4, full, model), BF16),
        ((4, full, model), BF16),
        ((images, 4, full, model), BF16),
        ((images, rows, model), F32),
        ((images, heads, seq, 128), BF16),
        ((images, heads, seq, 128), BF16),
        ((images, heads, seq, 128), BF16),
        ((images, 4, full, lanes(width)), BF16),
        ((groups, depth, lanes(3 * width)), BF16),
        ((groups, depth, lanes(width)), BF16),
        ((groups, depth, lanes(units)), BF16),
        ((groups, depth, lanes(units)), BF16),
    ]
    return pl.pallas_call(
        functools.partial(front_body, groups, rows, heads),
        out_shape=tuple(jax.ShapeDtypeStruct(*h) for h in held),
        in_specs=[VMEM] * 13,
        out_specs=(ANY,) * len(held),
        scratch_shapes=[pltpu.VMEM(*h) for h in held]
        + [pltpu.VMEM((heads, seq, HD), BF16), pltpu.VMEM((images, 4, full, model), BF16)]
        + scatter_scratch(images, full, model)
        + [pltpu.SemaphoreType.DMA((7 * images + 5,))]
        + sems(images, STEPS)
        + sems(STEPS)
        + sems(images, STEPS) * 2
        + sems(4, groups),
        compiler_params=params(0),
        name="front",
    )(block_input, grad_out, key_mask, *vectors, qv_bias, wq, wo, wh, wd)


class Reduce:
    def __init__(self, groups, grad_ref, twin_ref, far_ref, tsend, trecv, fsend, frecv):
        self.grad_ref, self.twin_ref, self.far_ref = grad_ref, twin_ref, far_ref
        depth = grad_ref.shape[0] // groups
        rows = lambda block: pl.ds(pl.multiple_of(block * depth, 16), depth)
        row = lax.axis_index("dp")
        core = lax.rem(row, 2)
        self.slot, self.mine = lax.div(row, 2), rows(row)
        self.near, self.away = [], []
        for k in range(groups // 2):
            theirs = grad_ref.at[rows(2 * k + 1 - core)]
            self.near.append(over_dp(theirs, twin_ref.at[k], tsend.at[k], trecv.at[k], row + 1 - 2 * core))
        for k in range(1, groups // 2):
            peer = lax.rem(row + 2 * k, groups)
            slot = lax.div(peer, 2)
            made = over_dp(twin_ref.at[slot], far_ref.at[k - 1], fsend.at[k], frecv.at[k], peer)
            self.away.append((slot, rows(peer), made))

    def start(self):
        for made in self.near:
            made.start()

    def pair(self):
        for made in self.near:
            made.wait_recv()
        for slot, part, made in self.away:
            mine = self.grad_ref[part].astype(F32)
            self.twin_ref[slot] = (self.twin_ref[slot].astype(F32) + mine).astype(BF16)
            made.start()

    def total(self):
        value = self.twin_ref[self.slot].astype(F32) + self.grad_ref[self.mine].astype(F32)
        for k, (_, _, made) in enumerate(self.away):
            made.wait_recv()
            value = value + self.far_ref[k].astype(F32)
        return value

    def finish(self):
        for made in self.near + [made for _, _, made in self.away]:
            made.wait_send()


def reduce_scratch(groups, depth, width):
    half, width = groups // 2, lanes(width)
    return [pltpu.VMEM((half, depth, width), BF16), pltpu.VMEM((half - 1, depth, width), BF16)] + sems(half) * 2


def outer(out_ref, left_ref, right_ref, width):
    images, blocks, full, model = left_ref.shape
    count = images * blocks * full
    tile = 384
    if out_ref.shape[1] > width:
        out_ref[:, width:] = jnp.zeros_like(out_ref[:, width:])

    def part(c, _):
        at = pl.ds(pl.multiple_of(c * tile, tile), tile)
        left = left_ref[:, :, :, at].reshape(count, tile)
        right = right_ref[:, :, :, :width].reshape(count, width)
        out_ref[at, :width] = dot(left, right, TN).astype(BF16)
        return 0

    lax.fori_loop(0, model // tile, part, 0)


def turn_body(
    groups, rows,
    two_hbm, full_hbm, wh_hbm, wd_hbm, hidden_hbm, grad_ref, gain_ref, hb_ref,
    glow_hbm, ghid_hbm, gwh_hbm, mpart_hbm, gwd_ref, sums_ref, hsum_ref,
    two_ref, wh_ref, wd_ref, hidden_ref, glow_ref, ghid_ref, gwh_ref, mpart_ref,
    full_ref, act_ref, gpl_ref, gpart_ref, gwd_part, lsem, osem,
    near, far, passing, twin, away, tsend, trecv, fsend, frecv, ssend, srecv, gsend, grecv, asend, arecv,
):
    images, _, full, model = two_ref.shape
    units = hb_ref.shape[0]
    me, side, over, _ = plane()
    loads, stores = Moves(lsem), Moves(osem)
    got = [[loads.start(two_hbm.at[0], two_ref.at[0])]]
    got[0].append(loads.start(wh_hbm, wh_ref))
    got[0].append(loads.start(full_hbm, full_ref.at[0]))
    got[0].append(loads.start(wd_hbm, wd_ref))
    for i in range(1, images):
        got.append([loads.start(two_hbm.at[i], two_ref.at[i])])
    got_hidden = loads.start(hidden_hbm, hidden_ref)
    put_mpart = [stores.plan(mpart_ref.at[i], mpart_hbm.at[i]) for i in range(images)]
    put_ghid = [stores.plan(ghid_ref.at[i], ghid_hbm.at[i]) for i in range(images)]
    put_glow = [stores.plan(glow_ref.at[i], glow_hbm.at[i]) for i in range(images)]
    put_gwh = stores.plan(gwh_ref, gwh_hbm)
    hsum_ref[...] = jnp.zeros_like(hsum_ref)
    sums, gathers, grads = [], [], [None]
    for i in range(images):
        clear_pads(glow_ref.at[i], rows)
        sums.append(Scatter(gpart_ref.at[i], rows, near.at[i], far.at[i], passing.at[i], ssend.at[i], srecv.at[i]))
        gathers.append(Gather(glow_ref.at[i], rows, gsend.at[i], grecv.at[i]))
        if i > 0:
            clear_pads(full_ref.at[i], rows)
            full_ref[i, me, :rows] = grad_ref[i]
            grads.append(Gather(full_ref.at[i], rows, asend.at[i], arecv.at[i]))
    down = Reduce(groups, gwd_part, twin, away, tsend, trecv, fsend, frecv)
    greet_both(groups, side, over)
    for step in grads[1:]:
        step.start()
    wide = lambda ref: ref[:, :, :units].reshape(model, units)
    shift = at_row(hb_ref)

    def ascend(i):
        def pair(c, _):
            at = pl.ds(2 * c, 2)
            pre = dot(two_ref[i, at].reshape(2 * full, model), wide(wh_ref)) + shift
            value, slope = gelu_both(pre)
            act_ref[i, at] = value.astype(BF16).reshape(2, full, units)
            grad_pre = dot(full_ref[i, at].reshape(2 * full, model), wide(wd_ref)) * slope
            hsum_ref[...] += jnp.sum(grad_pre, axis=0, keepdims=True)
            low = grad_pre.astype(BF16)
            gpl_ref[i, at] = low.reshape(2, full, units)
            gpart_ref[i, at] = dot(low, wide(wh_ref), NT).astype(BF16).reshape(2, full, model)
            return 0

        lax.fori_loop(0, 2, pair, 0)

    def descend(k, _):
        at = pl.ds(2 * lax.rem(k, 2), 2)
        i = lax.div(k, 2)
        part = dot(act_ref[i, at].reshape(2 * full, units), wide(wd_ref), NT)
        mpart_ref[i, at] = part.astype(BF16).reshape(2, full, model)
        return 0

    totals = [0.0, 0.0, 0.0, 0.0]

    def settle(i):
        sums[i].arrive()
        grad_normed = sums[i].total(pl.ds(0, rows))
        unit, inv_std = norm_stats(hidden_ref[i])
        upper = full_ref[i, me, :rows].astype(F32)
        grad_hidden = upper + norm_backward(grad_normed, unit, inv_std, at_row(gain_ref))
        ghid_ref[i] = grad_hidden
        glow_ref[i, me, :rows] = grad_hidden.astype(BF16)
        gathers[i].start()
        put_ghid[i].start()
        for k, term in enumerate((grad_normed * unit, grad_normed, grad_hidden, upper)):
            totals[k] = totals[k] + jnp.sum(term, axis=0, keepdims=True)

    def ready(k):
        for made in got[k]:
            made.wait()
        if k > 0:
            grads[k].arrive()

    def send(k):
        if k == 0:
            for step in grads[1:]:
                step.forward()
        if k > 0:
            sums[k - 1].forward()
        sums[k].start()

    def image(i, _):
        for_image(i, images, ready)
        ascend(i)
        for_image(i, images, send)
        return 0

    lax.fori_loop(0, images, image, 0)
    outer(gwd_part, full_ref, act_ref, units)
    down.start()
    got_hidden.wait()
    for i in range(images - 1):
        settle(i)
    sums[-1].forward()
    down.pair()
    outer(gwh_ref, two_ref, gpl_ref, units)
    put_gwh.start()
    for i in range(images - 1):
        gathers[i].forward()
    settle(images - 1)
    lax.fori_loop(0, 2 * images, descend, 0)
    for made in put_mpart:
        made.start()
    gathers[-1].forward()
    for k in range(4):
        sums_ref[k : k + 1] = totals[k]
    gwd_ref[...] = down.total()[:, :units]
    for i in range(images):
        gathers[i].arrive()
        put_glow[i].start()
    for step in sums + gathers + grads[1:] + [down]:
        step.finish()
    stores.finish()


def turn(groups, rows, two, full_grad, wh, wd, hidden, grad_out, gain, bias):
    images, _, full, model = two.shape
    units = bias.shape[0]
    depth = model // groups
    blocks = ((images, 4, full, model), BF16)
    wide = ((images, 4, full, units), BF16)
    outs = [blocks, ((images, rows, model), F32), ((model, lanes(units)), BF16), blocks]
    ins = [blocks, (wh.shape, BF16), (wh.shape, BF16), (hidden.shape, F32)]
    more = [((depth, units), F32), ((4, model), F32), ((1, units), F32)]
    return pl.pallas_call(
        functools.partial(turn_body, groups, rows),
        out_shape=tuple(jax.ShapeDtypeStruct(*h) for h in outs + more),
        in_specs=[ANY] * 5 + [VMEM] * 3,
        out_specs=(ANY,) * 4 + (VMEM,) * 3,
        scratch_shapes=[pltpu.VMEM(*h) for h in ins + outs + [blocks, wide, wide, blocks, ((model, lanes(units)), BF16)]]
        + [pltpu.SemaphoreType.DMA((images + 4,)), pltpu.SemaphoreType.DMA((3 * images + 1,))]
        + scatter_scratch(images, full, model)
        + reduce_scratch(groups, depth, units)
        + sems(images, STEPS) * 3,
        compiler_params=params(1),
        name="turn",
    )(two, full_grad, wh, wd, hidden, grad_out, gain, bias)


def close_body(
    groups, rows, heads,
    glow_hbm, mixed_hbm, gwh_hbm, mpart_hbm, wo_hbm, qh_hbm, kh_hbm, vh_hbm, wq_hbm, hidden_hbm, ghid_hbm, x_hbm, one_hbm,
    gain_ref, bias_ref, tsum_ref, hsum_ref,
    out_ref, gin_ref, gwq_ref, gwo_ref, gwh_ref, both_ref,
    tok, mixed_ref, gwh_part, mpart_ref, wo_ref, qh, kh, vh, wq_ref, hidden_ref, ghid_ref, x_ref,
    gq, gk, gv, gh, bsum, gproj, npart, gwq_part, gwo_part, lsem,
    near, far, passing, near2, far2, passing2,
    htwin, haway, htsend, htrecv, hfsend, hfrecv,
    otwin, oaway, otsend, otrecv, ofsend, ofrecv,
    qtwin, qaway, qtsend, qtrecv, qfsend, qfrecv,
    mid, msend, mrecv, ssend, srecv, vsend, vrecv, twin_in, far_in, side_in, over_in,
):
    images, _, full, model = tok.shape
    width = heads * HD
    seq = 4 * full
    me, side, over, _ = plane()
    mine = lax.axis_index("dp")
    loads = Moves(lsem)
    held = (
        (glow_hbm, tok), (mixed_hbm, mixed_ref), (gwh_hbm, gwh_part), (mpart_hbm, mpart_ref), (wo_hbm, wo_ref),
        (qh_hbm, qh), (kh_hbm, kh), (vh_hbm, vh), (wq_hbm, wq_ref), (hidden_hbm, hidden_ref), (ghid_hbm, ghid_ref),
        (x_hbm, x_ref),
    )
    got = [loads.start(src, dst) for src, dst in held]
    got_one = loads.plan(one_hbm, tok)
    bsum[...] = jnp.zeros_like(bsum)
    outs, sums = [], []
    for i in range(images):
        outs.append(Scatter(mpart_ref.at[i], rows, near2.at[i], far2.at[i], passing2.at[i], msend.at[i], mrecv.at[i]))
        sums.append(Scatter(npart.at[i], rows, near.at[i], far.at[i], passing.at[i], ssend.at[i], srecv.at[i]))
    red_h = Reduce(groups, gwh_part, htwin, haway, htsend, htrecv, hfsend, hfrecv)
    red_o = Reduce(groups, gwo_part, otwin, oaway, otsend, otrecv, ofsend, ofrecv)
    red_q = Reduce(groups, gwq_part, qtwin, qaway, qtsend, qtrecv, qfsend, qfrecv)
    greet_both(groups, side, over)
    for made in got[:4]:
        made.wait()
    red_h.start()
    for step in outs:
        step.start()
    outer(gwo_part, tok, mixed_ref, width)
    red_o.start()
    got[4].wait()

    def mix(i, _):
        value = dot(tok[i].reshape(seq, model), wo_ref[:, :, :width].reshape(model, width)).astype(BF16)
        for h in range(heads):
            gh[i, h] = value[:, h * HD : (h + 1) * HD]
        return 0

    lax.fori_loop(0, images, mix, 0)
    got_one.start()
    red_h.pair()
    outs[0].forward()
    red_o.pair()
    for made in got[5:]:
        made.wait()
    scale = HD**-0.5

    def attend(i):
        def head(h, _):
            queries = qh[i, h]
            grads = gh[i, h]
            keys_in = kh[i, h]
            probs = soft_open(keys_in, queries, scale * LOG2E)
            grad_probs = dot(vh[i, h, :, :HD], grads, NT)
            grad_values = dot(probs.astype(BF16), grads)
            delta = jnp.sum(probs * grad_probs, axis=0, keepdims=True)
            grad_scores = (probs * (grad_probs - delta) * scale).astype(BF16)
            grad_keys = dot(grad_scores, queries[:, :HD])
            grad_queries = dot(keys_in[:, :HD].T, grad_scores).T
            for c, (held, value) in enumerate(((gq, grad_queries), (gk, grad_keys), (gv, grad_values))):
                held[h] = value.astype(BF16)
                bsum[h, c : c + 1] += jnp.sum(value, axis=0, keepdims=True)
            return 0

        lax.fori_loop(0, heads, head, 0, unroll=4)
        for h in range(heads):
            for c, held in enumerate((gq, gk, gv)):
                at = slice(c * width + h * HD, c * width + (h + 1) * HD)
                for b in range(4):
                    gproj[i, b, :, at] = held[h, b * full : (b + 1) * full]

    def spread(i):
        def pair(c, _):
            at = pl.ds(2 * c, 2)
            part = dot(gproj[i, at].reshape(2 * full, 3 * width), wq_ref[:, :, : 3 * width].reshape(model, 3 * width), NT)
            npart[i, at] = part.astype(BF16).reshape(2, full, model)
            return 0

        lax.fori_loop(0, 2, pair, 0)

    def between(k):
        if k == 0:
            for step in outs[1:]:
                step.forward()

    def send(k):
        if k > 0:
            sums[k - 1].forward()
        sums[k].start()

    def image(i, _):
        attend(i)
        for_image(i, images, between)
        spread(i)
        for_image(i, images, send)
        return 0

    lax.fori_loop(0, images, image, 0)
    got_one.wait()
    outer(gwq_part, tok, gproj, 3 * width)
    red_q.start()
    totals = [0.0, 0.0]

    def settle(i):
        sums[i].arrive()
        grad_normed = sums[i].total(pl.ds(0, rows))
        unit, inv_std = norm_stats(x_ref[i].astype(F32))
        gin_ref[i] = ghid_ref[i] + norm_backward(grad_normed, unit, inv_std, at_row(gain_ref))
        for k, term in enumerate((grad_normed * unit, grad_normed)):
            totals[k] = totals[k] + jnp.sum(term, axis=0, keepdims=True)

    for i in range(images - 1):
        settle(i)
    red_q.pair()
    sums[-1].forward()
    for i in range(images):
        outs[i].arrive()
        out_ref[i] = (hidden_ref[i] + outs[i].total(pl.ds(0, rows)) + at_row(bias_ref)).astype(BF16)
    gwh_ref[...] = red_h.total()[:, : gwh_ref.shape[1]]
    gwo_ref[...] = red_o.total()[:, :width]
    settle(images - 1)

    mid[0] = jnp.zeros_like(mid[0])
    mid[0, 0:4] = tsum_ref[...]
    for k in range(2):
        mid[0, 4 + k : 5 + k] = totals[k]
    for h in range(heads):
        for c in range(3):
            mid[0, 6:7, c * width + h * HD : c * width + (h + 1) * HD] = bsum[h, c : c + 1]
    mid[0, 7:8, : hsum_ref.shape[1]] = hsum_ref[...]
    half = groups // 2
    place = lax.div(mine, 2)
    twin = over_dp(mid.at[0], twin_in, vsend.at[0], vrecv.at[0], mine + 1 - 2 * lax.rem(mine, 2))
    twin.start()
    twin.wait()
    mid[1] = mid[0] + twin_in[...]
    far_in[place] = mid[1]
    aways = []
    for k in range(1, half):
        peer = lax.rem(mine + 2 * k, groups)
        aways.append(over_dp(mid.at[1], far_in.at[place], vsend.at[k], vrecv.at[k], peer))
        aways[-1].start()
    for made in aways:
        made.wait()
    held = far_in[0]
    for k in range(1, half):
        held = held + far_in[k]
    mid[2] = held
    near_sum = remote(mid.at[2], side_in, vsend.at[half], vrecv.at[half], side)
    near_sum.start()
    near_sum.wait()
    mid[3] = mid[2] + side_in[...]
    over_sum = remote(mid.at[3], over_in, vsend.at[half + 1], vrecv.at[half + 1], over)
    over_sum.start()
    over_sum.wait()
    both_ref[0:6] = mid[3, 0:6] + over_in[0:6]
    both_ref[6:8] = mid[2, 6:8]
    total = red_q.total()
    for c in range(3):
        gwq_ref[c] = total[:, c * width : (c + 1) * width]
    for step in sums + outs + [red_h, red_o, red_q]:
        step.finish()


def close(groups, rows, heads, held, one, gain, bias, tsum, hsum):
    images, _, full, model = held[0].shape
    width = heads * HD
    units = hsum.shape[1]
    depth = model // groups
    seq = 4 * full
    piece = pltpu.VMEM((heads, seq, HD), BF16)
    small = pltpu.VMEM((8, model), F32)
    return pl.pallas_call(
        functools.partial(close_body, groups, rows, heads),
        out_shape=(
            jax.ShapeDtypeStruct((images, rows, model), BF16),
            jax.ShapeDtypeStruct((images, rows, model), F32),
            jax.ShapeDtypeStruct((3, depth, width), F32),
            jax.ShapeDtypeStruct((depth, width), F32),
            jax.ShapeDtypeStruct((depth, units), F32),
            jax.ShapeDtypeStruct((8, model), F32),
        ),
        in_specs=[ANY] * 13 + [VMEM] * 4,
        out_specs=(VMEM,) * 6,
        scratch_shapes=[pltpu.VMEM(h.shape, h.dtype) for h in held]
        + [piece] * 3
        + [
            pltpu.VMEM((images, heads, seq, HD), BF16),
            pltpu.VMEM((heads, 3, HD), F32),
            pltpu.VMEM((images, 4, full, 3 * width), BF16),
            pltpu.VMEM((images, 4, full, model), BF16),
            pltpu.VMEM((model, lanes(3 * width)), BF16),
            pltpu.VMEM((model, lanes(width)), BF16),
            pltpu.SemaphoreType.DMA((13,)),
        ]
        + scatter_scratch(images, full, model) * 2
        + reduce_scratch(groups, depth, units)
        + reduce_scratch(groups, depth, width)
        + reduce_scratch(groups, depth, 3 * width)
        + [pltpu.VMEM((4, 8, model), F32)]
        + sems(images, STEPS) * 2
        + sems(groups // 2 + 2)
        + [small, pltpu.VMEM((groups // 2, 8, model), F32), small, small],
        compiler_params=params(2),
        name="close",
    )(*held, one, gain, bias, tsum, hsum)


def deliver_body(width, out, gin, gwq, gwo, gwh, gwd, both, *refs):
    refs, sem = refs[:-1], refs[-1]
    loads = Moves(sem)
    for src, dst in zip((out, gin, gwq, gwo, gwh, gwd), refs):
        loads.start(src, dst)
    qv, unit = refs[6:8]
    qv[0:1] = both[6:7, :width]
    qv[1:2] = both[6:7, 2 * width : 3 * width]
    unit[...] = both[7, : unit.shape[0]]
    for k, dst in enumerate(refs[8:]):
        dst[...] = both[k]
    loads.finish()


def deliver(width, units, out, gin, gwq, gwo, gwh, gwd, both):
    model = both.shape[1]
    same = [jax.ShapeDtypeStruct(v.shape, v.dtype) for v in (out, gin, gwq, gwo, gwh, gwd)]
    more = [jax.ShapeDtypeStruct(dims, F32) for dims in ((2, width), (units,)) + ((model,),) * 6]
    return pl.pallas_call(
        functools.partial(deliver_body, width),
        out_shape=tuple(same + more),
        in_specs=[ANY] * 6 + [VMEM],
        out_specs=(VMEM,) * 14,
        scratch_shapes=[pltpu.SemaphoreType.DMA((6,))],
        compiler_params=pltpu.CompilerParams(vmem_limit_bytes=60 << 20),
        name="deliver",
    )(out, gin, gwq, gwo, gwh, gwd, both)


def gather_rows(rows):
    return lax.all_gather(rows, "tensor", axis=1, tiled=True)


def scatter_rows(part):
    return lax.psum_scatter(part, "tensor", scatter_dimension=1, tiled=True).astype(F32)


def shards(
    groups,
    ranks,
    block_input,
    key_mask,
    attn_norm_gain,
    attn_norm_bias,
    qkv_weight,
    qv_bias,
    out_weight,
    out_bias,
    mlp_norm_gain,
    mlp_norm_bias,
    hidden_weight,
    hidden_bias,
    down_weight,
    down_bias,
    grad_out,
):
    flat = ranks == 4
    images, rows, model = block_input.shape
    seq = key_mask.shape[1]
    width = qkv_weight.shape[2]
    units = hidden_weight.shape[1]

    def weight(shard):
        return lax.all_gather(shard, "dp", axis=0, tiled=True)

    def owned(grad):
        return lax.psum_scatter(grad.astype(BF16), "dp", scatter_dimension=0, tiled=True).astype(F32)

    out_rows, down_rows = out_weight.T, down_weight.T
    if flat:
        (
            normed_one, grad_full, normed_two, hidden_res, qh, kh, vh, mixed, qkv_all, out_all, hidden_all, down_all
        ) = front(
            groups,
            block_input,
            grad_out,
            key_mask,
            (attn_norm_gain, attn_norm_bias, out_bias, mlp_norm_gain, mlp_norm_bias),
            qv_bias,
            qkv_weight.transpose(1, 0, 2),
            out_rows,
            hidden_weight,
            down_rows,
        )
        hidden_full, grad_hidden, hidden_part, mpart, grad_down_w, mlp_sums, unit_sums = turn(
            groups, rows, normed_two, grad_full, hidden_all, down_all, hidden_res, grad_out, mlp_norm_gain, hidden_bias
        )
        held = (
            hidden_full, mixed, hidden_part, mpart, out_all, qh, kh, vh, qkv_all, hidden_res, grad_hidden, block_input
        )
        block_output, grad_input, grad_qkv_w, grad_out_w, grad_hidden_w, both = close(
            groups, rows, width // HD, held, normed_one, attn_norm_gain, down_bias, mlp_sums, unit_sums
        )
        (
            block_output, grad_input, grad_qkv_w, grad_out_w, grad_hidden_w, grad_down_w, grad_qv, grad_hidden_b, *both
        ) = deliver(
            width, units, block_output, grad_input, grad_qkv_w, grad_out_w, grad_hidden_w, grad_down_w, both
        )
        grad_qkv_w = grad_qkv_w.transpose(1, 0, 2)
        grad_out_w, grad_down_w = grad_out_w.T, grad_down_w.T
    else:
        qkv_rows = qkv_weight.reshape(-1, 3 * width)
        shift = jnp.concatenate([qv_bias[0], jnp.zeros_like(qv_bias[0]), qv_bias[1]])
        hidden_all, down_all = weight(hidden_weight), weight(down_rows)
        qkv_all, out_all = weight(qkv_rows), weight(out_rows)
        lens = jnp.sum(key_mask, axis=1)
        in_float = block_input.astype(F32)
        normed_one = gather_rows(norm_forward(in_float, attn_norm_gain, attn_norm_bias))
        grad_full = gather_rows(grad_out)
        proj = jnp.einsum("isd,df->isf", normed_one, qkv_all, preferred_element_type=F32) + shift
        proj = proj.astype(BF16)
        mixed = attend_forward(lens, proj)
        attn_part = jnp.einsum("isf,df->isd", mixed, out_all, preferred_element_type=F32).astype(BF16)
        hidden_res = in_float + scatter_rows(attn_part) + out_bias
        normed_two = gather_rows(norm_forward(hidden_res, mlp_norm_gain, mlp_norm_bias))
        pre_act = jnp.einsum("isd,df->isf", normed_two, hidden_all, preferred_element_type=F32) + hidden_bias
        value, slope = gelu_both(pre_act)
        activated = value.astype(BF16)
        grad_act = jnp.einsum("isd,df->isf", grad_full, down_all, preferred_element_type=F32)
        grad_pre = grad_act * slope
        grad_hidden_b = jnp.sum(grad_pre, axis=(0, 1))
        grad_pre_low = grad_pre.astype(BF16)
        gpart = jnp.einsum("isf,df->isd", grad_pre_low, hidden_all, preferred_element_type=F32).astype(BF16)
        mpart = jnp.einsum("isf,df->isd", activated, down_all, preferred_element_type=F32).astype(BF16)
        block_output = (hidden_res + scatter_rows(mpart) + down_bias).astype(BF16)
        grad_float = grad_out.astype(F32)
        grad_normed = scatter_rows(gpart)
        unit, inv_std = norm_stats(hidden_res)
        grad_hidden = grad_float + norm_backward(grad_normed, unit, inv_std, mlp_norm_gain)
        hidden_full = gather_rows(grad_hidden.astype(BF16))
        mlp_sums = jnp.stack(
            [jnp.sum(v, axis=(0, 1)) for v in (grad_normed * unit, grad_normed, grad_hidden, grad_float)]
        )
        grad_hidden_w = owned(jnp.einsum("isd,isf->df", normed_two, grad_pre_low, preferred_element_type=F32))
        grad_down_w = owned(jnp.einsum("isd,isf->df", grad_full, activated, preferred_element_type=F32)).T
        grad_mixed = jnp.einsum("isd,df->isf", hidden_full, out_all, preferred_element_type=F32).astype(BF16)
        grad_proj, proj_sums = attend_backward(lens, proj, grad_mixed)
        proj_sums = jnp.sum(proj_sums, axis=(0, 1))
        npart = jnp.einsum("isf,df->isd", grad_proj, qkv_all, preferred_element_type=F32).astype(BF16)
        grad_out_w = owned(jnp.einsum("isd,isf->df", hidden_full, mixed, preferred_element_type=F32)).T
        grad_qkv_w = owned(jnp.einsum("isd,isf->df", normed_one, grad_proj, preferred_element_type=F32))
        grad_normed = scatter_rows(npart)
        unit, inv_std = norm_stats(in_float)
        grad_input = grad_hidden + norm_backward(grad_normed, unit, inv_std, attn_norm_gain)
        attn_sums = jnp.stack([jnp.sum(v, axis=(0, 1)) for v in (grad_normed * unit, grad_normed)])
        both = lax.psum(jnp.concatenate([mlp_sums, attn_sums]), ("dp", "tensor"))
        proj_sums, grad_hidden_b = lax.psum((proj_sums, grad_hidden_b), "dp")
        grad_qv = jnp.stack([proj_sums[:width], proj_sums[2 * width :]])
        grad_qkv_w = grad_qkv_w.reshape(-1, 3, width)
    return (
        block_output,
        grad_input,
        both[4],
        both[5],
        grad_qkv_w,
        grad_qv,
        grad_out_w,
        both[2],
        both[0],
        both[1],
        grad_hidden_w,
        grad_hidden_b,
        grad_down_w,
        both[3],
    )


def solution(mesh):
    return jax.shard_map(
        functools.partial(shards, mesh.shape["dp"], mesh.shape["tensor"]),
        mesh=mesh,
        in_specs=(
            P("dp", "tensor", None),
            P("dp", None),
            P(),
            P(),
            P("dp", None, "tensor"),
            P(None, "tensor"),
            P("tensor", "dp"),
            P(),
            P(),
            P(),
            P("dp", "tensor"),
            P("tensor"),
            P("tensor", "dp"),
            P(),
            P("dp", "tensor", None),
        ),
        out_specs=(
            P("dp", "tensor", None),
            P("dp", "tensor", None),
            P(),
            P(),
            P("dp", None, "tensor"),
            P(None, "tensor"),
            P("tensor", "dp"),
            P(),
            P(),
            P(),
            P("dp", "tensor"),
            P("tensor"),
            P("tensor", "dp"),
            P(),
        ),
        check_vma=False,
    )
```

```python
import functools
import math

import jax
import jax.numpy as jnp
from jax import lax
from jax.experimental import pallas as pl
from jax.experimental.pallas import tpu as pltpu
from jax.sharding import PartitionSpec as P

HD = 72
CHUNK = 768
F32 = jnp.float32
BF16 = jnp.bfloat16
LOG2E = math.log2(math.e)
NN = (((1,), (0,)), ((), ()))
NT = (((1,), (1,)), ((), ()))
TN = (((0,), (0,)), ((), ()))
MESH = pl.DeviceIdType.MESH
ANY = pl.BlockSpec(memory_space=pl.ANY)
VMEM = pl.BlockSpec(memory_space=pltpu.VMEM)
SMEM = pl.BlockSpec(memory_space=pltpu.SMEM)


layer_eps = 1e-06
gelu_root = math.sqrt(2.0 / math.pi)
gelu_cubic = 0.044715


def norm_stats(rows):
    center = rows - jnp.mean(rows, axis=-1, keepdims=True)
    inv_std = lax.rsqrt(jnp.mean(center * center, axis=-1, keepdims=True) + layer_eps)
    return (center * inv_std, inv_std)


def norm_forward(rows, gain, shift):
    unit, _ = norm_stats(rows)
    return (unit * gain + shift).astype(BF16)


def norm_backward(grad_normed, unit, inv_std, gain):
    scaled = grad_normed * gain
    return inv_std * (
        scaled
        - jnp.mean(scaled, axis=-1, keepdims=True)
        - unit * jnp.mean(scaled * unit, axis=-1, keepdims=True)
    )


def gelu_both(pre):
    tangent = jnp.tanh(gelu_root * (pre + gelu_cubic * pre * pre * pre))
    value = 0.5 * pre * (1.0 + tangent)
    slope = 0.5 * (1.0 + tangent) + 0.5 * pre * (1.0 - tangent * tangent) * gelu_root * (
        1.0 + 3.0 * gelu_cubic * pre * pre
    )
    return (value, slope)


def dot(a, b, dims=NN):
    return lax.dot_general(a, b, dims, preferred_element_type=F32)


def soft_columns(keys_in, queries, row_ok, factor):
    raw = jnp.where(row_ok, dot(keys_in, queries, NT), -1e30)
    top = jnp.max(raw, axis=0, keepdims=True)
    grown = jnp.exp2((raw - top) * factor)
    total = jnp.sum(grown, axis=0, keepdims=True)
    return grown * (1.0 / total)


def attend_forward_body(seq, heads, lens_ref, proj_ref, mixed_ref, qh, kh, vh, oh):
    width = heads * HD
    padded = qh.shape[1]
    for h in range(heads):
        qh[h, :seq] = proj_ref[0, :, h * HD : (h + 1) * HD]
        qh[h, seq:] = jnp.zeros((padded - seq, HD), BF16)
        kh[h] = proj_ref[0, :, width + h * HD : width + (h + 1) * HD]
        vh[h] = proj_ref[0, :, 2 * width + h * HD : 2 * width + (h + 1) * HD].T
    length = lens_ref[pl.program_id(0)]
    factor = HD**-0.5 * LOG2E

    def head(h, _):
        def chunk(c, _):
            row_ok = lax.broadcasted_iota(jnp.int32, (seq, CHUNK), 0) < length
            at = pl.ds(pl.multiple_of(c * CHUNK, CHUNK), CHUNK)
            probs = soft_columns(kh[h], qh[h, at], row_ok, factor)
            oh[h, at] = dot(vh[h], probs.astype(BF16)).T.astype(BF16)
            return 0

        return lax.fori_loop(0, padded // CHUNK, chunk, 0)

    lax.fori_loop(0, heads, head, 0)
    for h in range(heads):
        mixed_ref[0, :, h * HD : (h + 1) * HD] = oh[h, :seq]


def attend_forward(lens, proj):
    images, seq, triple = proj.shape
    heads = triple // (3 * HD)
    padded = -(-seq // CHUNK) * CHUNK
    return pl.pallas_call(
        functools.partial(attend_forward_body, seq, heads),
        out_shape=jax.ShapeDtypeStruct((images, seq, heads * HD), BF16),
        grid=(images,),
        in_specs=[SMEM, pl.BlockSpec((1, seq, triple), lambda i: (i, 0, 0))],
        out_specs=pl.BlockSpec((1, seq, heads * HD), lambda i: (i, 0, 0)),
        scratch_shapes=[
            pltpu.VMEM((heads, padded, HD), BF16),
            pltpu.VMEM((heads, seq, HD), BF16),
            pltpu.VMEM((heads, HD, seq), BF16),
            pltpu.VMEM((heads, padded, HD), BF16),
        ],
        name="attend_forward",
    )(lens, proj)


def attend_backward_body(
    seq, heads, lens_ref, proj_ref, gmix_ref, gproj_ref, gbias_ref, qh, kh, kt, vh, gh, gq, gk, gv
):
    width = heads * HD
    padded = qh.shape[1]
    for h in range(heads):
        qh[h, :seq] = proj_ref[0, :, h * HD : (h + 1) * HD]
        qh[h, seq:] = jnp.zeros((padded - seq, HD), BF16)
        gh[h, :seq] = gmix_ref[0, :, h * HD : (h + 1) * HD]
        gh[h, seq:] = jnp.zeros((padded - seq, HD), BF16)
        keys_in = proj_ref[0, :, width + h * HD : width + (h + 1) * HD]
        kh[h] = keys_in
        kt[h] = keys_in.T
        vh[h] = proj_ref[0, :, 2 * width + h * HD : 2 * width + (h + 1) * HD]
    length = lens_ref[pl.program_id(0)]
    scale = HD**-0.5
    factor = scale * LOG2E

    def head(h, _):
        gk[h] = jnp.zeros((seq, HD), F32)
        gv[h] = jnp.zeros((seq, HD), F32)

        def chunk(c, _):
            row_ok = lax.broadcasted_iota(jnp.int32, (seq, CHUNK), 0) < length
            at = pl.ds(pl.multiple_of(c * CHUNK, CHUNK), CHUNK)
            queries = qh[h, at]
            grads = gh[h, at]
            probs = soft_columns(kh[h], queries, row_ok, factor)
            grad_probs = dot(vh[h], grads, NT)
            gv[h] += dot(probs.astype(BF16), grads)
            delta = jnp.sum(probs * grad_probs, axis=0, keepdims=True)
            grad_scores = (probs * (grad_probs - delta) * scale).astype(BF16)
            gk[h] += dot(grad_scores, queries)
            gq[h, at] = dot(kt[h], grad_scores).T
            return 0

        return lax.fori_loop(0, padded // CHUNK, chunk, 0)

    lax.fori_loop(0, heads, head, 0)
    for h in range(heads):
        for c, held in enumerate((gq, gk, gv)):
            value = held[h, :seq]
            at = slice(c * width + h * HD, c * width + (h + 1) * HD)
            gproj_ref[0, :, at] = value.astype(BF16)
            gbias_ref[0, :, at] = jnp.sum(value, axis=0, keepdims=True)


def attend_backward(lens, proj, gmix):
    images, seq, triple = proj.shape
    heads = triple // (3 * HD)
    padded = -(-seq // CHUNK) * CHUNK
    return pl.pallas_call(
        functools.partial(attend_backward_body, seq, heads),
        out_shape=(
            jax.ShapeDtypeStruct((images, seq, triple), BF16),
            jax.ShapeDtypeStruct((images, 1, triple), F32),
        ),
        grid=(images,),
        in_specs=[
            SMEM,
            pl.BlockSpec((1, seq, triple), lambda i: (i, 0, 0)),
            pl.BlockSpec((1, seq, heads * HD), lambda i: (i, 0, 0)),
        ],
        out_specs=(
            pl.BlockSpec((1, seq, triple), lambda i: (i, 0, 0)),
            pl.BlockSpec((1, 1, triple), lambda i: (i, 0, 0)),
        ),
        scratch_shapes=[
            pltpu.VMEM((heads, padded, HD), BF16),
            pltpu.VMEM((heads, seq, HD), BF16),
            pltpu.VMEM((heads, HD, seq), BF16),
            pltpu.VMEM((heads, seq, HD), BF16),
            pltpu.VMEM((heads, padded, HD), BF16),
            pltpu.VMEM((heads, padded, HD), F32),
            pltpu.VMEM((heads, seq, HD), F32),
            pltpu.VMEM((heads, seq, HD), F32),
        ],
        name="attend_backward",
    )(lens, proj, gmix)


def plane():
    me = lax.axis_index("tensor")
    side = me + 1 - 2 * lax.rem(me, 2)
    over = lax.rem(me + 2, 4)
    return (me, side, over, lax.rem(side + 2, 4))


def greet(peers):
    barrier = pltpu.get_barrier_semaphore()
    for peer in peers:
        pl.semaphore_signal(barrier, inc=1, device_id={"tensor": peer}, device_id_type=MESH)
    pl.semaphore_wait(barrier, len(peers))


def greet_both(groups, side, over):
    row = lax.axis_index("dp")
    barrier = pltpu.get_barrier_semaphore()
    peers = [{"tensor": side}, {"tensor": over}, {"dp": row + 1 - 2 * lax.rem(row, 2)}]
    peers += [{"dp": lax.rem(row + 2 * k, groups)} for k in range(1, groups // 2)]
    for peer in peers:
        pl.semaphore_signal(barrier, inc=1, device_id=peer, device_id_type=MESH)
    pl.semaphore_wait(barrier, len(peers))


def greet_all(groups):
    row, me = lax.axis_index("dp"), lax.axis_index("tensor")
    barrier = pltpu.get_barrier_semaphore()
    peers = [{"dp": lax.rem(row + k, groups)} for k in range(1, groups)]
    peers += [{"tensor": lax.rem(me + k, 4)} for k in range(1, 4)]
    for peer in peers:
        pl.semaphore_signal(barrier, inc=1, device_id=peer, device_id_type=MESH)
    pl.semaphore_wait(barrier, len(peers))


def remote(src, dst, send, recv, peer):
    return pltpu.make_async_remote_copy(
        src_ref=src,
        dst_ref=dst,
        send_sem=send,
        recv_sem=recv,
        device_id={"tensor": peer},
        device_id_type=MESH,
    )


def halves_of(rows):
    first = -(-rows // 32) * 16
    return (pl.ds(0, first), pl.ds(first, rows - first))


class Gather:
    def __init__(self, all_ref, rows, send, recv):
        me, side, over, _ = plane()
        low, high = halves_of(rows)
        plan = (
            (me, low, side),
            (me, high, over),
            (me, high, side),
            (me, low, over),
            (side, low, over),
            (over, high, side),
        )
        self.copies = []
        for k, (block, part, peer) in enumerate(plan):
            ref = all_ref.at[block, part]
            self.copies.append(remote(ref, ref, send.at[k], recv.at[k], peer))

    def start(self):
        for made in self.copies[:4]:
            made.start()

    def forward(self):
        for k in range(2):
            self.copies[k].wait_recv()
            self.copies[4 + k].start()

    def arrive(self):
        for made in self.copies[2:]:
            made.wait_recv()

    def finish(self):
        for made in self.copies:
            made.wait_send()


class Scatter:
    def __init__(self, part_ref, rows, near_ref, far_ref, pass_ref, send, recv):
        self.me, self.side, self.over, cross = plane()
        self.part_ref, self.near_ref, self.far_ref, self.pass_ref = part_ref, near_ref, far_ref, pass_ref
        self.halves = low, high = halves_of(rows)
        plan = (
            (part_ref.at[cross, low], near_ref.at[1, low], self.side),
            (part_ref.at[cross, high], near_ref.at[1, high], self.over),
            (part_ref.at[self.side, low], near_ref.at[0, low], self.side),
            (part_ref.at[self.over, high], near_ref.at[0, high], self.over),
            (pass_ref.at[low], far_ref.at[low], self.over),
            (pass_ref.at[high], far_ref.at[high], self.side),
        )
        self.copies = [remote(src, dst, send.at[k], recv.at[k], peer) for k, (src, dst, peer) in enumerate(plan)]

    def start(self):
        for made in self.copies[:4]:
            made.start()

    def forward(self):
        for k, (part, block) in enumerate(zip(self.halves, (self.over, self.side))):
            self.copies[k].wait_recv()
            mine = self.part_ref[block, part].astype(F32)
            self.pass_ref[part] = (mine + self.near_ref[1, part].astype(F32)).astype(BF16)
            self.copies[4 + k].start()

    def arrive(self):
        for made in self.copies[2:]:
            made.wait_recv()

    def total(self, rows):
        return (
            self.part_ref[self.me, rows].astype(F32)
            + self.near_ref[0, rows].astype(F32)
            + self.far_ref[rows].astype(F32)
        )

    def finish(self):
        for made in self.copies:
            made.wait_send()


STEPS = 6


def sems(*shape):
    return [pltpu.SemaphoreType.DMA(shape), pltpu.SemaphoreType.DMA(shape)]


def scatter_scratch(images, rows, width):
    return [
        pltpu.VMEM((images, 2, rows, width), BF16),
        pltpu.VMEM((images, rows, width), BF16),
        pltpu.VMEM((images, rows, width), BF16),
    ]


def params(cid):
    return pltpu.CompilerParams(collective_id=cid, has_side_effects=True, vmem_limit_bytes=67043328)


def lanes(width):
    return -(-width // 128) * 128


def pad_rows(rows):
    return -(-rows // 16) * 16


def clear_pads(ref, rows):
    full = ref.shape[1]
    for b in range(ref.shape[0]):
        ref[b, rows:full] = jnp.zeros((full - rows, ref.shape[2]), ref.dtype)


def at_row(ref):
    return ref[...].reshape(1, -1)


def for_image(i, images, act):
    for k in range(images):
        pl.when(i == k)(functools.partial(act, k))


def key_bias(mask, rows, full, seq):
    length = jnp.sum(mask.astype(F32), axis=1, keepdims=True).astype(jnp.int32)
    at = lax.broadcasted_iota(jnp.int32, (seq, 128 - HD), 0)
    lane = lax.broadcasted_iota(jnp.int32, (seq, 128 - HD), 1)
    block = sum((at >= b * full).astype(jnp.int32) for b in range(1, seq // full))
    inner = at - block * full
    good = (inner < rows) & (inner + block * rows < length)
    bias = jnp.where(good, 0.0, -1e30)
    ones = jnp.where(lane == 0, 1.0, 0.0)
    return (jnp.where(lane == 0, bias, 0.0).astype(BF16), ones.astype(BF16))


def soft_open(keys_in, queries, factor):
    raw = dot(keys_in, queries, NT)
    top = jnp.max(raw, axis=0, keepdims=True)
    grown = jnp.exp2((raw - top) * factor)
    total = jnp.sum(grown, axis=0, keepdims=True)
    return grown * (1.0 / total)


def over_dp(src, dst, send, recv, peer):
    return pltpu.make_async_remote_copy(
        src_ref=src, dst_ref=dst, send_sem=send, recv_sem=recv, device_id={"dp": peer}, device_id_type=MESH
    )


class Spread:
    def __init__(self, groups, all_ref, send, recv):
        row = lax.axis_index("dp")
        twin = row + 1 - 2 * lax.rem(row, 2)
        half = groups // 2
        chip = lax.div(row, 2)
        self.relayed = half == 4
        self.out, self.back = [], []
        for k in range(half):
            came = all_ref.at[lax.rem(row + groups - 2 * k, groups)]
            self.back.append(over_dp(came, came, send.at[half + k], recv.at[half + k], twin))
            if k > 0:
                mine = all_ref.at[row]
                self.out.append(over_dp(mine, mine, send.at[k], recv.at[k], lax.rem(row + 2 * k, groups)))
        self.asked = {}
        if self.relayed:
            self.asked = {0: chip != 3, 2: chip != 0}
            self.inner = (chip == 1) | (chip == 2)
            up = lax.div(chip, 2)
            came = all_ref.at[lax.rem(row + 4, groups)]
            self.relay = over_dp(came, came, send.at[0], recv.at[1 + 2 * up], row + 4 * up - 2)

    def where(self, k, act):
        if k in self.asked:
            pl.when(self.asked[k])(act)
        else:
            act()

    def start(self):
        for k in (1, 0, 2) if self.relayed else range(len(self.out)):
            self.where(k, self.out[k].start)
        self.back[0].start()

    def hop(self):
        if self.relayed:
            self.out[1].wait_recv()
            pl.when(self.inner)(self.relay.start)
            self.back[2].start()

    def forward(self):
        for k, (far, near) in enumerate(zip(self.out, self.back[1:])):
            if k != 1 or not self.relayed:
                far.wait_recv()
                near.start()

    def arrive(self):
        for made in self.back:
            made.wait_recv()

    def finish(self):
        for k, made in enumerate(self.out):
            self.where(k, made.wait_send)
        for made in self.back:
            made.wait_send()
        if self.relayed:
            pl.when(self.inner)(self.relay.wait_send)


class Moves:
    def __init__(self, sem):
        self.sem, self.made = sem, []

    def plan(self, src, dst):
        made = pltpu.make_async_copy(src, dst, self.sem.at[len(self.made)])
        self.made.append(made)
        return made

    def start(self, src, dst):
        made = self.plan(src, dst)
        made.start()
        return made

    def finish(self):
        for made in self.made:
            made.wait()


class Reduce:
    def __init__(self, groups, grad_ref, twin_ref, far_ref, tsend, trecv, fsend, frecv):
        self.grad_ref, self.twin_ref, self.far_ref = grad_ref, twin_ref, far_ref
        depth = grad_ref.shape[0] // groups
        rows = lambda block: pl.ds(pl.multiple_of(block * depth, 16), depth)
        row = lax.axis_index("dp")
        core = lax.rem(row, 2)
        self.slot, self.mine = lax.div(row, 2), rows(row)
        self.near, self.away = [], []
        for k in range(groups // 2):
            theirs = grad_ref.at[rows(2 * k + 1 - core)]
            self.near.append(over_dp(theirs, twin_ref.at[k], tsend.at[k], trecv.at[k], row + 1 - 2 * core))
        for k in range(1, groups // 2):
            peer = lax.rem(row + 2 * k, groups)
            slot = lax.div(peer, 2)
            made = over_dp(twin_ref.at[slot], far_ref.at[k - 1], fsend.at[k], frecv.at[k], peer)
            self.away.append((slot, rows(peer), made))

    def start(self):
        for made in self.near:
            made.start()

    def pair(self):
        for made in self.near:
            made.wait_recv()
        for slot, part, made in self.away:
            mine = self.grad_ref[part].astype(F32)
            self.twin_ref[slot] = (self.twin_ref[slot].astype(F32) + mine).astype(BF16)
            made.start()

    def total(self):
        value = self.twin_ref[self.slot].astype(F32) + self.grad_ref[self.mine].astype(F32)
        for k, (_, _, made) in enumerate(self.away):
            made.wait_recv()
            value = value + self.far_ref[k].astype(F32)
        return value

    def finish(self):
        for made in self.near + [made for _, _, made in self.away]:
            made.wait_send()


def reduce_scratch(groups, depth, width):
    half, width = groups // 2, lanes(width)
    return [pltpu.VMEM((half, depth, width), BF16), pltpu.VMEM((half - 1, depth, width), BF16)] + sems(half) * 2


def outer(out_ref, left_ref, right_ref, width):
    images, blocks, full, model = left_ref.shape
    count = images * blocks * full
    tile = 384
    if out_ref.shape[1] > width:
        out_ref[:, width:] = jnp.zeros_like(out_ref[:, width:])

    def part(c, _):
        at = pl.ds(pl.multiple_of(c * tile, tile), tile)
        left = left_ref[:, :, :, at].reshape(count, tile)
        right = right_ref[:, :, :, :width].reshape(count, width)
        out_ref[at, :width] = dot(left, right, TN).astype(BF16)
        return 0

    lax.fori_loop(0, model // tile, part, 0)


def main_body(
    groups, rows, heads,
    x_ref, grad_ref, mask_ref, gain_one, bias_one, bias_out, gain_two, bias_two, qv_ref, hb_ref,
    wq_ref, wo_ref, wh_ref, wd_ref,
    one_out, hidden_out, qh_out, kh_out, vh_out, mixed_out, wq_out, wo_out, glow_out, ghid_out, gwh_out, mpart_out,
    gwd_ref, sums_ref, hsum_ref,
    one_ref, full_ref, two_ref, hidden_ref, qh, kh, vh, mixed_ref, wq_all, wo_all, wh_all, wd_all,
    oh, part_ref, ghid_ref, act_ref, gpl_ref, gwh_part, gwd_part,
    near, far, passing, osem, twin, away, tsend, trecv, fsend, frecv,
    asend, arecv, csend, crecv, ssend, srecv, gsend, grecv, usend, urecv, vsend, vrecv, wsend, wrecv,
):
    images = x_ref.shape[0]
    _, _, full, model = one_ref.shape
    units = hb_ref.shape[0]
    seq = 4 * full
    width = heads * HD
    me, side, over, _ = plane()
    mine = lax.axis_index("dp")
    wq_all[mine, :, 3 * width :] = jnp.zeros_like(wq_all[mine, :, 3 * width :])
    for c in range(3):
        wq_all[mine, :, c * width : (c + 1) * width] = wq_ref[c]
    weights = [Spread(groups, wq_all, wsend.at[0], wrecv.at[0])]
    for k, (own, everyone) in enumerate(((wo_ref, wo_all), (wh_ref, wh_all), (wd_ref, wd_all))):
        count = own.shape[1]
        everyone[mine, :, count:] = jnp.zeros_like(everyone[mine, :, count:])
        everyone[mine, :, :count] = own[...]
        weights.append(Spread(groups, everyone, wsend.at[k + 1], wrecv.at[k + 1]))
    wq, wo, wh, wd = weights
    ones, sums, twos, grads, turns, lows = [], [], [], [], [], []
    for i in range(images):
        for ref in (one_ref, two_ref, full_ref):
            clear_pads(ref.at[i], rows)
        slots = (near.at[i], far.at[i], passing.at[i])
        ones.append(Gather(one_ref.at[i], rows, asend.at[i], arecv.at[i]))
        grads.append(Gather(full_ref.at[i], rows, csend.at[i], crecv.at[i]))
        sums.append(Scatter(part_ref.at[i], rows, *slots, ssend.at[i], srecv.at[i]))
        twos.append(Gather(two_ref.at[i], rows, gsend.at[i], grecv.at[i]))
        turns.append(Scatter(part_ref.at[i], rows, *slots, usend.at[i], urecv.at[i]))
        if i < images - 1:
            lows.append(Gather(one_ref.at[i], rows, vsend.at[i], vrecv.at[i]))
    down = Reduce(groups, gwd_part, twin, away, tsend, trecv, fsend, frecv)
    stores = Moves(osem)
    put_wq, put_wo, put_gwh = [
        stores.plan(a, b) for a, b in ((wq_all, wq_out), (wo_all, wo_out), (gwh_part, gwh_out))
    ]
    pairs = (
        (one_ref, one_out), (hidden_ref, hidden_out), (qh, qh_out), (kh, kh_out), (vh, vh_out), (mixed_ref, mixed_out),
        (two_ref, mpart_out), (ghid_ref, ghid_out),
    )
    put = [[stores.plan(a.at[i], b.at[i]) for a, b in pairs] for i in range(images)]
    put_low = [stores.plan(one_ref.at[i], glow_out.at[i]) for i in range(images - 1)]

    def enter(i):
        one_ref[i, me, :rows] = norm_forward(x_ref[i].astype(F32), at_row(gain_one), at_row(bias_one))

    enter(0)
    greet_both(groups, side, over)
    ones[0].start()
    wq.start()
    for i in range(1, images):
        enter(i)
        ones[i].start()
    for step in (wo, wh, wd):
        step.start()
    mixed_ref[:, :, :, width:] = jnp.zeros_like(mixed_ref[:, :, :, width:])
    hsum_ref[...] = jnp.zeros_like(hsum_ref)
    for i in range(images):
        full_ref[i, me, :rows] = grad_ref[i]
        bias, tail = key_bias(mask_ref[i : i + 1], rows, full, seq)
        for h in range(heads):
            kh[i, h, :, HD:] = bias
            vh[i, h, :, HD:] = jnp.zeros_like(bias)
            qh[i, h, :, HD:] = tail
    for step in ones:
        step.forward()
    grads[0].start()
    wq.hop()
    wq.forward()
    factor = HD**-0.5 * LOG2E
    shift_q, shift_v = qv_ref[0:1], qv_ref[1:2]

    def project(i):
        weight = wq_all[:, :, : 3 * width].reshape(-1, 3 * width)

        def block(b, _):
            at = pl.ds(pl.multiple_of(b * full, 16), full)
            value = dot(one_ref[i, b], weight)
            queries = (value[:, :width] + shift_q).astype(BF16)
            keys_in = value[:, width : 2 * width].astype(BF16)
            values = (value[:, 2 * width :] + shift_v).astype(BF16)
            for h in range(heads):
                here = slice(h * HD, (h + 1) * HD)
                qh[i, h, at, :HD] = queries[:, here]
                kh[i, h, at, :HD] = keys_in[:, here]
                vh[i, h, at, :HD] = values[:, here]
            return 0

        lax.fori_loop(0, 4, block, 0)

    def attend(i):
        def head(h, _):
            probs = soft_open(kh[i, h], qh[i, h], factor)
            oh[h] = dot(vh[i, h, :, :HD].T, probs.astype(BF16)).T.astype(BF16)
            return 0

        lax.fori_loop(0, heads, head, 0, unroll=2)
        for h in range(heads):
            for b in range(4):
                mixed_ref[i, b, :, h * HD : (h + 1) * HD] = oh[h, b * full : (b + 1) * full]

    def combine(i):
        weight = wo_all[:, :, :width].reshape(-1, width)

        def block(b, _):
            part_ref[i, b] = dot(mixed_ref[i, b, :, :width], weight, NT).astype(BF16)
            return 0

        lax.fori_loop(0, 4, block, 0)

    def ready(k):
        ones[k].arrive()
        put[k][0].start()
        if k == 0:
            wq.arrive()
            put_wq.start()

    def between(k):
        for made in put[k][2:6]:
            made.start()
        if k == 0:
            grads[0].forward()
            wo.hop()
            wo.forward()
            wh.hop()
            wo.arrive()
            put_wo.start()

    def send(k):
        if k > 0:
            sums[k - 1].forward()
        sums[k].start()

    def image(i, _):
        for_image(i, images, ready)
        project(i)
        attend(i)
        for_image(i, images, between)
        combine(i)
        for_image(i, images, send)
        return 0

    lax.fori_loop(0, images, image, 0)

    def settle(i):
        sums[i].arrive()
        hidden = x_ref[i].astype(F32) + sums[i].total(pl.ds(0, rows)) + at_row(bias_out)
        hidden_ref[i] = hidden
        two_ref[i, me, :rows] = norm_forward(hidden, at_row(gain_two), at_row(bias_two))
        twos[i].start()
        put[i][1].start()

    for i in range(images - 1):
        settle(i)
    sums[-1].forward()
    wd.hop()
    for i in range(images - 1):
        twos[i].forward()
    settle(images - 1)
    for step in grads[1:]:
        step.start()
    wh.forward()
    wd.forward()
    twos[-1].forward()
    for step in sums + ones:
        step.finish()
    for i in range(images):
        put[i][0].wait()
    wide = lambda ref: ref[:, :, :units].reshape(model, units)
    shift = at_row(hb_ref)

    def ascend(i):
        def pair(c, _):
            at = pl.ds(2 * c, 2)
            pre = dot(two_ref[i, at].reshape(2 * full, model), wide(wh_all)) + shift
            value, slope = gelu_both(pre)
            act_ref[i, at] = value.astype(BF16).reshape(2, full, units)
            grad_pre = dot(full_ref[i, at].reshape(2 * full, model), wide(wd_all)) * slope
            hsum_ref[...] += jnp.sum(grad_pre, axis=0, keepdims=True)
            low = grad_pre.astype(BF16)
            gpl_ref[i, at] = low.reshape(2, full, units)
            part_ref[i, at] = dot(low, wide(wh_all), NT).astype(BF16).reshape(2, full, model)
            return 0

        lax.fori_loop(0, 2, pair, 0)

    def descend(k, _):
        at = pl.ds(2 * lax.rem(k, 2), 2)
        i = lax.div(k, 2)
        part = dot(act_ref[i, at].reshape(2 * full, units), wide(wd_all), NT)
        two_ref[i, at] = part.astype(BF16).reshape(2, full, model)
        return 0

    totals = [0.0, 0.0, 0.0, 0.0]

    def settle_back(i):
        turns[i].arrive()
        grad_normed = turns[i].total(pl.ds(0, rows))
        unit, inv_std = norm_stats(hidden_ref[i])
        upper = full_ref[i, me, :rows].astype(F32)
        grad_hidden = upper + norm_backward(grad_normed, unit, inv_std, at_row(gain_two))
        ghid_ref[i] = grad_hidden
        put[i][7].start()
        if i < images - 1:
            one_ref[i, me, :rows] = grad_hidden.astype(BF16)
            lows[i].start()
        for k, term in enumerate((grad_normed * unit, grad_normed, grad_hidden, upper)):
            totals[k] = totals[k] + jnp.sum(term, axis=0, keepdims=True)

    def ready_back(k):
        twos[k].arrive()
        if k == 0:
            wh.arrive()
            wd.arrive()
        grads[k].arrive()

    def send_back(k):
        if k == 0:
            for step in grads[1:]:
                step.forward()
        if k > 0:
            turns[k - 1].forward()
        turns[k].start()

    def image_back(i, _):
        for_image(i, images, ready_back)
        ascend(i)
        for_image(i, images, send_back)
        return 0

    lax.fori_loop(0, images, image_back, 0)
    outer(gwd_part, full_ref, act_ref, units)
    down.start()
    for i in range(images - 1):
        settle_back(i)
    turns[-1].forward()
    down.pair()
    outer(gwh_part, two_ref, gpl_ref, units)
    put_gwh.start()
    for step in lows:
        step.forward()
    settle_back(images - 1)
    for step in twos:
        step.finish()
    lax.fori_loop(0, 2 * images, descend, 0)
    for i in range(images):
        put[i][6].start()
    for k in range(4):
        sums_ref[k : k + 1] = totals[k]
    gwd_ref[...] = down.total()[:, :units]
    for step, made in zip(lows, put_low):
        step.arrive()
        made.start()
    for step in turns + lows + grads + weights + [down]:
        step.finish()
    for i in range(images):
        for made in put[i][1:]:
            made.wait()
    for made in put_low + [put_wq, put_wo, put_gwh]:
        made.wait()


def main(groups, block_input, grad_out, key_mask, vectors, qv_bias, bias, wq, wo, wh, wd):
    images, rows, model = block_input.shape
    full = pad_rows(rows)
    width = wo.shape[1]
    units = wh.shape[1]
    heads = width // HD
    seq = 4 * full
    depth = wo.shape[0]
    blocks = ((images, 4, full, model), BF16)
    own = ((images, rows, model), F32)
    heads_wide = ((images, heads, seq, 128), BF16)
    mixed = ((images, 4, full, lanes(width)), BF16)
    wide = ((images, 4, full, units), BF16)
    square = ((model, lanes(units)), BF16)
    weight = lambda count: ((groups, depth, lanes(count)), BF16)
    outs = [
        blocks, own, heads_wide, heads_wide, heads_wide, mixed, weight(3 * width), weight(width),
        ((images - 1, 4, full, model), BF16), own, square, blocks,
    ]
    more = [((depth, units), F32), ((4, model), F32), ((1, units), F32)]
    held = [blocks, blocks, blocks, own, heads_wide, heads_wide, heads_wide, mixed]
    held += [weight(3 * width), weight(width), weight(units), weight(units)]
    held += [((heads, seq, HD), BF16), blocks, own, wide, wide, square, square]
    return pl.pallas_call(
        functools.partial(main_body, groups, rows, heads),
        out_shape=tuple(jax.ShapeDtypeStruct(*h) for h in outs + more),
        in_specs=[VMEM] * 14,
        out_specs=(ANY,) * len(outs) + (VMEM,) * len(more),
        scratch_shapes=[pltpu.VMEM(*h) for h in held]
        + scatter_scratch(images, full, model)
        + [pltpu.SemaphoreType.DMA((9 * images + 3,))]
        + reduce_scratch(groups, depth, units)
        + sems(images, STEPS) * 6
        + sems(4, groups),
        compiler_params=params(0),
        name="main",
    )(block_input, grad_out, key_mask, *vectors, qv_bias, bias, wq, wo, wh, wd)


def close_body(
    groups, rows, heads,
    glow_hbm, mixed_hbm, gwh_hbm, mpart_hbm, wo_hbm, qh_hbm, kh_hbm, vh_hbm, wq_hbm, hidden_hbm, ghid_hbm, x_hbm, one_hbm,
    gain_ref, bias_ref, tsum_ref, hsum_ref,
    out_ref, gin_ref, gwq_ref, gwo_ref, gwh_ref, both_ref,
    tok, mixed_ref, gwh_part, mpart_ref, wo_ref, qh, kh, vh, wq_ref, hidden_ref, ghid_ref, x_ref,
    gq, gk, gv, gh, bsum, gproj, npart, gwq_part, gwo_part, lsem,
    near, far, passing, near2, far2, passing2,
    htwin, haway, htsend, htrecv, hfsend, hfrecv,
    otwin, oaway, otsend, otrecv, ofsend, ofrecv,
    qtwin, qaway, qtsend, qtrecv, qfsend, qfrecv,
    mid, msend, mrecv, ssend, srecv, lsend, lrecv, vsend, vrecv, row_in, flat_in,
):
    images, _, full, model = tok.shape
    width = heads * HD
    seq = 4 * full
    me, side, over, _ = plane()
    mine = lax.axis_index("dp")
    loads = Moves(lsem)
    held = (
        (ghid_hbm.at[images - 1], ghid_ref.at[images - 1]), (glow_hbm, tok.at[pl.ds(0, images - 1)]), (wo_hbm, wo_ref),
        (gwh_hbm, gwh_part), (mpart_hbm, mpart_ref), (qh_hbm, qh), (kh_hbm, kh), (vh_hbm, vh), (mixed_hbm, mixed_ref),
        (wq_hbm, wq_ref), (hidden_hbm, hidden_ref), (x_hbm, x_ref),
        (ghid_hbm.at[pl.ds(0, images - 1)], ghid_ref.at[pl.ds(0, images - 1)]),
    )
    got = [loads.start(src, dst) for src, dst in held]
    got_one = loads.plan(one_hbm, tok)
    bsum[...] = jnp.zeros_like(bsum)
    outs, sums = [], []
    for i in range(images):
        outs.append(Scatter(mpart_ref.at[i], rows, near2.at[i], far2.at[i], passing2.at[i], msend.at[i], mrecv.at[i]))
        sums.append(Scatter(npart.at[i], rows, near.at[i], far.at[i], passing.at[i], ssend.at[i], srecv.at[i]))
    red_h = Reduce(groups, gwh_part, htwin, haway, htsend, htrecv, hfsend, hfrecv)
    red_o = Reduce(groups, gwo_part, otwin, oaway, otsend, otrecv, ofsend, ofrecv)
    red_q = Reduce(groups, gwq_part, qtwin, qaway, qtsend, qtrecv, qfsend, qfrecv)
    last = images - 1
    clear_pads(tok.at[last], rows)
    low = Gather(tok.at[last], rows, lsend, lrecv)
    got[0].wait()
    tok[last, me, :rows] = ghid_ref[last].astype(BF16)
    greet_all(groups)
    low.start()
    for made in got[1:5]:
        made.wait()
    red_h.start()
    for step in outs[:-1]:
        step.start()

    def mix(i):
        value = dot(tok[i].reshape(seq, model), wo_ref[:, :, :width].reshape(model, width)).astype(BF16)
        for h in range(heads):
            gh[i, h] = value[:, h * HD : (h + 1) * HD]

    for i in range(last):
        mix(i)
    low.forward()
    red_h.pair()
    for made in got[5:]:
        made.wait()
    scale = HD**-0.5

    def attend(i):
        def head(h, _):
            queries = qh[i, h]
            grads = gh[i, h]
            keys_in = kh[i, h]
            probs = soft_open(keys_in, queries, scale * LOG2E)
            grad_probs = dot(vh[i, h, :, :HD], grads, NT)
            grad_values = dot(probs.astype(BF16), grads)
            delta = jnp.sum(probs * grad_probs, axis=0, keepdims=True)
            grad_scores = (probs * (grad_probs - delta) * scale).astype(BF16)
            grad_keys = dot(grad_scores, queries[:, :HD])
            grad_queries = dot(keys_in[:, :HD].T, grad_scores).T
            for c, (held, value) in enumerate(((gq, grad_queries), (gk, grad_keys), (gv, grad_values))):
                held[h] = value.astype(BF16)
                bsum[h, c : c + 1] += jnp.sum(value, axis=0, keepdims=True)
            return 0

        lax.fori_loop(0, heads, head, 0, unroll=4)
        for h in range(heads):
            for c, held in enumerate((gq, gk, gv)):
                at = slice(c * width + h * HD, c * width + (h + 1) * HD)
                for b in range(4):
                    gproj[i, b, :, at] = held[h, b * full : (b + 1) * full]

    def spread(i):
        def pair(c, _):
            at = pl.ds(2 * c, 2)
            part = dot(gproj[i, at].reshape(2 * full, 3 * width), wq_ref[:, :, : 3 * width].reshape(model, 3 * width), NT)
            npart[i, at] = part.astype(BF16).reshape(2, full, model)
            return 0

        lax.fori_loop(0, 2, pair, 0)

    def between(k):
        if k == 0:
            for step in outs[:-1]:
                step.forward()

    def send(k):
        if k > 0:
            sums[k - 1].forward()
        sums[k].start()
        if k == images - 2:
            low.arrive()
            mix(last)
            outer(gwo_part, tok, mixed_ref, width)
            red_o.start()
            low.finish()
            got_one.start()

    def image(i, _):
        attend(i)
        for_image(i, images, between)
        spread(i)
        for_image(i, images, send)
        return 0

    lax.fori_loop(0, images, image, 0)
    red_o.pair()
    got_one.wait()
    outer(gwq_part, tok, gproj, 3 * width)
    red_q.start()
    totals = [0.0, 0.0]

    def settle(i):
        sums[i].arrive()
        grad_normed = sums[i].total(pl.ds(0, rows))
        unit, inv_std = norm_stats(x_ref[i].astype(F32))
        gin_ref[i] = ghid_ref[i] + norm_backward(grad_normed, unit, inv_std, at_row(gain_ref))
        for k, term in enumerate((grad_normed * unit, grad_normed)):
            totals[k] = totals[k] + jnp.sum(term, axis=0, keepdims=True)

    for i in range(images - 1):
        settle(i)
    red_q.pair()
    sums[-1].forward()
    outs[-1].start()

    def finish_out(i):
        outs[i].arrive()
        out_ref[i] = (hidden_ref[i] + outs[i].total(pl.ds(0, rows)) + at_row(bias_ref)).astype(BF16)

    for i in range(images - 1):
        finish_out(i)
    gwh_ref[...] = red_h.total()[:, : gwh_ref.shape[1]]
    gwo_ref[...] = red_o.total()[:, :width]
    mid[0] = jnp.zeros_like(mid[0])
    mid[0, 0:4] = tsum_ref[...]
    for h in range(heads):
        for c in range(3):
            mid[0, 6:7, c * width + h * HD : c * width + (h + 1) * HD] = bsum[h, c : c + 1]
    mid[0, 7:8, : hsum_ref.shape[1]] = hsum_ref[...]
    settle(images - 1)

    for k in range(2):
        mid[0, 4 + k : 5 + k] = totals[k]
    row_in[mine] = mid[0]
    aways = []
    for k in range(1, groups):
        aways.append(over_dp(mid.at[0], row_in.at[mine], vsend.at[k], vrecv.at[k], lax.rem(mine + k, groups)))
        aways[-1].start()
    outs[-1].forward()
    for made in aways:
        made.wait()
    held = row_in[0]
    for k in range(1, groups):
        held = held + row_in[k]
    mid[1] = held
    flat_in[me] = mid[1]
    planes = []
    for k in range(1, 4):
        at = groups + k
        planes.append(remote(mid.at[1], flat_in.at[me], vsend.at[at], vrecv.at[at], lax.rem(me + k, 4)))
        planes[-1].start()
    for made in planes:
        made.wait()
    both_ref[0:6] = (flat_in[0] + flat_in[1] + flat_in[2] + flat_in[3])[0:6]
    both_ref[6:8] = mid[1, 6:8]
    finish_out(images - 1)
    total = red_q.total()
    for c in range(3):
        gwq_ref[c] = total[:, c * width : (c + 1) * width]
    for step in sums + outs + [red_h, red_o, red_q]:
        step.finish()


def close(groups, rows, heads, held, one, gain, bias, tsum, hsum):
    images, _, full, model = one.shape
    width = heads * HD
    units = hsum.shape[1]
    depth = model // groups
    seq = 4 * full
    piece = pltpu.VMEM((heads, seq, HD), BF16)
    return pl.pallas_call(
        functools.partial(close_body, groups, rows, heads),
        out_shape=(
            jax.ShapeDtypeStruct((images, rows, model), BF16),
            jax.ShapeDtypeStruct((images, rows, model), F32),
            jax.ShapeDtypeStruct((3, depth, width), F32),
            jax.ShapeDtypeStruct((depth, width), F32),
            jax.ShapeDtypeStruct((depth, units), F32),
            jax.ShapeDtypeStruct((8, model), F32),
        ),
        in_specs=[ANY] * 13 + [VMEM] * 4,
        out_specs=(VMEM,) * 6,
        scratch_shapes=[pltpu.VMEM(h.shape, h.dtype) for h in (one,) + held[1:]]
        + [piece] * 3
        + [
            pltpu.VMEM((images, heads, seq, HD), BF16),
            pltpu.VMEM((heads, 3, HD), F32),
            pltpu.VMEM((images, 4, full, 3 * width), BF16),
            pltpu.VMEM((images, 4, full, model), BF16),
            pltpu.VMEM((model, lanes(3 * width)), BF16),
            pltpu.VMEM((model, lanes(width)), BF16),
            pltpu.SemaphoreType.DMA((14,)),
        ]
        + scatter_scratch(images, full, model) * 2
        + reduce_scratch(groups, depth, units)
        + reduce_scratch(groups, depth, width)
        + reduce_scratch(groups, depth, 3 * width)
        + [pltpu.VMEM((2, 8, model), F32)]
        + sems(images, STEPS) * 2
        + sems(STEPS)
        + sems(groups + 4)
        + [pltpu.VMEM((groups, 8, model), F32), pltpu.VMEM((4, 8, model), F32)],
        compiler_params=params(2),
        name="close",
    )(*held, one, gain, bias, tsum, hsum)


def deliver_body(width, out, gin, gwq, gwo, gwh, gwd, both, *refs):
    refs, sem = refs[:-1], refs[-1]
    loads = Moves(sem)
    for src, dst in zip((out, gin, gwq, gwo, gwh, gwd), refs):
        loads.start(src, dst)
    qv, unit = refs[6:8]
    qv[0:1] = both[6:7, :width]
    qv[1:2] = both[6:7, 2 * width : 3 * width]
    unit[...] = both[7, : unit.shape[0]]
    for k, dst in enumerate(refs[8:]):
        dst[...] = both[k]
    loads.finish()


def deliver(width, units, out, gin, gwq, gwo, gwh, gwd, both):
    model = both.shape[1]
    same = [jax.ShapeDtypeStruct(v.shape, v.dtype) for v in (out, gin, gwq, gwo, gwh, gwd)]
    more = [jax.ShapeDtypeStruct(dims, F32) for dims in ((2, width), (units,)) + ((model,),) * 6]
    return pl.pallas_call(
        functools.partial(deliver_body, width),
        out_shape=tuple(same + more),
        in_specs=[ANY] * 6 + [VMEM],
        out_specs=(VMEM,) * 14,
        scratch_shapes=[pltpu.SemaphoreType.DMA((6,))],
        compiler_params=pltpu.CompilerParams(vmem_limit_bytes=60 << 20),
        name="deliver",
    )(out, gin, gwq, gwo, gwh, gwd, both)


def gather_rows(rows):
    return lax.all_gather(rows, "tensor", axis=1, tiled=True)


def scatter_rows(part):
    return lax.psum_scatter(part, "tensor", scatter_dimension=1, tiled=True).astype(F32)


def shards(
    groups,
    ranks,
    block_input,
    key_mask,
    attn_norm_gain,
    attn_norm_bias,
    qkv_weight,
    qv_bias,
    out_weight,
    out_bias,
    mlp_norm_gain,
    mlp_norm_bias,
    hidden_weight,
    hidden_bias,
    down_weight,
    down_bias,
    grad_out,
):
    flat = ranks == 4
    images, rows, model = block_input.shape
    seq = key_mask.shape[1]
    width = qkv_weight.shape[2]
    units = hidden_weight.shape[1]

    def weight(shard):
        return lax.all_gather(shard, "dp", axis=0, tiled=True)

    def owned(grad):
        return lax.psum_scatter(grad.astype(BF16), "dp", scatter_dimension=0, tiled=True).astype(F32)

    out_rows, down_rows = out_weight.T, down_weight.T
    if flat:
        (
            normed_one, hidden_res, qh, kh, vh, mixed, qkv_all, out_all, hidden_full, grad_hidden, hidden_part, mpart,
            grad_down_w, mlp_sums, unit_sums,
        ) = main(
            groups,
            block_input,
            grad_out,
            key_mask,
            (attn_norm_gain, attn_norm_bias, out_bias, mlp_norm_gain, mlp_norm_bias),
            qv_bias,
            hidden_bias,
            qkv_weight.transpose(1, 0, 2),
            out_rows,
            hidden_weight,
            down_rows,
        )
        held = (
            hidden_full, mixed, hidden_part, mpart, out_all, qh, kh, vh, qkv_all, hidden_res, grad_hidden, block_input
        )
        block_output, grad_input, grad_qkv_w, grad_out_w, grad_hidden_w, both = close(
            groups, rows, width // HD, held, normed_one, attn_norm_gain, down_bias, mlp_sums, unit_sums
        )
        (
            block_output, grad_input, grad_qkv_w, grad_out_w, grad_hidden_w, grad_down_w, grad_qv, grad_hidden_b, *both
        ) = deliver(
            width, units, block_output, grad_input, grad_qkv_w, grad_out_w, grad_hidden_w, grad_down_w, both
        )
        grad_qkv_w = grad_qkv_w.transpose(1, 0, 2)
        grad_out_w, grad_down_w = grad_out_w.T, grad_down_w.T
    else:
        qkv_rows = qkv_weight.reshape(-1, 3 * width)
        shift = jnp.concatenate([qv_bias[0], jnp.zeros_like(qv_bias[0]), qv_bias[1]])
        hidden_all, down_all = weight(hidden_weight), weight(down_rows)
        qkv_all, out_all = weight(qkv_rows), weight(out_rows)
        lens = jnp.sum(key_mask, axis=1)
        in_float = block_input.astype(F32)
        normed_one = gather_rows(norm_forward(in_float, attn_norm_gain, attn_norm_bias))
        grad_full = gather_rows(grad_out)
        proj = jnp.einsum("isd,df->isf", normed_one, qkv_all, preferred_element_type=F32) + shift
        proj = proj.astype(BF16)
        mixed = attend_forward(lens, proj)
        attn_part = jnp.einsum("isf,df->isd", mixed, out_all, preferred_element_type=F32).astype(BF16)
        hidden_res = in_float + scatter_rows(attn_part) + out_bias
        normed_two = gather_rows(norm_forward(hidden_res, mlp_norm_gain, mlp_norm_bias))
        pre_act = jnp.einsum("isd,df->isf", normed_two, hidden_all, preferred_element_type=F32) + hidden_bias
        value, slope = gelu_both(pre_act)
        activated = value.astype(BF16)
        grad_act = jnp.einsum("isd,df->isf", grad_full, down_all, preferred_element_type=F32)
        grad_pre = grad_act * slope
        grad_hidden_b = jnp.sum(grad_pre, axis=(0, 1))
        grad_pre_low = grad_pre.astype(BF16)
        gpart = jnp.einsum("isf,df->isd", grad_pre_low, hidden_all, preferred_element_type=F32).astype(BF16)
        mpart = jnp.einsum("isf,df->isd", activated, down_all, preferred_element_type=F32).astype(BF16)
        block_output = (hidden_res + scatter_rows(mpart) + down_bias).astype(BF16)
        grad_float = grad_out.astype(F32)
        grad_normed = scatter_rows(gpart)
        unit, inv_std = norm_stats(hidden_res)
        grad_hidden = grad_float + norm_backward(grad_normed, unit, inv_std, mlp_norm_gain)
        hidden_full = gather_rows(grad_hidden.astype(BF16))
        mlp_sums = jnp.stack(
            [jnp.sum(v, axis=(0, 1)) for v in (grad_normed * unit, grad_normed, grad_hidden, grad_float)]
        )
        grad_hidden_w = owned(jnp.einsum("isd,isf->df", normed_two, grad_pre_low, preferred_element_type=F32))
        grad_down_w = owned(jnp.einsum("isd,isf->df", grad_full, activated, preferred_element_type=F32)).T
        grad_mixed = jnp.einsum("isd,df->isf", hidden_full, out_all, preferred_element_type=F32).astype(BF16)
        grad_proj, proj_sums = attend_backward(lens, proj, grad_mixed)
        proj_sums = jnp.sum(proj_sums, axis=(0, 1))
        npart = jnp.einsum("isf,df->isd", grad_proj, qkv_all, preferred_element_type=F32).astype(BF16)
        grad_out_w = owned(jnp.einsum("isd,isf->df", hidden_full, mixed, preferred_element_type=F32)).T
        grad_qkv_w = owned(jnp.einsum("isd,isf->df", normed_one, grad_proj, preferred_element_type=F32))
        grad_normed = scatter_rows(npart)
        unit, inv_std = norm_stats(in_float)
        grad_input = grad_hidden + norm_backward(grad_normed, unit, inv_std, attn_norm_gain)
        attn_sums = jnp.stack([jnp.sum(v, axis=(0, 1)) for v in (grad_normed * unit, grad_normed)])
        both = lax.psum(jnp.concatenate([mlp_sums, attn_sums]), ("dp", "tensor"))
        proj_sums, grad_hidden_b = lax.psum((proj_sums, grad_hidden_b), "dp")
        grad_qv = jnp.stack([proj_sums[:width], proj_sums[2 * width :]])
        grad_qkv_w = grad_qkv_w.reshape(-1, 3, width)
    return (
        block_output,
        grad_input,
        both[4],
        both[5],
        grad_qkv_w,
        grad_qv,
        grad_out_w,
        both[2],
        both[0],
        both[1],
        grad_hidden_w,
        grad_hidden_b,
        grad_down_w,
        both[3],
    )


def solution(mesh):
    return jax.shard_map(
        functools.partial(shards, mesh.shape["dp"], mesh.shape["tensor"]),
        mesh=mesh,
        in_specs=(
            P("dp", "tensor", None),
            P("dp", None),
            P(),
            P(),
            P("dp", None, "tensor"),
            P(None, "tensor"),
            P("tensor", "dp"),
            P(),
            P(),
            P(),
            P("dp", "tensor"),
            P("tensor"),
            P("tensor", "dp"),
            P(),
            P("dp", "tensor", None),
        ),
        out_specs=(
            P("dp", "tensor", None),
            P("dp", "tensor", None),
            P(),
            P(),
            P("dp", None, "tensor"),
            P(None, "tensor"),
            P("tensor", "dp"),
            P(),
            P(),
            P(),
            P("dp", "tensor"),
            P("tensor"),
            P("tensor", "dp"),
            P(),
        ),
        check_vma=False,
    )
```

```python
import functools
import math

import jax
import jax.numpy as jnp
from jax import lax
from jax.experimental import pallas as pl
from jax.experimental.pallas import tpu as pltpu
from jax.sharding import PartitionSpec as P

HD = 72
CHUNK = 768
F32 = jnp.float32
BF16 = jnp.bfloat16
LOG2E = math.log2(math.e)
NN = (((1,), (0,)), ((), ()))
NT = (((1,), (1,)), ((), ()))
TN = (((0,), (0,)), ((), ()))
MESH = pl.DeviceIdType.MESH
ANY = pl.BlockSpec(memory_space=pl.ANY)
VMEM = pl.BlockSpec(memory_space=pltpu.VMEM)
SMEM = pl.BlockSpec(memory_space=pltpu.SMEM)


layer_eps = 1e-06
gelu_root = math.sqrt(2.0 / math.pi)
gelu_cubic = 0.044715


def norm_stats(rows):
    center = rows - jnp.mean(rows, axis=-1, keepdims=True)
    inv_std = lax.rsqrt(jnp.mean(center * center, axis=-1, keepdims=True) + layer_eps)
    return (center * inv_std, inv_std)


def norm_forward(rows, gain, shift):
    unit, _ = norm_stats(rows)
    return (unit * gain + shift).astype(BF16)


def norm_backward(grad_normed, unit, inv_std, gain):
    scaled = grad_normed * gain
    return inv_std * (
        scaled
        - jnp.mean(scaled, axis=-1, keepdims=True)
        - unit * jnp.mean(scaled * unit, axis=-1, keepdims=True)
    )


def gelu_both(pre):
    tangent = jnp.tanh(gelu_root * (pre + gelu_cubic * pre * pre * pre))
    value = 0.5 * pre * (1.0 + tangent)
    slope = 0.5 * (1.0 + tangent) + 0.5 * pre * (1.0 - tangent * tangent) * gelu_root * (
        1.0 + 3.0 * gelu_cubic * pre * pre
    )
    return (value, slope)


def dot(a, b, dims=NN):
    return lax.dot_general(a, b, dims, preferred_element_type=F32)


def soft_columns(keys_in, queries, row_ok, factor):
    raw = jnp.where(row_ok, dot(keys_in, queries, NT), -1e30)
    top = jnp.max(raw, axis=0, keepdims=True)
    grown = jnp.exp2((raw - top) * factor)
    total = jnp.sum(grown, axis=0, keepdims=True)
    return grown * (1.0 / total)


def attend_forward_body(seq, heads, lens_ref, proj_ref, mixed_ref, qh, kh, vh, oh):
    width = heads * HD
    padded = qh.shape[1]
    for h in range(heads):
        qh[h, :seq] = proj_ref[0, :, h * HD : (h + 1) * HD]
        qh[h, seq:] = jnp.zeros((padded - seq, HD), BF16)
        kh[h] = proj_ref[0, :, width + h * HD : width + (h + 1) * HD]
        vh[h] = proj_ref[0, :, 2 * width + h * HD : 2 * width + (h + 1) * HD].T
    length = lens_ref[pl.program_id(0)]
    factor = HD**-0.5 * LOG2E

    def head(h, _):
        def chunk(c, _):
            row_ok = lax.broadcasted_iota(jnp.int32, (seq, CHUNK), 0) < length
            at = pl.ds(pl.multiple_of(c * CHUNK, CHUNK), CHUNK)
            probs = soft_columns(kh[h], qh[h, at], row_ok, factor)
            oh[h, at] = dot(vh[h], probs.astype(BF16)).T.astype(BF16)
            return 0

        return lax.fori_loop(0, padded // CHUNK, chunk, 0)

    lax.fori_loop(0, heads, head, 0)
    for h in range(heads):
        mixed_ref[0, :, h * HD : (h + 1) * HD] = oh[h, :seq]


def attend_forward(lens, proj):
    images, seq, triple = proj.shape
    heads = triple // (3 * HD)
    padded = -(-seq // CHUNK) * CHUNK
    return pl.pallas_call(
        functools.partial(attend_forward_body, seq, heads),
        out_shape=jax.ShapeDtypeStruct((images, seq, heads * HD), BF16),
        grid=(images,),
        in_specs=[SMEM, pl.BlockSpec((1, seq, triple), lambda i: (i, 0, 0))],
        out_specs=pl.BlockSpec((1, seq, heads * HD), lambda i: (i, 0, 0)),
        scratch_shapes=[
            pltpu.VMEM((heads, padded, HD), BF16),
            pltpu.VMEM((heads, seq, HD), BF16),
            pltpu.VMEM((heads, HD, seq), BF16),
            pltpu.VMEM((heads, padded, HD), BF16),
        ],
        name="attend_forward",
    )(lens, proj)


def attend_backward_body(
    seq, heads, lens_ref, proj_ref, gmix_ref, gproj_ref, gbias_ref, qh, kh, kt, vh, gh, gq, gk, gv
):
    width = heads * HD
    padded = qh.shape[1]
    for h in range(heads):
        qh[h, :seq] = proj_ref[0, :, h * HD : (h + 1) * HD]
        qh[h, seq:] = jnp.zeros((padded - seq, HD), BF16)
        gh[h, :seq] = gmix_ref[0, :, h * HD : (h + 1) * HD]
        gh[h, seq:] = jnp.zeros((padded - seq, HD), BF16)
        keys_in = proj_ref[0, :, width + h * HD : width + (h + 1) * HD]
        kh[h] = keys_in
        kt[h] = keys_in.T
        vh[h] = proj_ref[0, :, 2 * width + h * HD : 2 * width + (h + 1) * HD]
    length = lens_ref[pl.program_id(0)]
    scale = HD**-0.5
    factor = scale * LOG2E

    def head(h, _):
        gk[h] = jnp.zeros((seq, HD), F32)
        gv[h] = jnp.zeros((seq, HD), F32)

        def chunk(c, _):
            row_ok = lax.broadcasted_iota(jnp.int32, (seq, CHUNK), 0) < length
            at = pl.ds(pl.multiple_of(c * CHUNK, CHUNK), CHUNK)
            queries = qh[h, at]
            grads = gh[h, at]
            probs = soft_columns(kh[h], queries, row_ok, factor)
            grad_probs = dot(vh[h], grads, NT)
            gv[h] += dot(probs.astype(BF16), grads)
            delta = jnp.sum(probs * grad_probs, axis=0, keepdims=True)
            grad_scores = (probs * (grad_probs - delta) * scale).astype(BF16)
            gk[h] += dot(grad_scores, queries)
            gq[h, at] = dot(kt[h], grad_scores).T
            return 0

        return lax.fori_loop(0, padded // CHUNK, chunk, 0)

    lax.fori_loop(0, heads, head, 0)
    for h in range(heads):
        for c, held in enumerate((gq, gk, gv)):
            value = held[h, :seq]
            at = slice(c * width + h * HD, c * width + (h + 1) * HD)
            gproj_ref[0, :, at] = value.astype(BF16)
            gbias_ref[0, :, at] = jnp.sum(value, axis=0, keepdims=True)


def attend_backward(lens, proj, gmix):
    images, seq, triple = proj.shape
    heads = triple // (3 * HD)
    padded = -(-seq // CHUNK) * CHUNK
    return pl.pallas_call(
        functools.partial(attend_backward_body, seq, heads),
        out_shape=(
            jax.ShapeDtypeStruct((images, seq, triple), BF16),
            jax.ShapeDtypeStruct((images, 1, triple), F32),
        ),
        grid=(images,),
        in_specs=[
            SMEM,
            pl.BlockSpec((1, seq, triple), lambda i: (i, 0, 0)),
            pl.BlockSpec((1, seq, heads * HD), lambda i: (i, 0, 0)),
        ],
        out_specs=(
            pl.BlockSpec((1, seq, triple), lambda i: (i, 0, 0)),
            pl.BlockSpec((1, 1, triple), lambda i: (i, 0, 0)),
        ),
        scratch_shapes=[
            pltpu.VMEM((heads, padded, HD), BF16),
            pltpu.VMEM((heads, seq, HD), BF16),
            pltpu.VMEM((heads, HD, seq), BF16),
            pltpu.VMEM((heads, seq, HD), BF16),
            pltpu.VMEM((heads, padded, HD), BF16),
            pltpu.VMEM((heads, padded, HD), F32),
            pltpu.VMEM((heads, seq, HD), F32),
            pltpu.VMEM((heads, seq, HD), F32),
        ],
        name="attend_backward",
    )(lens, proj, gmix)


def plane():
    me = lax.axis_index("tensor")
    side = me + 1 - 2 * lax.rem(me, 2)
    over = lax.rem(me + 2, 4)
    return (me, side, over, lax.rem(side + 2, 4))


def greet(peers):
    barrier = pltpu.get_barrier_semaphore()
    for peer in peers:
        pl.semaphore_signal(barrier, inc=1, device_id={"tensor": peer}, device_id_type=MESH)
    pl.semaphore_wait(barrier, len(peers))


def greet_all(groups):
    row, me = lax.axis_index("dp"), lax.axis_index("tensor")
    barrier = pltpu.get_barrier_semaphore()
    peers = [{"dp": lax.rem(row + k, groups)} for k in range(1, groups)]
    peers += [{"tensor": lax.rem(me + k, 4)} for k in range(1, 4)]
    for peer in peers:
        pl.semaphore_signal(barrier, inc=1, device_id=peer, device_id_type=MESH)
    pl.semaphore_wait(barrier, len(peers))


def remote(src, dst, send, recv, peer):
    return pltpu.make_async_remote_copy(
        src_ref=src,
        dst_ref=dst,
        send_sem=send,
        recv_sem=recv,
        device_id={"tensor": peer},
        device_id_type=MESH,
    )


def halves_of(rows):
    first = -(-rows // 32) * 16
    return (pl.ds(0, first), pl.ds(first, rows - first))


class Gather:
    def __init__(self, all_ref, rows, send, recv):
        me, side, over, _ = plane()
        low, high = halves_of(rows)
        plan = (
            (me, low, side),
            (me, high, over),
            (me, high, side),
            (me, low, over),
            (side, low, over),
            (over, high, side),
        )
        self.copies = []
        for k, (block, part, peer) in enumerate(plan):
            ref = all_ref.at[block, part]
            self.copies.append(remote(ref, ref, send.at[k], recv.at[k], peer))

    def start(self):
        for made in self.copies[:4]:
            made.start()

    def forward(self):
        for k in range(2):
            self.copies[k].wait_recv()
            self.copies[4 + k].start()

    def arrive(self):
        for made in self.copies[2:]:
            made.wait_recv()

    def finish(self):
        for made in self.copies:
            made.wait_send()


class Scatter:
    def __init__(self, part_ref, rows, slots, send, recv):
        self.me, self.side, self.over, cross = plane()
        self.part_ref = part_ref
        self.own, self.other, self.far, self.passing = slots
        self.halves = low, high = halves_of(rows)
        plan = (
            (part_ref.at[cross, low], self.other.at[low], self.side),
            (part_ref.at[cross, high], self.other.at[high], self.over),
            (part_ref.at[self.side, low], self.own.at[low], self.side),
            (part_ref.at[self.over, high], self.own.at[high], self.over),
            (self.passing.at[low], self.far.at[low], self.over),
            (self.passing.at[high], self.far.at[high], self.side),
        )
        self.copies = [remote(src, dst, send.at[k], recv.at[k], peer) for k, (src, dst, peer) in enumerate(plan)]

    def start(self):
        for made in self.copies[:4]:
            made.start()

    def forward(self):
        for k, (part, block) in enumerate(zip(self.halves, (self.over, self.side))):
            self.copies[k].wait_recv()
            mine = self.part_ref[block, part].astype(F32)
            self.passing[part] = (mine + self.other[part].astype(F32)).astype(BF16)
            self.copies[4 + k].start()

    def arrive(self):
        for made in self.copies[2:]:
            made.wait_recv()

    def total(self, rows):
        return (
            self.part_ref[self.me, rows].astype(F32) + self.own[rows].astype(F32) + self.far[rows].astype(F32)
        )

    def finish(self):
        for made in self.copies:
            made.wait_send()


STEPS = 6


def sems(*shape):
    return [pltpu.SemaphoreType.DMA(shape), pltpu.SemaphoreType.DMA(shape)]


def params(cid):
    return pltpu.CompilerParams(collective_id=cid, has_side_effects=True, vmem_limit_bytes=67043328)


def lanes(width):
    return -(-width // 128) * 128


def pad_rows(rows):
    return -(-rows // 16) * 16


def clear_pads(ref, rows):
    full = ref.shape[1]
    for b in range(ref.shape[0]):
        ref[b, rows:full] = jnp.zeros((full - rows, ref.shape[2]), ref.dtype)


def at_row(ref):
    return ref[...].reshape(1, -1)


def for_image(i, images, act):
    for k in range(images):
        pl.when(i == k)(functools.partial(act, k))


def key_bias(mask, rows, full, seq):
    length = jnp.sum(mask.astype(F32), axis=1, keepdims=True).astype(jnp.int32)
    at = lax.broadcasted_iota(jnp.int32, (seq, 128 - HD), 0)
    lane = lax.broadcasted_iota(jnp.int32, (seq, 128 - HD), 1)
    block = sum((at >= b * full).astype(jnp.int32) for b in range(1, seq // full))
    inner = at - block * full
    good = (inner < rows) & (inner + block * rows < length)
    bias = jnp.where(good, 0.0, -1e30)
    ones = jnp.where(lane == 0, 1.0, 0.0)
    return (jnp.where(lane == 0, bias, 0.0).astype(BF16), ones.astype(BF16))


def soft_open(keys_in, queries, factor):
    raw = dot(keys_in, queries, NT)
    top = jnp.max(raw, axis=0, keepdims=True)
    grown = jnp.exp2((raw - top) * factor)
    total = jnp.sum(grown, axis=0, keepdims=True)
    return grown * (1.0 / total)


def block_of(ref, block, groups):
    if len(ref.shape) == 3:
        return ref.at[block]
    depth = ref.shape[0] // groups
    return ref.at[pl.ds(pl.multiple_of(block * depth, 16), depth)]


def over_dp(src, dst, send, recv, peer):
    return pltpu.make_async_remote_copy(
        src_ref=src, dst_ref=dst, send_sem=send, recv_sem=recv, device_id={"dp": peer}, device_id_type=MESH
    )


class Spread:
    def __init__(self, groups, all_ref, send, recv):
        row = lax.axis_index("dp")
        twin = row + 1 - 2 * lax.rem(row, 2)
        half = groups // 2
        chip = lax.div(row, 2)
        self.relayed = half == 4
        self.out, self.back = [], []
        for k in range(half):
            came = block_of(all_ref, lax.rem(row + groups - 2 * k, groups), groups)
            self.back.append(over_dp(came, came, send.at[half + k], recv.at[half + k], twin))
            if k > 0:
                mine = block_of(all_ref, row, groups)
                self.out.append(over_dp(mine, mine, send.at[k], recv.at[k], lax.rem(row + 2 * k, groups)))
        self.asked = {}
        if self.relayed:
            self.asked = {0: chip != 3, 2: chip != 0}
            self.inner = (chip == 1) | (chip == 2)
            up = lax.div(chip, 2)
            came = block_of(all_ref, lax.rem(row + 4, groups), groups)
            self.relay = over_dp(came, came, send.at[0], recv.at[1 + 2 * up], row + 4 * up - 2)

    def where(self, k, act):
        if k in self.asked:
            pl.when(self.asked[k])(act)
        else:
            act()

    def start(self):
        for k in (1, 0, 2) if self.relayed else range(len(self.out)):
            self.where(k, self.out[k].start)
        self.back[0].start()

    def hop(self):
        if self.relayed:
            self.out[1].wait_recv()
            pl.when(self.inner)(self.relay.start)
            self.back[2].start()

    def forward(self):
        for k, (far, near) in enumerate(zip(self.out, self.back[1:])):
            if k != 1 or not self.relayed:
                far.wait_recv()
                near.start()

    def arrive(self):
        for made in self.back:
            made.wait_recv()

    def finish(self):
        for k, made in enumerate(self.out):
            self.where(k, made.wait_send)
        for made in self.back:
            made.wait_send()
        if self.relayed:
            pl.when(self.inner)(self.relay.wait_send)


class Moves:
    def __init__(self, sem):
        self.sem, self.made = sem, []

    def plan(self, src, dst):
        made = pltpu.make_async_copy(src, dst, self.sem.at[len(self.made)])
        self.made.append(made)
        return made

    def start(self, src, dst):
        made = self.plan(src, dst)
        made.start()
        return made

    def finish(self):
        for made in self.made:
            made.wait()


class Reduce:
    def __init__(self, groups, grad_ref, twin_ref, far_ref, tsend, trecv, fsend, frecv):
        self.grad_ref = grad_ref
        depth = grad_ref.shape[0] // groups
        if far_ref is None:
            near, first = twin_ref, depth * (groups // 2)
            self.twin = lambda slot: near.at[pl.ds(pl.multiple_of(slot * depth, 16), depth)]
            self.far = [near.at[pl.ds(first + k * depth, depth)] for k in range(groups // 2 - 1)]
        else:
            self.twin = lambda slot: twin_ref.at[slot]
            self.far = [far_ref.at[k] for k in range(groups // 2 - 1)]
        rows = lambda block: pl.ds(pl.multiple_of(block * depth, 16), depth)
        row = lax.axis_index("dp")
        core = lax.rem(row, 2)
        self.kept, self.mine = self.twin(lax.div(row, 2)), rows(row)
        self.near, self.away = [], []
        for k in range(groups // 2):
            theirs = grad_ref.at[rows(2 * k + 1 - core)]
            self.near.append(over_dp(theirs, self.twin(k), tsend.at[k], trecv.at[k], row + 1 - 2 * core))
        for k in range(1, groups // 2):
            peer = lax.rem(row + 2 * k, groups)
            slot = lax.div(peer, 2)
            held = self.twin(slot)
            made = over_dp(held, self.far[k - 1], fsend.at[k], frecv.at[k], peer)
            self.away.append((held, rows(peer), made))

    def start(self):
        for made in self.near:
            made.start()

    def pair(self):
        for made in self.near:
            made.wait_recv()
        for held, part, made in self.away:
            held[...] = (held[...].astype(F32) + self.grad_ref[part].astype(F32)).astype(BF16)
            made.start()

    def total(self):
        value = self.kept[...].astype(F32) + self.grad_ref[self.mine].astype(F32)
        for (_, _, made), came in zip(self.away, self.far):
            made.wait_recv()
            value = value + came[...].astype(F32)
        return value

    def finish(self):
        for made in self.near + [made for _, _, made in self.away]:
            made.wait_send()


def reduce_scratch(groups, depth, width):
    half, width = groups // 2, lanes(width)
    return [pltpu.VMEM((half, depth, width), BF16), pltpu.VMEM((half - 1, depth, width), BF16)] + sems(half) * 2


def outer(out_ref, left_ref, right_ref, width):
    images, blocks, full, model = left_ref.shape
    count = images * blocks * full
    tile = 384
    extra = out_ref.shape[1] - width
    if extra > 0:
        out_ref[:, width:] = jnp.zeros((out_ref.shape[0], extra), BF16)

    def part(c, _):
        at = pl.ds(pl.multiple_of(c * tile, tile), tile)
        left = left_ref[:, :, :, at].reshape(count, tile)
        right = right_ref[:, :, :, :width].reshape(count, width)
        out_ref[at, :width] = dot(left, right, TN).astype(BF16)
        return 0

    lax.fori_loop(0, model // tile, part, 0)


def whole_body(
    groups, rows, heads,
    x_ref, grad_ref, mask_ref, gain_one, bias_one, bias_out, gain_two, bias_two, bias_down, qv_ref, hb_ref,
    wq_ref, wo_ref, wh_ref, wd_ref,
    one_out, block_out, gin_out, gwq_ref, gwo_ref, gwh_ref, gwd_ref, both_ref,
    one_ref, full_ref, two_ref, hidden_ref, qh, kh, vh, mixed_ref, wq_all, wo_all, wh_all, wd_all,
    gq, part_ref, ghid_ref, act_ref, gpl_ref, gwh_part, gwd_part, gwo_part, slots, osem,
    dtwin, daway, dtsend, dtrecv, dfsend, dfrecv,
    otwin, oaway, otsend, otrecv, ofsend, ofrecv,
    htsend, htrecv, hfsend, hfrecv, qtsend, qtrecv, qfsend, qfrecv,
    gsend, grecv, wsend, wrecv,
    hsum, bsum, mid, row_in, flat_in, vsend, vrecv,
):
    images = x_ref.shape[0]
    _, _, full, model = one_ref.shape
    units = hb_ref.shape[0]
    seq = 4 * full
    width = heads * HD
    last = images - 1
    me, side, over, _ = plane()
    mine = lax.axis_index("dp")
    wq_all[mine, :, 3 * width :] = jnp.zeros_like(wq_all[mine, :, 3 * width :])
    for c in range(3):
        wq_all[mine, :, c * width : (c + 1) * width] = wq_ref[c]
    weights = [Spread(groups, wq_all, wsend.at[0], wrecv.at[0])]
    for k, (own, everyone) in enumerate(((wo_ref, wo_all), (wh_ref, wh_all), (wd_ref, wd_all))):
        count = own.shape[1]
        place = block_of(everyone, mine, groups)
        place[:, count:] = jnp.zeros((own.shape[0], everyone.shape[-1] - count), BF16)
        place[:, :count] = own[...]
        weights.append(Spread(groups, everyone, wsend.at[k + 1], wrecv.at[k + 1]))
    wq, wo, wh, wd = weights
    ones, sums, twos, grads, turns, lows, outs, backs = [], [], [], [], [], [], [], []
    for i in range(images):
        for ref in (one_ref, two_ref, full_ref):
            clear_pads(ref.at[i], rows)
        pair = lambda k: (gsend.at[k, i], grecv.at[k, i])
        four = [slots.at[i, k] for k in range(4)]
        spare = [act_ref.at[i, k] for k in range(4)]
        ones.append(Gather(one_ref.at[i], rows, *pair(0)))
        grads.append(Gather(full_ref.at[i], rows, *pair(1)))
        sums.append(Scatter(part_ref.at[i], rows, four, *pair(2)))
        twos.append(Gather(two_ref.at[i], rows, *pair(3)))
        turns.append(Scatter(part_ref.at[i], rows, four, *pair(4)))
        lows.append(Gather(one_ref.at[i], rows, *pair(5)))
        outs.append(Scatter(two_ref.at[i], rows, spare, *pair(6)))
        backs.append(Scatter(part_ref.at[i], rows, four, *pair(7)))
    down = Reduce(groups, gwd_part, dtwin, daway, dtsend, dtrecv, dfsend, dfrecv)
    red_h = Reduce(groups, gwh_part, wh_all.at[:, pl.ds(0, lanes(units))], None, htsend, htrecv, hfsend, hfrecv)
    red_o = Reduce(groups, gwo_part, otwin, oaway, otsend, otrecv, ofsend, ofrecv)
    gwq_part = gwd_part.at[:, pl.ds(0, lanes(3 * width))]
    red_q = Reduce(groups, gwq_part, wd_all.at[:, pl.ds(0, lanes(3 * width))], None, qtsend, qtrecv, qfsend, qfrecv)
    moves = Moves(osem)
    keep_one = [moves.plan(one_ref.at[i], one_out.at[i]) for i in range(images)]
    take_one = [moves.plan(one_out.at[i], full_ref.at[i]) for i in range(images)]
    take_grad = [moves.plan(grad_ref.at[i], full_ref.at[i, me, pl.ds(0, rows)]) for i in range(images)]
    for made in take_grad:
        made.start()
    put_out = [moves.plan(two_ref.at[i, me, pl.ds(0, rows)], block_out.at[i]) for i in range(images)]
    put_gin = [moves.plan(ghid_ref.at[i], gin_out.at[i]) for i in range(images)]

    def enter(i):
        one_ref[i, me, :rows] = norm_forward(x_ref[i].astype(F32), at_row(gain_one), at_row(bias_one))

    enter(0)
    for made in take_grad:
        made.wait()
    greet_all(groups)
    ones[0].start()
    wq.start()
    for i in range(1, images):
        enter(i)
        ones[i].start()
    for step in (wo, wh, wd):
        step.start()
    hsum[...] = jnp.zeros_like(hsum)
    bsum[...] = jnp.zeros_like(bsum)
    mixed_ref[:, :, :, width:] = jnp.zeros_like(mixed_ref[:, :, :, width:])
    for i in range(images):
        bias, tail = key_bias(mask_ref[i : i + 1], rows, full, seq)
        for h in range(heads):
            kh[i, h, :, HD:] = bias
            vh[i, h, :, HD:] = jnp.zeros_like(bias)
            qh[i, h, :, HD:] = tail
    for step in ones:
        step.forward()
    grads[0].start()
    wq.hop()
    wq.forward()
    scale = HD**-0.5
    shift_q, shift_v = qv_ref[0:1], qv_ref[1:2]

    def project(i):
        weight = wq_all[:, :, : 3 * width].reshape(-1, 3 * width)

        def block(b, _):
            at = pl.ds(pl.multiple_of(b * full, 16), full)
            value = dot(one_ref[i, b], weight)
            queries = (value[:, :width] + shift_q).astype(BF16)
            keys_in = value[:, width : 2 * width].astype(BF16)
            values = (value[:, 2 * width :] + shift_v).astype(BF16)
            for h in range(heads):
                here = slice(h * HD, (h + 1) * HD)
                qh[i, h, at, :HD] = queries[:, here]
                kh[i, h, at, :HD] = keys_in[:, here]
                vh[i, h, at, :HD] = values[:, here]
            return 0

        lax.fori_loop(0, 4, block, 0)

    def attend(i):
        def head(h, _):
            probs = soft_open(kh[i, h], qh[i, h], scale * LOG2E)
            gq[h] = dot(vh[i, h, :, :HD].T, probs.astype(BF16)).T.astype(BF16)
            return 0

        lax.fori_loop(0, heads, head, 0, unroll=2)
        for h in range(heads):
            for b in range(4):
                mixed_ref[i, b, :, h * HD : (h + 1) * HD] = gq[h, b * full : (b + 1) * full]

    def combine(i):
        weight = wo_all[:, :, :width].reshape(-1, width)

        def block(b, _):
            part_ref[i, b] = dot(mixed_ref[i, b, :, :width], weight, NT).astype(BF16)
            return 0

        lax.fori_loop(0, 4, block, 0)

    def ready(k):
        ones[k].arrive()
        keep_one[k].start()
        if k == 0:
            wq.arrive()

    def between(k):
        if k == 0:
            grads[0].forward()
            wo.hop()
            wo.forward()
            wh.hop()
            wo.arrive()

    def send(k):
        if k > 0:
            sums[k - 1].forward()
        sums[k].start()

    def image(i, _):
        for_image(i, images, ready)
        project(i)
        attend(i)
        for_image(i, images, between)
        combine(i)
        for_image(i, images, send)
        return 0

    lax.fori_loop(0, images, image, 0)

    def settle(i):
        sums[i].arrive()
        hidden = x_ref[i].astype(F32) + sums[i].total(pl.ds(0, rows)) + at_row(bias_out)
        hidden_ref[i] = hidden
        two_ref[i, me, :rows] = norm_forward(hidden, at_row(gain_two), at_row(bias_two))
        twos[i].start()

    for i in range(last):
        settle(i)
    sums[-1].forward()
    wd.hop()
    for i in range(last):
        twos[i].forward()
    settle(last)
    for step in grads[1:]:
        step.start()
    wh.forward()
    wd.forward()
    twos[-1].forward()
    for step in sums + ones:
        step.finish()
    for made in keep_one:
        made.wait()
    wide = lambda ref: ref[:, :units]
    shift = at_row(hb_ref)

    def ascend(i):
        def pair(c, _):
            at = pl.ds(2 * c, 2)
            pre = dot(two_ref[i, at].reshape(2 * full, model), wide(wh_all)) + shift
            value, slope = gelu_both(pre)
            act_ref[i, at, :, :units] = value.astype(BF16).reshape(2, full, units)
            grad_pre = dot(full_ref[i, at].reshape(2 * full, model), wide(wd_all)) * slope
            hsum[...] += jnp.sum(grad_pre, axis=0, keepdims=True)
            low = grad_pre.astype(BF16)
            gpl_ref[i, at, :, :units] = low.reshape(2, full, units)
            part_ref[i, at] = dot(low, wide(wh_all), NT).astype(BF16).reshape(2, full, model)
            return 0

        lax.fori_loop(0, 2, pair, 0)

    def descend(k, _):
        at = pl.ds(2 * lax.rem(k, 2), 2)
        i = lax.div(k, 2)
        part = dot(act_ref[i, at, :, :units].reshape(2 * full, units), wide(wd_all), NT)
        two_ref[i, at] = part.astype(BF16).reshape(2, full, model)
        return 0

    totals = [0.0] * 6

    def add_up(first, terms):
        for k, term in enumerate(terms):
            totals[first + k] = totals[first + k] + jnp.sum(term, axis=0, keepdims=True)

    def settle_back(i):
        turns[i].arrive()
        grad_normed = turns[i].total(pl.ds(0, rows))
        unit, inv_std = norm_stats(hidden_ref[i])
        upper = full_ref[i, me, :rows].astype(F32)
        grad_hidden = upper + norm_backward(grad_normed, unit, inv_std, at_row(gain_two))
        ghid_ref[i] = grad_hidden
        one_ref[i, me, :rows] = grad_hidden.astype(BF16)
        lows[i].start()
        add_up(0, (grad_normed * unit, grad_normed, grad_hidden, upper))

    def ready_back(k):
        twos[k].arrive()
        if k == 0:
            wh.arrive()
            wd.arrive()
        grads[k].arrive()

    def send_back(k):
        if k == 0:
            for step in grads[1:]:
                step.forward()
        if k > 0:
            turns[k - 1].forward()
        turns[k].start()

    def image_back(i, _):
        for_image(i, images, ready_back)
        ascend(i)
        for_image(i, images, send_back)
        return 0

    lax.fori_loop(0, images, image_back, 0)
    for step in weights:
        step.finish()
    outer(gwd_part, full_ref, act_ref, units)
    down.start()
    for i in range(last):
        settle_back(i)
    turns[-1].forward()
    down.pair()
    outer(gwh_part, two_ref, gpl_ref, units)
    red_h.start()
    for i in range(last):
        lows[i].forward()
    for step in twos:
        step.finish()
    lax.fori_loop(0, 2 * images, descend, 0)
    settle_back(last)
    for step in turns + grads:
        step.finish()
    for made in take_one:
        made.start()

    def mix(i):
        value = dot(one_ref[i].reshape(seq, model), wo_all[:, :, :width].reshape(model, width)).astype(BF16)
        gpl_ref[i, :, :, 3 * width : 4 * width] = value.reshape(4, full, width)

    def attend_back(i):
        for h in range(heads):
            here = slice(3 * width + h * HD, 3 * width + (h + 1) * HD)
            queries = qh[i, h]
            grads_in = gpl_ref[i, :, :, here].reshape(seq, HD)
            keys_in = kh[i, h]
            probs = soft_open(keys_in, queries, scale * LOG2E)
            grad_probs = dot(vh[i, h, :, :HD], grads_in, NT)
            grad_values = dot(probs.astype(BF16), grads_in)
            delta = jnp.sum(probs * grad_probs, axis=0, keepdims=True)
            grad_scores = (probs * (grad_probs - delta) * scale).astype(BF16)
            grad_keys = dot(grad_scores, queries[:, :HD])
            grad_queries = dot(keys_in[:, :HD].T, grad_scores).T
            for c, value in enumerate((grad_queries, grad_keys, grad_values)):
                here = slice(c * width + h * HD, c * width + (h + 1) * HD)
                gpl_ref[i, :, :, here] = value.astype(BF16).reshape(4, full, HD)
                bsum[h, c : c + 1] += jnp.sum(value, axis=0, keepdims=True)

    def spread(i):
        def pair(c, _):
            at = pl.ds(2 * c, 2)
            left = gpl_ref[i, at, :, : 3 * width].reshape(2 * full, 3 * width)
            part = dot(left, wq_all[:, :, : 3 * width].reshape(model, 3 * width), NT)
            part_ref[i, at] = part.astype(BF16).reshape(2, full, model)
            return 0

        lax.fori_loop(0, 2, pair, 0)

    def ready_last(k):
        lows[k].arrive()

    def send_last(k):
        if k < last:
            lows[k + 1].forward()
        if k > 0:
            backs[k - 1].forward()
        backs[k].start()
        if k == 0:
            gwd_ref[...] = down.total()[:, :units]
            red_h.pair()

    def image_last(i, _):
        for_image(i, images, ready_last)
        mix(i)
        attend_back(i)
        spread(i)
        for_image(i, images, send_last)
        return 0

    lax.fori_loop(0, images, image_last, 0)
    down.finish()
    outer(gwo_part, one_ref, mixed_ref, width)
    red_o.start()
    for made in take_one:
        made.wait()
    outer(gwq_part, full_ref, gpl_ref, 3 * width)
    red_o.pair()
    red_q.start()

    def settle_last(i):
        backs[i].arrive()
        grad_normed = backs[i].total(pl.ds(0, rows))
        unit, inv_std = norm_stats(x_ref[i].astype(F32))
        ghid_ref[i] = ghid_ref[i] + norm_backward(grad_normed, unit, inv_std, at_row(gain_one))
        put_gin[i].start()
        add_up(4, (grad_normed * unit, grad_normed))

    def finish_out(i):
        outs[i].arrive()
        value = hidden_ref[i] + outs[i].total(pl.ds(0, rows)) + at_row(bias_down)
        two_ref[i, me, :rows] = value.astype(BF16)
        put_out[i].start()

    for i in range(last):
        settle_last(i)
    backs[-1].forward()
    for step in outs:
        step.start()
    gwh_ref[...] = red_h.total()[:, :units]
    red_q.pair()
    mid[0] = jnp.zeros_like(mid[0])
    for h in range(heads):
        for c in range(3):
            mid[0, 6:7, c * width + h * HD : c * width + (h + 1) * HD] = bsum[h, c : c + 1]
    mid[0, 7:8, :units] = hsum[...]
    for step in outs[:-1]:
        step.forward()
    settle_last(last)

    for k in range(6):
        mid[0, k : k + 1] = totals[k]
    row_in[mine] = mid[0]
    aways = []
    for k in range(1, groups):
        aways.append(over_dp(mid.at[0], row_in.at[mine], vsend.at[k], vrecv.at[k], lax.rem(mine + k, groups)))
        aways[-1].start()
    outs[-1].forward()
    for made in aways:
        made.wait()
    held = row_in[0]
    for k in range(1, groups):
        held = held + row_in[k]
    mid[1] = held
    flat_in[me] = mid[1]
    planes = []
    for k in range(1, 4):
        at = groups + k
        planes.append(remote(mid.at[1], flat_in.at[me], vsend.at[at], vrecv.at[at], lax.rem(me + k, 4)))
        planes[-1].start()
    for i in range(last):
        finish_out(i)
    for made in planes:
        made.wait()
    both_ref[0:6] = (flat_in[0] + flat_in[1] + flat_in[2] + flat_in[3])[0:6]
    both_ref[6:8] = mid[1, 6:8]
    gwo_ref[...] = red_o.total()[:, :width]
    finish_out(last)
    total = red_q.total()
    for c in range(3):
        gwq_ref[c] = total[:, c * width : (c + 1) * width]
    for step in lows + outs + backs + [red_h, red_o, red_q]:
        step.finish()
    for made in put_out + put_gin:
        made.wait()


def whole(groups, block_input, grad_out, key_mask, vectors, qv_bias, bias, wq, wo, wh, wd):
    images, rows, model = block_input.shape
    full = pad_rows(rows)
    width = wo.shape[1]
    units = wh.shape[1]
    heads = width // HD
    seq = 4 * full
    depth = wo.shape[0]
    blocks = ((images, 4, full, model), BF16)
    own = ((images, rows, model), F32)
    heads_wide = ((images, heads, seq, 128), BF16)
    piece = ((heads, seq, HD), BF16)
    square = ((model, lanes(units)), BF16)
    weight = lambda count: ((groups, depth, lanes(count)), BF16)
    outs = [blocks, (block_input.shape, BF16), own]
    more = [((3, depth, width), F32), ((depth, width), F32), ((depth, units), F32), ((depth, units), F32), ((8, model), F32)]
    held = [blocks, blocks, blocks, own, heads_wide, heads_wide, heads_wide, ((images, 4, full, lanes(width)), BF16)]
    held += [weight(3 * width), weight(width), square, square]
    held += [piece, blocks, own, blocks, blocks, square, square, ((model, lanes(width)), BF16), blocks]
    return pl.pallas_call(
        functools.partial(whole_body, groups, rows, heads),
        out_shape=tuple(jax.ShapeDtypeStruct(*h) for h in outs + more),
        in_specs=[VMEM, ANY] + [VMEM] * 13,
        out_specs=(ANY,) * len(outs) + (VMEM,) * len(more),
        scratch_shapes=[pltpu.VMEM(*h) for h in held]
        + [pltpu.SemaphoreType.DMA((5 * images,))]
        + reduce_scratch(groups, depth, units)
        + reduce_scratch(groups, depth, width)
        + sems(groups // 2) * 4
        + sems(8, images, STEPS)
        + sems(4, groups)
        + [
            pltpu.VMEM((1, units), F32),
            pltpu.VMEM((heads, 3, HD), F32),
            pltpu.VMEM((2, 8, model), F32),
            pltpu.VMEM((groups, 8, model), F32),
            pltpu.VMEM((4, 8, model), F32),
        ]
        + sems(groups + 4),
        compiler_params=params(0),
        name="whole",
    )(block_input, grad_out, key_mask, *vectors, qv_bias, bias, wq, wo, wh, wd)


def deliver_body(width, out, gin, gwq, gwo, gwh, gwd, both, *refs):
    refs, sem = refs[:-1], refs[-1]
    loads = Moves(sem)
    for src, dst in zip((out, gin, gwq, gwo, gwh, gwd), refs):
        loads.start(src, dst)
    qv, unit = refs[6:8]
    qv[0:1] = both[6:7, :width]
    qv[1:2] = both[6:7, 2 * width : 3 * width]
    unit[...] = both[7, : unit.shape[0]]
    for k, dst in enumerate(refs[8:]):
        dst[...] = both[k]
    loads.finish()


def deliver(width, units, out, gin, gwq, gwo, gwh, gwd, both):
    model = both.shape[1]
    same = [jax.ShapeDtypeStruct(v.shape, v.dtype) for v in (out, gin, gwq, gwo, gwh, gwd)]
    more = [jax.ShapeDtypeStruct(dims, F32) for dims in ((2, width), (units,)) + ((model,),) * 6]
    return pl.pallas_call(
        functools.partial(deliver_body, width),
        out_shape=tuple(same + more),
        in_specs=[ANY] * 6 + [VMEM],
        out_specs=(VMEM,) * 14,
        scratch_shapes=[pltpu.SemaphoreType.DMA((6,))],
        compiler_params=pltpu.CompilerParams(vmem_limit_bytes=60 << 20),
        name="deliver",
    )(out, gin, gwq, gwo, gwh, gwd, both)


def gather_rows(rows):
    return lax.all_gather(rows, "tensor", axis=1, tiled=True)


def scatter_rows(part):
    return lax.psum_scatter(part, "tensor", scatter_dimension=1, tiled=True).astype(F32)


def shards(
    groups,
    ranks,
    block_input,
    key_mask,
    attn_norm_gain,
    attn_norm_bias,
    qkv_weight,
    qv_bias,
    out_weight,
    out_bias,
    mlp_norm_gain,
    mlp_norm_bias,
    hidden_weight,
    hidden_bias,
    down_weight,
    down_bias,
    grad_out,
):
    images, rows, model = block_input.shape
    flat = ranks == 4 and images == 2 and groups > 2 and groups % 2 == 0 and hidden_weight.shape[1] <= model and 4 * qkv_weight.shape[2] <= lanes(hidden_weight.shape[1])
    seq = key_mask.shape[1]
    width = qkv_weight.shape[2]
    units = hidden_weight.shape[1]

    def weight(shard):
        return lax.all_gather(shard, "dp", axis=0, tiled=True)

    def owned(grad):
        return lax.psum_scatter(grad.astype(BF16), "dp", scatter_dimension=0, tiled=True).astype(F32)

    out_rows, down_rows = out_weight.T, down_weight.T
    if flat:
        _, block_output, grad_input, grad_qkv_w, grad_out_w, grad_hidden_w, grad_down_w, both = whole(
            groups,
            block_input,
            grad_out,
            key_mask,
            (attn_norm_gain, attn_norm_bias, out_bias, mlp_norm_gain, mlp_norm_bias, down_bias),
            qv_bias,
            hidden_bias,
            qkv_weight.transpose(1, 0, 2),
            out_rows,
            hidden_weight,
            down_rows,
        )
        (
            block_output, grad_input, grad_qkv_w, grad_out_w, grad_hidden_w, grad_down_w, grad_qv, grad_hidden_b, *both
        ) = deliver(
            width, units, block_output, grad_input, grad_qkv_w, grad_out_w, grad_hidden_w, grad_down_w, both
        )
        grad_qkv_w = grad_qkv_w.transpose(1, 0, 2)
        grad_out_w, grad_down_w = grad_out_w.T, grad_down_w.T
    else:
        qkv_rows = qkv_weight.reshape(-1, 3 * width)
        shift = jnp.concatenate([qv_bias[0], jnp.zeros_like(qv_bias[0]), qv_bias[1]])
        hidden_all, down_all = weight(hidden_weight), weight(down_rows)
        qkv_all, out_all = weight(qkv_rows), weight(out_rows)
        lens = jnp.sum(key_mask, axis=1)
        in_float = block_input.astype(F32)
        normed_one = gather_rows(norm_forward(in_float, attn_norm_gain, attn_norm_bias))
        grad_full = gather_rows(grad_out)
        proj = jnp.einsum("isd,df->isf", normed_one, qkv_all, preferred_element_type=F32) + shift
        proj = proj.astype(BF16)
        mixed = attend_forward(lens, proj)
        attn_part = jnp.einsum("isf,df->isd", mixed, out_all, preferred_element_type=F32).astype(BF16)
        hidden_res = in_float + scatter_rows(attn_part) + out_bias
        normed_two = gather_rows(norm_forward(hidden_res, mlp_norm_gain, mlp_norm_bias))
        pre_act = jnp.einsum("isd,df->isf", normed_two, hidden_all, preferred_element_type=F32) + hidden_bias
        value, slope = gelu_both(pre_act)
        activated = value.astype(BF16)
        grad_act = jnp.einsum("isd,df->isf", grad_full, down_all, preferred_element_type=F32)
        grad_pre = grad_act * slope
        grad_hidden_b = jnp.sum(grad_pre, axis=(0, 1))
        grad_pre_low = grad_pre.astype(BF16)
        gpart = jnp.einsum("isf,df->isd", grad_pre_low, hidden_all, preferred_element_type=F32).astype(BF16)
        mpart = jnp.einsum("isf,df->isd", activated, down_all, preferred_element_type=F32).astype(BF16)
        block_output = (hidden_res + scatter_rows(mpart) + down_bias).astype(BF16)
        grad_float = grad_out.astype(F32)
        grad_normed = scatter_rows(gpart)
        unit, inv_std = norm_stats(hidden_res)
        grad_hidden = grad_float + norm_backward(grad_normed, unit, inv_std, mlp_norm_gain)
        hidden_full = gather_rows(grad_hidden.astype(BF16))
        mlp_sums = jnp.stack(
            [jnp.sum(v, axis=(0, 1)) for v in (grad_normed * unit, grad_normed, grad_hidden, grad_float)]
        )
        grad_hidden_w = owned(jnp.einsum("isd,isf->df", normed_two, grad_pre_low, preferred_element_type=F32))
        grad_down_w = owned(jnp.einsum("isd,isf->df", grad_full, activated, preferred_element_type=F32)).T
        grad_mixed = jnp.einsum("isd,df->isf", hidden_full, out_all, preferred_element_type=F32).astype(BF16)
        grad_proj, proj_sums = attend_backward(lens, proj, grad_mixed)
        proj_sums = jnp.sum(proj_sums, axis=(0, 1))
        npart = jnp.einsum("isf,df->isd", grad_proj, qkv_all, preferred_element_type=F32).astype(BF16)
        grad_out_w = owned(jnp.einsum("isd,isf->df", hidden_full, mixed, preferred_element_type=F32)).T
        grad_qkv_w = owned(jnp.einsum("isd,isf->df", normed_one, grad_proj, preferred_element_type=F32))
        grad_normed = scatter_rows(npart)
        unit, inv_std = norm_stats(in_float)
        grad_input = grad_hidden + norm_backward(grad_normed, unit, inv_std, attn_norm_gain)
        attn_sums = jnp.stack([jnp.sum(v, axis=(0, 1)) for v in (grad_normed * unit, grad_normed)])
        both = lax.psum(jnp.concatenate([mlp_sums, attn_sums]), ("dp", "tensor"))
        proj_sums, grad_hidden_b = lax.psum((proj_sums, grad_hidden_b), "dp")
        grad_qv = jnp.stack([proj_sums[:width], proj_sums[2 * width :]])
        grad_qkv_w = grad_qkv_w.reshape(-1, 3, width)
    return (
        block_output,
        grad_input,
        both[4],
        both[5],
        grad_qkv_w,
        grad_qv,
        grad_out_w,
        both[2],
        both[0],
        both[1],
        grad_hidden_w,
        grad_hidden_b,
        grad_down_w,
        both[3],
    )


def solution(mesh):
    return jax.shard_map(
        functools.partial(shards, mesh.shape["dp"], mesh.shape["tensor"]),
        mesh=mesh,
        in_specs=(
            P("dp", "tensor", None),
            P("dp", None),
            P(),
            P(),
            P("dp", None, "tensor"),
            P(None, "tensor"),
            P("tensor", "dp"),
            P(),
            P(),
            P(),
            P("dp", "tensor"),
            P("tensor"),
            P("tensor", "dp"),
            P(),
            P("dp", "tensor", None),
        ),
        out_specs=(
            P("dp", "tensor", None),
            P("dp", "tensor", None),
            P(),
            P(),
            P("dp", None, "tensor"),
            P(None, "tensor"),
            P("tensor", "dp"),
            P(),
            P(),
            P(),
            P("dp", "tensor"),
            P("tensor"),
            P("tensor", "dp"),
            P(),
        ),
        check_vma=False,
    )
```

```python
import functools
import math

import jax
import jax.numpy as jnp
from jax import lax
from jax.experimental import pallas as pl
from jax.experimental.pallas import tpu as pltpu
from jax.sharding import PartitionSpec as P

HD = 72
CHUNK = 768
F32 = jnp.float32
BF16 = jnp.bfloat16
LOG2E = math.log2(math.e)
NN = (((1,), (0,)), ((), ()))
NT = (((1,), (1,)), ((), ()))
TN = (((0,), (0,)), ((), ()))
MESH = pl.DeviceIdType.MESH
ANY = pl.BlockSpec(memory_space=pl.ANY)
VMEM = pl.BlockSpec(memory_space=pltpu.VMEM)
SMEM = pl.BlockSpec(memory_space=pltpu.SMEM)


layer_eps = 1e-06
gelu_root = math.sqrt(2.0 / math.pi)
gelu_cubic = 0.044715


def norm_stats(rows):
    center = rows - jnp.mean(rows, axis=-1, keepdims=True)
    inv_std = lax.rsqrt(jnp.mean(center * center, axis=-1, keepdims=True) + layer_eps)
    return (center * inv_std, inv_std)


def norm_forward(rows, gain, shift):
    unit, _ = norm_stats(rows)
    return (unit * gain + shift).astype(BF16)


def norm_backward(grad_normed, unit, inv_std, gain):
    scaled = grad_normed * gain
    return inv_std * (
        scaled
        - jnp.mean(scaled, axis=-1, keepdims=True)
        - unit * jnp.mean(scaled * unit, axis=-1, keepdims=True)
    )


def gelu_both(pre):
    tangent = jnp.tanh(gelu_root * (pre + gelu_cubic * pre * pre * pre))
    value = 0.5 * pre * (1.0 + tangent)
    slope = 0.5 * (1.0 + tangent) + 0.5 * pre * (1.0 - tangent * tangent) * gelu_root * (
        1.0 + 3.0 * gelu_cubic * pre * pre
    )
    return (value, slope)


def dot(a, b, dims=NN):
    return lax.dot_general(a, b, dims, preferred_element_type=F32)


def soft_columns(keys_in, queries, row_ok, factor):
    raw = jnp.where(row_ok, dot(keys_in, queries, NT), -1e30)
    top = jnp.max(raw, axis=0, keepdims=True)
    grown = jnp.exp2((raw - top) * factor)
    total = jnp.sum(grown, axis=0, keepdims=True)
    return grown * (1.0 / total)


def attend_forward_body(seq, heads, lens_ref, proj_ref, mixed_ref, qh, kh, vh, oh):
    width = heads * HD
    padded = qh.shape[1]
    for h in range(heads):
        qh[h, :seq] = proj_ref[0, :, h * HD : (h + 1) * HD]
        qh[h, seq:] = jnp.zeros((padded - seq, HD), BF16)
        kh[h] = proj_ref[0, :, width + h * HD : width + (h + 1) * HD]
        vh[h] = proj_ref[0, :, 2 * width + h * HD : 2 * width + (h + 1) * HD].T
    length = lens_ref[pl.program_id(0)]
    factor = HD**-0.5 * LOG2E

    def head(h, _):
        def chunk(c, _):
            row_ok = lax.broadcasted_iota(jnp.int32, (seq, CHUNK), 0) < length
            at = pl.ds(pl.multiple_of(c * CHUNK, CHUNK), CHUNK)
            probs = soft_columns(kh[h], qh[h, at], row_ok, factor)
            oh[h, at] = dot(vh[h], probs.astype(BF16)).T.astype(BF16)
            return 0

        return lax.fori_loop(0, padded // CHUNK, chunk, 0)

    lax.fori_loop(0, heads, head, 0)
    for h in range(heads):
        mixed_ref[0, :, h * HD : (h + 1) * HD] = oh[h, :seq]


def attend_forward(lens, proj):
    images, seq, triple = proj.shape
    heads = triple // (3 * HD)
    padded = -(-seq // CHUNK) * CHUNK
    return pl.pallas_call(
        functools.partial(attend_forward_body, seq, heads),
        out_shape=jax.ShapeDtypeStruct((images, seq, heads * HD), BF16),
        grid=(images,),
        in_specs=[SMEM, pl.BlockSpec((1, seq, triple), lambda i: (i, 0, 0))],
        out_specs=pl.BlockSpec((1, seq, heads * HD), lambda i: (i, 0, 0)),
        scratch_shapes=[
            pltpu.VMEM((heads, padded, HD), BF16),
            pltpu.VMEM((heads, seq, HD), BF16),
            pltpu.VMEM((heads, HD, seq), BF16),
            pltpu.VMEM((heads, padded, HD), BF16),
        ],
        name="attend_forward",
    )(lens, proj)


def attend_backward_body(
    seq, heads, lens_ref, proj_ref, gmix_ref, gproj_ref, gbias_ref, qh, kh, kt, vh, gh, gq, gk, gv
):
    width = heads * HD
    padded = qh.shape[1]
    for h in range(heads):
        qh[h, :seq] = proj_ref[0, :, h * HD : (h + 1) * HD]
        qh[h, seq:] = jnp.zeros((padded - seq, HD), BF16)
        gh[h, :seq] = gmix_ref[0, :, h * HD : (h + 1) * HD]
        gh[h, seq:] = jnp.zeros((padded - seq, HD), BF16)
        keys_in = proj_ref[0, :, width + h * HD : width + (h + 1) * HD]
        kh[h] = keys_in
        kt[h] = keys_in.T
        vh[h] = proj_ref[0, :, 2 * width + h * HD : 2 * width + (h + 1) * HD]
    length = lens_ref[pl.program_id(0)]
    scale = HD**-0.5
    factor = scale * LOG2E

    def head(h, _):
        gk[h] = jnp.zeros((seq, HD), F32)
        gv[h] = jnp.zeros((seq, HD), F32)

        def chunk(c, _):
            row_ok = lax.broadcasted_iota(jnp.int32, (seq, CHUNK), 0) < length
            at = pl.ds(pl.multiple_of(c * CHUNK, CHUNK), CHUNK)
            queries = qh[h, at]
            grads = gh[h, at]
            probs = soft_columns(kh[h], queries, row_ok, factor)
            grad_probs = dot(vh[h], grads, NT)
            gv[h] += dot(probs.astype(BF16), grads)
            delta = jnp.sum(probs * grad_probs, axis=0, keepdims=True)
            grad_scores = (probs * (grad_probs - delta) * scale).astype(BF16)
            gk[h] += dot(grad_scores, queries)
            gq[h, at] = dot(kt[h], grad_scores).T
            return 0

        return lax.fori_loop(0, padded // CHUNK, chunk, 0)

    lax.fori_loop(0, heads, head, 0)
    for h in range(heads):
        for c, held in enumerate((gq, gk, gv)):
            value = held[h, :seq]
            at = slice(c * width + h * HD, c * width + (h + 1) * HD)
            gproj_ref[0, :, at] = value.astype(BF16)
            gbias_ref[0, :, at] = jnp.sum(value, axis=0, keepdims=True)


def attend_backward(lens, proj, gmix):
    images, seq, triple = proj.shape
    heads = triple // (3 * HD)
    padded = -(-seq // CHUNK) * CHUNK
    return pl.pallas_call(
        functools.partial(attend_backward_body, seq, heads),
        out_shape=(
            jax.ShapeDtypeStruct((images, seq, triple), BF16),
            jax.ShapeDtypeStruct((images, 1, triple), F32),
        ),
        grid=(images,),
        in_specs=[
            SMEM,
            pl.BlockSpec((1, seq, triple), lambda i: (i, 0, 0)),
            pl.BlockSpec((1, seq, heads * HD), lambda i: (i, 0, 0)),
        ],
        out_specs=(
            pl.BlockSpec((1, seq, triple), lambda i: (i, 0, 0)),
            pl.BlockSpec((1, 1, triple), lambda i: (i, 0, 0)),
        ),
        scratch_shapes=[
            pltpu.VMEM((heads, padded, HD), BF16),
            pltpu.VMEM((heads, seq, HD), BF16),
            pltpu.VMEM((heads, HD, seq), BF16),
            pltpu.VMEM((heads, seq, HD), BF16),
            pltpu.VMEM((heads, padded, HD), BF16),
            pltpu.VMEM((heads, padded, HD), F32),
            pltpu.VMEM((heads, seq, HD), F32),
            pltpu.VMEM((heads, seq, HD), F32),
        ],
        name="attend_backward",
    )(lens, proj, gmix)


def plane():
    me = lax.axis_index("tensor")
    side = me + 1 - 2 * lax.rem(me, 2)
    over = lax.rem(me + 2, 4)
    return (me, side, over, lax.rem(side + 2, 4))


def greet(peers):
    barrier = pltpu.get_barrier_semaphore()
    for peer in peers:
        pl.semaphore_signal(barrier, inc=1, device_id={"tensor": peer}, device_id_type=MESH)
    pl.semaphore_wait(barrier, len(peers))


def greet_all(groups, work):
    row, me = lax.axis_index("dp"), lax.axis_index("tensor")
    barrier = pltpu.get_barrier_semaphore()
    peers = [{"dp": lax.rem(row + k, groups)} for k in range(1, groups)]
    peers += [{"tensor": lax.rem(me + k, 4)} for k in range(1, 4)]
    for peer in peers:
        pl.semaphore_signal(barrier, inc=1, device_id=peer, device_id_type=MESH)
    work()
    pl.semaphore_wait(barrier, len(peers))


def remote(src, dst, send, recv, peer):
    return pltpu.make_async_remote_copy(
        src_ref=src,
        dst_ref=dst,
        send_sem=send,
        recv_sem=recv,
        device_id={"tensor": peer},
        device_id_type=MESH,
    )


def halves_of(rows):
    first = -(-rows // 32) * 16
    return (pl.ds(0, first), pl.ds(first, rows - first))


class Gather:
    def __init__(self, all_ref, rows, send, recv):
        me, side, over, _ = plane()
        low, high = halves_of(rows)
        plan = (
            (me, low, side),
            (me, high, over),
            (me, high, side),
            (me, low, over),
            (side, low, over),
            (over, high, side),
        )
        self.copies = []
        for k, (block, part, peer) in enumerate(plan):
            ref = all_ref.at[block, part]
            self.copies.append(remote(ref, ref, send.at[k], recv.at[k], peer))

    def start(self):
        for made in self.copies[:4]:
            made.start()

    def forward(self):
        for k in range(2):
            self.copies[k].wait_recv()
            self.copies[4 + k].start()

    def arrive(self, first=2, last=6):
        for made in self.copies[first:last]:
            made.wait_recv()

    def finish(self):
        for made in self.copies:
            made.wait_send()


class Scatter:
    def __init__(self, part_ref, rows, slots, send, recv):
        self.me, self.side, self.over, cross = plane()
        self.part_ref = part_ref
        self.own, self.other, self.far, self.passing = slots
        self.halves = low, high = halves_of(rows)
        plan = (
            (part_ref.at[cross, low], self.other.at[low], self.side),
            (part_ref.at[cross, high], self.other.at[high], self.over),
            (part_ref.at[self.side, low], self.own.at[low], self.side),
            (part_ref.at[self.over, high], self.own.at[high], self.over),
            (self.passing.at[low], self.far.at[low], self.over),
            (self.passing.at[high], self.far.at[high], self.side),
        )
        self.copies = [remote(src, dst, send.at[k], recv.at[k], peer) for k, (src, dst, peer) in enumerate(plan)]

    def start(self):
        for made in self.copies[:4]:
            made.start()

    def forward(self):
        for k, (part, block) in enumerate(zip(self.halves, (self.over, self.side))):
            self.copies[k].wait_recv()
            mine = self.part_ref[block, part].astype(F32)
            self.passing[part] = (mine + self.other[part].astype(F32)).astype(BF16)
            self.copies[4 + k].start()

    def arrive(self):
        for made in self.copies[2:]:
            made.wait_recv()

    def total(self, rows):
        return (
            self.part_ref[self.me, rows].astype(F32) + self.own[rows].astype(F32) + self.far[rows].astype(F32)
        )

    def finish(self):
        for made in self.copies:
            made.wait_send()


STEPS = 6


def sems(*shape):
    return [pltpu.SemaphoreType.DMA(shape), pltpu.SemaphoreType.DMA(shape)]


def params(cid):
    return pltpu.CompilerParams(collective_id=cid, has_side_effects=True, vmem_limit_bytes=67043328)


def lanes(width):
    return -(-width // 128) * 128


def pad_rows(rows):
    return -(-rows // 16) * 16


def clear_pads(ref, rows):
    full = ref.shape[1]
    for b in range(ref.shape[0]):
        ref[b, rows:full] = jnp.zeros((full - rows, ref.shape[2]), ref.dtype)


def at_row(ref):
    return ref[...].reshape(1, -1)


def for_image(i, images, act):
    for k in range(images):
        pl.when(i == k)(functools.partial(act, k))


def key_bias(mask, rows, full, seq):
    length = jnp.sum(mask.astype(F32), axis=1, keepdims=True).astype(jnp.int32)
    at = lax.broadcasted_iota(jnp.int32, (seq, 128 - HD), 0)
    lane = lax.broadcasted_iota(jnp.int32, (seq, 128 - HD), 1)
    block = sum((at >= b * full).astype(jnp.int32) for b in range(1, seq // full))
    inner = at - block * full
    good = (inner < rows) & (inner + block * rows < length)
    bias = jnp.where(good, 0.0, -1e30)
    ones = jnp.where(lane == 0, 1.0, 0.0)
    return (jnp.where(lane == 0, bias, 0.0).astype(BF16), ones.astype(BF16))


def soft_open(keys_in, queries, factor):
    raw = dot(keys_in, queries, NT)
    top = jnp.max(raw, axis=0, keepdims=True)
    grown = jnp.exp2((raw - top) * factor)
    total = jnp.sum(grown, axis=0, keepdims=True)
    return grown * (1.0 / total)


def block_of(ref, block, groups):
    if len(ref.shape) == 3:
        return ref.at[block]
    depth = ref.shape[0] // groups
    return ref.at[pl.ds(pl.multiple_of(block * depth, 16), depth)]


def over_dp(src, dst, send, recv, peer):
    return pltpu.make_async_remote_copy(
        src_ref=src, dst_ref=dst, send_sem=send, recv_sem=recv, device_id={"dp": peer}, device_id_type=MESH
    )


class Spread:
    def __init__(self, groups, all_ref, send, recv):
        row = lax.axis_index("dp")
        twin = row + 1 - 2 * lax.rem(row, 2)
        half = groups // 2
        chip = lax.div(row, 2)
        self.relayed = half == 4
        self.out, self.back = [], []
        for k in range(half):
            came = block_of(all_ref, lax.rem(row + groups - 2 * k, groups), groups)
            self.back.append(over_dp(came, came, send.at[half + k], recv.at[half + k], twin))
            if k > 0:
                mine = block_of(all_ref, row, groups)
                self.out.append(over_dp(mine, mine, send.at[k], recv.at[k], lax.rem(row + 2 * k, groups)))
        self.asked = {}
        if self.relayed:
            self.asked = {0: chip != 3, 2: chip != 0}
            self.inner = (chip == 1) | (chip == 2)
            up = lax.div(chip, 2)
            came = block_of(all_ref, lax.rem(row + 4, groups), groups)
            self.relay = over_dp(came, came, send.at[0], recv.at[1 + 2 * up], row + 4 * up - 2)

    def where(self, k, act):
        if k in self.asked:
            pl.when(self.asked[k])(act)
        else:
            act()

    def start(self):
        for k in (1, 0, 2) if self.relayed else range(len(self.out)):
            self.where(k, self.out[k].start)
        self.back[0].start()

    def hop(self):
        if self.relayed:
            self.out[1].wait_recv()
            pl.when(self.inner)(self.relay.start)
            self.back[2].start()

    def forward(self):
        for k, (far, near) in enumerate(zip(self.out, self.back[1:])):
            if k != 1 or not self.relayed:
                far.wait_recv()
                near.start()

    def arrive(self):
        for made in self.back:
            made.wait_recv()

    def finish(self):
        for k, made in enumerate(self.out):
            self.where(k, made.wait_send)
        for made in self.back:
            made.wait_send()
        if self.relayed:
            pl.when(self.inner)(self.relay.wait_send)


class Moves:
    def __init__(self, sem):
        self.sem, self.made = sem, []

    def plan(self, src, dst):
        made = pltpu.make_async_copy(src, dst, self.sem.at[len(self.made)])
        self.made.append(made)
        return made

    def start(self, src, dst):
        made = self.plan(src, dst)
        made.start()
        return made

    def finish(self):
        for made in self.made:
            made.wait()


class Reduce:
    def __init__(self, groups, grad_ref, twin_ref, far_ref, tsend, trecv, fsend, frecv):
        self.grad_ref = grad_ref
        depth = grad_ref.shape[0] // groups
        if far_ref is None:
            near, first = twin_ref, depth * (groups // 2)
            self.twin = lambda slot: near.at[pl.ds(pl.multiple_of(slot * depth, 16), depth)]
            self.far = [near.at[pl.ds(first + k * depth, depth)] for k in range(groups // 2 - 1)]
        else:
            self.twin = lambda slot: twin_ref.at[slot]
            self.far = [far_ref.at[k] for k in range(groups // 2 - 1)]
        rows = lambda block: pl.ds(pl.multiple_of(block * depth, 16), depth)
        row = lax.axis_index("dp")
        core = lax.rem(row, 2)
        self.kept, self.mine = self.twin(lax.div(row, 2)), rows(row)
        self.near, self.away = [], []
        for k in range(groups // 2):
            theirs = grad_ref.at[rows(2 * k + 1 - core)]
            self.near.append(over_dp(theirs, self.twin(k), tsend.at[k], trecv.at[k], row + 1 - 2 * core))
        for k in range(1, groups // 2):
            peer = lax.rem(row + 2 * k, groups)
            slot = lax.div(peer, 2)
            held = self.twin(slot)
            made = over_dp(held, self.far[k - 1], fsend.at[k], frecv.at[k], peer)
            self.away.append((held, rows(peer), made))

    def start(self):
        for made in self.near:
            made.start()

    def pair(self):
        for made in self.near:
            made.wait_recv()
        for held, part, made in self.away:
            held[...] = (held[...].astype(F32) + self.grad_ref[part].astype(F32)).astype(BF16)
            made.start()

    def total(self):
        value = self.kept[...].astype(F32) + self.grad_ref[self.mine].astype(F32)
        for (_, _, made), came in zip(self.away, self.far):
            made.wait_recv()
            value = value + came[...].astype(F32)
        return value

    def finish(self):
        for made in self.near + [made for _, _, made in self.away]:
            made.wait_send()


def reduce_scratch(groups, depth, width):
    half, width = groups // 2, lanes(width)
    return [pltpu.VMEM((half, depth, width), BF16), pltpu.VMEM((half - 1, depth, width), BF16)] + sems(half) * 2


def outer(out_ref, left_ref, right_ref, width, first=0):
    images, blocks, full, model = left_ref.shape
    count = images * blocks * full
    tile = 384

    def part(c, _):
        at = pl.ds(pl.multiple_of(c * tile, tile), tile)
        left = left_ref[:, :, :, at].reshape(count, tile)
        right = right_ref[:, :, :, :width].reshape(count, width)
        out_ref[at, first : first + width] = dot(left, right, TN).astype(BF16)
        return 0

    lax.fori_loop(0, model // tile, part, 0)


def whole_body(
    groups, rows, heads,
    x_ref, grad_ref, mask_ref, gain_one, bias_one, bias_out, gain_two, bias_two, bias_down, qv_ref, hb_ref,
    wq_ref, wo_ref, wh_ref, wd_ref,
    one_out, block_out, gin_out, gwq_ref, gwo_ref, gwh_ref, gwd_ref, both_ref,
    one_ref, full_ref, two_ref, hidden_ref, qh, kh, vh, mixed_ref, wq_all, wo_all, wh_all, wd_all,
    gq, part_ref, ghid_ref, act_ref, gpl_ref, gwh_part, gwd_part, slots, osem,
    dtwin, daway, dtsend, dtrecv, dfsend, dfrecv,
    htwin, haway, htsend, htrecv, hfsend, hfrecv,
    qtsend, qtrecv, qfsend, qfrecv,
    gsend, grecv, wsend, wrecv,
    hsum, bsum, mid, row_in, flat_in, vsend, vrecv,
):
    images = x_ref.shape[0]
    _, _, full, model = one_ref.shape
    units = hb_ref.shape[0]
    seq = 4 * full
    width = heads * HD
    last = images - 1
    me, side, over, _ = plane()
    mine = lax.axis_index("dp")
    wq_all[mine, :, 3 * width :] = jnp.zeros_like(wq_all[mine, :, 3 * width :])
    for c in range(3):
        wq_all[mine, :, c * width : (c + 1) * width] = wq_ref[c]
    weights = [Spread(groups, wq_all, wsend.at[0], wrecv.at[0])]
    for k, (own, everyone) in enumerate(((wo_ref, wo_all), (wh_ref, wh_all), (wd_ref, wd_all))):
        count = own.shape[1]
        place = block_of(everyone, mine, groups)
        place[:, count:] = jnp.zeros((own.shape[0], everyone.shape[-1] - count), BF16)
        place[:, :count] = own[...]
        weights.append(Spread(groups, everyone, wsend.at[k + 1], wrecv.at[k + 1]))
    wq, wo, wh, wd = weights
    ones, sums, twos, grads, turns, lows, outs, backs = [], [], [], [], [], [], [], []
    for i in range(images):
        for ref in (one_ref, two_ref, full_ref):
            clear_pads(ref.at[i], rows)
        pair = lambda k: (gsend.at[k, i], grecv.at[k, i])
        four = [slots.at[i, k] for k in range(4)]
        spare = [act_ref.at[i, k] for k in range(4)]
        ones.append(Gather(one_ref.at[i], rows, *pair(0)))
        grads.append(Gather(full_ref.at[i], rows, *pair(1)))
        sums.append(Scatter(part_ref.at[i], rows, four, *pair(2)))
        twos.append(Gather(two_ref.at[i], rows, *pair(3)))
        turns.append(Scatter(part_ref.at[i], rows, four, *pair(4)))
        lows.append(Gather(one_ref.at[i], rows, *pair(5)))
        outs.append(Scatter(two_ref.at[i], rows, spare, *pair(6)))
        backs.append(Scatter(part_ref.at[i], rows, four, *pair(7)))
    down = Reduce(groups, gwd_part, dtwin, daway, dtsend, dtrecv, dfsend, dfrecv)
    red_h = Reduce(groups, gwh_part, htwin, haway, htsend, htrecv, hfsend, hfrecv)
    red_q = Reduce(groups, gwd_part, wd_all, None, qtsend, qtrecv, qfsend, qfrecv)
    moves = Moves(osem)
    keep_one = [moves.plan(one_ref.at[i], one_out.at[i]) for i in range(images)]
    take_one = [moves.plan(one_out.at[i], full_ref.at[i]) for i in range(images)]
    take_grad = [moves.plan(grad_ref.at[i], full_ref.at[i, me, pl.ds(0, rows)]) for i in range(images)]
    put_out = [moves.plan(two_ref.at[i, me, pl.ds(0, rows)], block_out.at[i]) for i in range(images)]
    put_gin = [moves.plan(ghid_ref.at[i], gin_out.at[i]) for i in range(images)]

    def enter(i):
        one_ref[i, me, :rows] = norm_forward(x_ref[i].astype(F32), at_row(gain_one), at_row(bias_one))

    for made in take_grad:
        made.start()
    greet_all(groups, lambda: enter(0))
    ones[0].start()
    wq.start()
    for i in range(1, images):
        enter(i)
        ones[i].start()
    for step in (wo, wh, wd):
        step.start()
    hsum[...] = jnp.zeros_like(hsum)
    bsum[...] = jnp.zeros_like(bsum)
    mixed_ref[:, :, :, width:] = jnp.zeros_like(mixed_ref[:, :, :, width:])
    for i in range(images):
        bias, tail = key_bias(mask_ref[i : i + 1], rows, full, seq)
        for h in range(heads):
            kh[i, h, :, HD:] = bias
            vh[i, h, :, HD:] = jnp.zeros_like(bias)
            qh[i, h, :, HD:] = tail
    for step in ones:
        step.forward()
    for made in take_grad:
        made.wait()
    grads[0].start()
    wq.hop()
    wq.forward()
    scale = HD**-0.5
    shift_q, shift_v = qv_ref[0:1], qv_ref[1:2]

    def project(i):
        weight = wq_all[:, :, : 3 * width].reshape(-1, 3 * width)

        def block(b, _):
            at = pl.ds(pl.multiple_of(b * full, 16), full)
            value = dot(one_ref[i, b], weight)
            queries = (value[:, :width] + shift_q).astype(BF16)
            keys_in = value[:, width : 2 * width].astype(BF16)
            values = (value[:, 2 * width :] + shift_v).astype(BF16)
            for h in range(heads):
                here = slice(h * HD, (h + 1) * HD)
                qh[i, h, at, :HD] = queries[:, here]
                kh[i, h, at, :HD] = keys_in[:, here]
                vh[i, h, at, :HD] = values[:, here]
            return 0

        lax.fori_loop(0, 4, block, 0)

    def attend(i):
        def head(h, _):
            probs = soft_open(kh[i, h], qh[i, h], scale * LOG2E)
            gq[h] = dot(vh[i, h, :, :HD].T, probs.astype(BF16)).T.astype(BF16)
            return 0

        lax.fori_loop(0, heads, head, 0, unroll=2)
        for h in range(heads):
            for b in range(4):
                mixed_ref[i, b, :, h * HD : (h + 1) * HD] = gq[h, b * full : (b + 1) * full]

    def combine(i):
        weight = wo_all[:, :, :width].reshape(-1, width)

        def block(b, _):
            part_ref[i, b] = dot(mixed_ref[i, b, :, :width], weight, NT).astype(BF16)
            return 0

        lax.fori_loop(0, 4, block, 0)

    def ready(k):
        ones[k].arrive()
        keep_one[k].start()
        if k == 0:
            wq.arrive()

    def between(k):
        if k == 0:
            wo.hop()
            wo.forward()
            wh.hop()
            wo.arrive()

    def send(k):
        if k > 0:
            sums[k - 1].forward()
        sums[k].start()
        if k == 0:
            grads[0].forward()

    def image(i, _):
        for_image(i, images, ready)
        project(i)
        attend(i)
        for_image(i, images, between)
        combine(i)
        for_image(i, images, send)
        return 0

    lax.fori_loop(0, images, image, 0)

    def settle(i):
        sums[i].arrive()
        hidden = x_ref[i].astype(F32) + sums[i].total(pl.ds(0, rows)) + at_row(bias_out)
        hidden_ref[i] = hidden
        two_ref[i, me, :rows] = norm_forward(hidden, at_row(gain_two), at_row(bias_two))
        twos[i].start()

    for i in range(last):
        settle(i)
    sums[-1].forward()
    wd.hop()
    for i in range(last):
        twos[i].forward()
    settle(last)
    wh.forward()
    wd.forward()
    twos[-1].forward()
    for step in grads[1:]:
        step.start()
    for step in sums + ones:
        step.finish()
    for made in keep_one:
        made.wait()
    wide = lambda ref: ref[:, :units]
    shift = at_row(hb_ref)

    def ascend(i):
        def pair(c, _):
            at = pl.ds(2 * c, 2)
            pre = dot(two_ref[i, at].reshape(2 * full, model), wide(wh_all)) + shift
            value, slope = gelu_both(pre)
            act_ref[i, at, :, :units] = value.astype(BF16).reshape(2, full, units)
            grad_pre = dot(full_ref[i, at].reshape(2 * full, model), wide(wd_all)) * slope
            hsum[...] += jnp.sum(grad_pre, axis=0, keepdims=True)
            low = grad_pre.astype(BF16)
            gpl_ref[i, at, :, :units] = low.reshape(2, full, units)
            part_ref[i, at] = dot(low, wide(wh_all), NT).astype(BF16).reshape(2, full, model)
            return 0

        lax.fori_loop(0, 2, pair, 0)

    def descend(k, _):
        at = pl.ds(2 * lax.rem(k, 2), 2)
        i = lax.div(k, 2)
        part = dot(act_ref[i, at, :, :units].reshape(2 * full, units), wide(wd_all), NT)
        two_ref[i, at] = part.astype(BF16).reshape(2, full, model)
        return 0

    totals = [0.0] * 6

    def add_up(first, terms):
        for k, term in enumerate(terms):
            totals[first + k] = totals[first + k] + jnp.sum(term, axis=0, keepdims=True)

    def settle_back(i):
        turns[i].arrive()
        grad_normed = turns[i].total(pl.ds(0, rows))
        unit, inv_std = norm_stats(hidden_ref[i])
        upper = full_ref[i, me, :rows].astype(F32)
        grad_hidden = upper + norm_backward(grad_normed, unit, inv_std, at_row(gain_two))
        ghid_ref[i] = grad_hidden
        one_ref[i, me, :rows] = grad_hidden.astype(BF16)
        lows[i].start()
        add_up(0, (grad_normed * unit, grad_normed, grad_hidden, upper))

    def ready_back(k):
        twos[k].arrive()
        if k == 0:
            wh.arrive()
            wd.arrive()
        grads[k].arrive()

    def send_back(k):
        if k == 0:
            for step in grads[1:]:
                step.forward()
        if k > 0:
            turns[k - 1].forward()
        turns[k].start()

    def image_back(i, _):
        for_image(i, images, ready_back)
        ascend(i)
        for_image(i, images, send_back)
        return 0

    lax.fori_loop(0, images, image_back, 0)
    for step in weights:
        step.finish()
    gwd_part[:, units:] = jnp.zeros((model, lanes(units) - units), BF16)
    outer(gwd_part, full_ref, act_ref, units)
    down.start()
    for i in range(last):
        settle_back(i)
    turns[-1].forward()
    down.pair()
    gwh_part[:, units:] = jnp.zeros((model, lanes(units) - units), BF16)
    outer(gwh_part, two_ref, gpl_ref, units)
    for i in range(last):
        lows[i].forward()
    for step in twos:
        step.finish()
    lax.fori_loop(0, 2 * images, descend, 0)
    red_h.start()
    settle_back(last)
    red_h.pair()
    for step in turns + grads:
        step.finish()
    for made in take_one:
        made.start()

    def mix(i):
        value = dot(one_ref[i].reshape(seq, model), wo_all[:, :, :width].reshape(model, width)).astype(BF16)
        gpl_ref[i, :, :, 3 * width : 4 * width] = value.reshape(4, full, width)

    def midway(k):
        if k < last:
            lows[k + 1].forward()
        if k > 0:
            backs[k - 1].forward()

    def attend_back(i):
        for h in range(heads):
            if h == heads // 2:
                for_image(i, images, midway)
            here = slice(3 * width + h * HD, 3 * width + (h + 1) * HD)
            queries = qh[i, h]
            grads_in = gpl_ref[i, :, :, here].reshape(seq, HD)
            keys_in = kh[i, h]
            probs = soft_open(keys_in, queries, scale * LOG2E)
            grad_probs = dot(vh[i, h, :, :HD], grads_in, NT)
            grad_values = dot(probs.astype(BF16), grads_in)
            delta = jnp.sum(probs * grad_probs, axis=0, keepdims=True)
            grad_scores = (probs * (grad_probs - delta) * scale).astype(BF16)
            grad_keys = dot(grad_scores, queries[:, :HD])
            grad_queries = dot(keys_in[:, :HD].T, grad_scores).T
            for c, value in enumerate((grad_queries, grad_keys, grad_values)):
                here = slice(c * width + h * HD, c * width + (h + 1) * HD)
                gpl_ref[i, :, :, here] = value.astype(BF16).reshape(4, full, HD)
                bsum[h, c : c + 1] += jnp.sum(value, axis=0, keepdims=True)

    def spread(i):
        def pair(c, _):
            at = pl.ds(2 * c, 2)
            left = gpl_ref[i, at, :, : 3 * width].reshape(2 * full, 3 * width)
            part = dot(left, wq_all[:, :, : 3 * width].reshape(model, 3 * width), NT)
            part_ref[i, at] = part.astype(BF16).reshape(2, full, model)
            return 0

        lax.fori_loop(0, 2, pair, 0)

    def ready_last(k):
        lows[k].arrive(4 if k > 0 else 2)

    def send_last(k):
        backs[k].start()
        if k < last:
            lows[k + 1].arrive(2, 4)
            outs[k].start()
        else:
            outs[k - 1].forward()

    def image_last(i, _):
        for_image(i, images, ready_last)
        mix(i)
        attend_back(i)
        spread(i)
        for_image(i, images, send_last)
        return 0

    lax.fori_loop(0, images, image_last, 0)
    gwd_ref[...] = down.total()[:, :units]
    down.finish()
    outer(gwd_part, one_ref, mixed_ref, width, 3 * width)
    for made in take_one:
        made.wait()
    outer(gwd_part, full_ref, gpl_ref, 3 * width)
    red_q.start()

    def settle_last(i):
        backs[i].arrive()
        grad_normed = backs[i].total(pl.ds(0, rows))
        unit, inv_std = norm_stats(x_ref[i].astype(F32))
        ghid_ref[i] = ghid_ref[i] + norm_backward(grad_normed, unit, inv_std, at_row(gain_one))
        put_gin[i].start()
        add_up(4, (grad_normed * unit, grad_normed))

    def finish_out(i):
        outs[i].arrive()
        value = hidden_ref[i] + outs[i].total(pl.ds(0, rows)) + at_row(bias_down)
        two_ref[i, me, :rows] = value.astype(BF16)
        put_out[i].start()

    for i in range(last):
        settle_last(i)
    backs[-1].forward()
    outs[-1].start()
    gwh_ref[...] = red_h.total()[:, :units]
    red_q.pair()
    mid[0] = jnp.zeros_like(mid[0])
    for h in range(heads):
        for c in range(3):
            mid[0, 6:7, c * width + h * HD : c * width + (h + 1) * HD] = bsum[h, c : c + 1]
    mid[0, 7:8, :units] = hsum[...]
    settle_last(last)

    for k in range(6):
        mid[0, k : k + 1] = totals[k]
    row_in[mine] = mid[0]
    aways = []
    for k in range(1, groups):
        aways.append(over_dp(mid.at[0], row_in.at[mine], vsend.at[k], vrecv.at[k], lax.rem(mine + k, groups)))
        aways[-1].start()
    outs[-1].forward()
    for made in aways:
        made.wait()
    held = row_in[0]
    for k in range(1, groups):
        held = held + row_in[k]
    mid[1] = held
    flat_in[me] = mid[1]
    planes = []
    for k in range(1, 4):
        at = groups + k
        planes.append(remote(mid.at[1], flat_in.at[me], vsend.at[at], vrecv.at[at], lax.rem(me + k, 4)))
        planes[-1].start()
    for i in range(last):
        finish_out(i)
    for made in planes:
        made.wait()
    both_ref[0:6] = (flat_in[0] + flat_in[1] + flat_in[2] + flat_in[3])[0:6]
    both_ref[6:8] = mid[1, 6:8]
    finish_out(last)
    total = red_q.total()
    for c in range(3):
        gwq_ref[c] = total[:, c * width : (c + 1) * width]
    gwo_ref[...] = total[:, 3 * width : 4 * width]
    for step in lows + outs + backs + [red_h, red_q]:
        step.finish()
    for made in put_out + put_gin:
        made.wait()


def whole(groups, block_input, grad_out, key_mask, vectors, qv_bias, bias, wq, wo, wh, wd):
    images, rows, model = block_input.shape
    full = pad_rows(rows)
    width = wo.shape[1]
    units = wh.shape[1]
    heads = width // HD
    seq = 4 * full
    depth = wo.shape[0]
    blocks = ((images, 4, full, model), BF16)
    own = ((images, rows, model), F32)
    heads_wide = ((images, heads, seq, 128), BF16)
    piece = ((heads, seq, HD), BF16)
    square = ((model, lanes(units)), BF16)
    weight = lambda count: ((groups, depth, lanes(count)), BF16)
    outs = [blocks, (block_input.shape, BF16), own]
    more = [((3, depth, width), F32), ((depth, width), F32), ((depth, units), F32), ((depth, units), F32), ((8, model), F32)]
    held = [blocks, blocks, blocks, own, heads_wide, heads_wide, heads_wide, ((images, 4, full, lanes(width)), BF16)]
    held += [weight(3 * width), weight(width), square, square]
    held += [piece, blocks, own, blocks, blocks, square, square, blocks]
    return pl.pallas_call(
        functools.partial(whole_body, groups, rows, heads),
        out_shape=tuple(jax.ShapeDtypeStruct(*h) for h in outs + more),
        in_specs=[VMEM, ANY] + [VMEM] * 13,
        out_specs=(ANY,) * len(outs) + (VMEM,) * len(more),
        scratch_shapes=[pltpu.VMEM(*h) for h in held]
        + [pltpu.SemaphoreType.DMA((5 * images,))]
        + reduce_scratch(groups, depth, units) * 2
        + sems(groups // 2) * 2
        + sems(8, images, STEPS)
        + sems(4, groups)
        + [
            pltpu.VMEM((1, units), F32),
            pltpu.VMEM((heads, 3, HD), F32),
            pltpu.VMEM((2, 8, model), F32),
            pltpu.VMEM((groups, 8, model), F32),
            pltpu.VMEM((4, 8, model), F32),
        ]
        + sems(groups + 4),
        compiler_params=params(0),
        name="whole",
    )(block_input, grad_out, key_mask, *vectors, qv_bias, bias, wq, wo, wh, wd)


def deliver_body(width, out, gin, gwq, gwo, gwh, gwd, both, *refs):
    refs, held, lsem, ssem = refs[:14], refs[14:20], refs[20], refs[21]
    loads, stores = Moves(lsem), Moves(ssem)
    sources = (out, gin, gwq, gwo, gwh, gwd)
    got = [loads.start(src, mid) for src, mid in zip(sources, held)]
    qv, unit = refs[6:8]
    qv[0:1] = both[6:7, :width]
    qv[1:2] = both[6:7, 2 * width : 3 * width]
    unit[...] = both[7, : unit.shape[0]]
    for k, dst in enumerate(refs[8:]):
        dst[...] = both[k]
    for made, mid, dst in zip(got, held, refs):
        made.wait()
        stores.start(mid, dst)
    stores.finish()


def deliver(width, units, out, gin, gwq, gwo, gwh, gwd, both):
    model = both.shape[1]
    same = [jax.ShapeDtypeStruct(v.shape, v.dtype) for v in (out, gin, gwq, gwo, gwh, gwd)]
    more = [jax.ShapeDtypeStruct(dims, F32) for dims in ((2, width), (units,)) + ((model,),) * 6]
    return pl.pallas_call(
        functools.partial(deliver_body, width),
        out_shape=tuple(same + more),
        in_specs=[ANY] * 6 + [VMEM],
        out_specs=(ANY,) * 6 + (VMEM,) * 8,
        scratch_shapes=[pltpu.VMEM(v.shape, v.dtype) for v in same]
        + [pltpu.SemaphoreType.DMA((6,)), pltpu.SemaphoreType.DMA((6,))],
        compiler_params=pltpu.CompilerParams(vmem_limit_bytes=60 << 20),
        name="deliver",
    )(out, gin, gwq, gwo, gwh, gwd, both)


def gather_rows(rows):
    return lax.all_gather(rows, "tensor", axis=1, tiled=True)


def scatter_rows(part):
    return lax.psum_scatter(part, "tensor", scatter_dimension=1, tiled=True).astype(F32)


def shards(
    groups,
    ranks,
    block_input,
    key_mask,
    attn_norm_gain,
    attn_norm_bias,
    qkv_weight,
    qv_bias,
    out_weight,
    out_bias,
    mlp_norm_gain,
    mlp_norm_bias,
    hidden_weight,
    hidden_bias,
    down_weight,
    down_bias,
    grad_out,
):
    images, rows, model = block_input.shape
    flat = ranks == 4 and images == 2 and groups > 2 and groups % 2 == 0 and hidden_weight.shape[1] <= model and 4 * qkv_weight.shape[2] == lanes(hidden_weight.shape[1])
    seq = key_mask.shape[1]
    width = qkv_weight.shape[2]
    units = hidden_weight.shape[1]

    def weight(shard):
        return lax.all_gather(shard, "dp", axis=0, tiled=True)

    def owned(grad):
        return lax.psum_scatter(grad.astype(BF16), "dp", scatter_dimension=0, tiled=True).astype(F32)

    out_rows, down_rows = out_weight.T, down_weight.T
    if flat:
        _, block_output, grad_input, grad_qkv_w, grad_out_w, grad_hidden_w, grad_down_w, both = whole(
            groups,
            block_input,
            grad_out,
            key_mask,
            (attn_norm_gain, attn_norm_bias, out_bias, mlp_norm_gain, mlp_norm_bias, down_bias),
            qv_bias,
            hidden_bias,
            qkv_weight.transpose(1, 0, 2),
            out_rows,
            hidden_weight,
            down_rows,
        )
        (
            block_output, grad_input, grad_qkv_w, grad_out_w, grad_hidden_w, grad_down_w, grad_qv, grad_hidden_b, *both
        ) = deliver(
            width, units, block_output, grad_input, grad_qkv_w, grad_out_w, grad_hidden_w, grad_down_w, both
        )
        grad_qkv_w = grad_qkv_w.transpose(1, 0, 2)
        grad_out_w, grad_down_w = grad_out_w.T, grad_down_w.T
    else:
        qkv_rows = qkv_weight.reshape(-1, 3 * width)
        shift = jnp.concatenate([qv_bias[0], jnp.zeros_like(qv_bias[0]), qv_bias[1]])
        hidden_all, down_all = weight(hidden_weight), weight(down_rows)
        qkv_all, out_all = weight(qkv_rows), weight(out_rows)
        lens = jnp.sum(key_mask, axis=1)
        in_float = block_input.astype(F32)
        normed_one = gather_rows(norm_forward(in_float, attn_norm_gain, attn_norm_bias))
        grad_full = gather_rows(grad_out)
        proj = jnp.einsum("isd,df->isf", normed_one, qkv_all, preferred_element_type=F32) + shift
        proj = proj.astype(BF16)
        mixed = attend_forward(lens, proj)
        attn_part = jnp.einsum("isf,df->isd", mixed, out_all, preferred_element_type=F32).astype(BF16)
        hidden_res = in_float + scatter_rows(attn_part) + out_bias
        normed_two = gather_rows(norm_forward(hidden_res, mlp_norm_gain, mlp_norm_bias))
        pre_act = jnp.einsum("isd,df->isf", normed_two, hidden_all, preferred_element_type=F32) + hidden_bias
        value, slope = gelu_both(pre_act)
        activated = value.astype(BF16)
        grad_act = jnp.einsum("isd,df->isf", grad_full, down_all, preferred_element_type=F32)
        grad_pre = grad_act * slope
        grad_hidden_b = jnp.sum(grad_pre, axis=(0, 1))
        grad_pre_low = grad_pre.astype(BF16)
        gpart = jnp.einsum("isf,df->isd", grad_pre_low, hidden_all, preferred_element_type=F32).astype(BF16)
        mpart = jnp.einsum("isf,df->isd", activated, down_all, preferred_element_type=F32).astype(BF16)
        block_output = (hidden_res + scatter_rows(mpart) + down_bias).astype(BF16)
        grad_float = grad_out.astype(F32)
        grad_normed = scatter_rows(gpart)
        unit, inv_std = norm_stats(hidden_res)
        grad_hidden = grad_float + norm_backward(grad_normed, unit, inv_std, mlp_norm_gain)
        hidden_full = gather_rows(grad_hidden.astype(BF16))
        mlp_sums = jnp.stack(
            [jnp.sum(v, axis=(0, 1)) for v in (grad_normed * unit, grad_normed, grad_hidden, grad_float)]
        )
        grad_hidden_w = owned(jnp.einsum("isd,isf->df", normed_two, grad_pre_low, preferred_element_type=F32))
        grad_down_w = owned(jnp.einsum("isd,isf->df", grad_full, activated, preferred_element_type=F32)).T
        grad_mixed = jnp.einsum("isd,df->isf", hidden_full, out_all, preferred_element_type=F32).astype(BF16)
        grad_proj, proj_sums = attend_backward(lens, proj, grad_mixed)
        proj_sums = jnp.sum(proj_sums, axis=(0, 1))
        npart = jnp.einsum("isf,df->isd", grad_proj, qkv_all, preferred_element_type=F32).astype(BF16)
        grad_out_w = owned(jnp.einsum("isd,isf->df", hidden_full, mixed, preferred_element_type=F32)).T
        grad_qkv_w = owned(jnp.einsum("isd,isf->df", normed_one, grad_proj, preferred_element_type=F32))
        grad_normed = scatter_rows(npart)
        unit, inv_std = norm_stats(in_float)
        grad_input = grad_hidden + norm_backward(grad_normed, unit, inv_std, attn_norm_gain)
        attn_sums = jnp.stack([jnp.sum(v, axis=(0, 1)) for v in (grad_normed * unit, grad_normed)])
        both = lax.psum(jnp.concatenate([mlp_sums, attn_sums]), ("dp", "tensor"))
        proj_sums, grad_hidden_b = lax.psum((proj_sums, grad_hidden_b), "dp")
        grad_qv = jnp.stack([proj_sums[:width], proj_sums[2 * width :]])
        grad_qkv_w = grad_qkv_w.reshape(-1, 3, width)
    return (
        block_output,
        grad_input,
        both[4],
        both[5],
        grad_qkv_w,
        grad_qv,
        grad_out_w,
        both[2],
        both[0],
        both[1],
        grad_hidden_w,
        grad_hidden_b,
        grad_down_w,
        both[3],
    )


def solution(mesh):
    return jax.shard_map(
        functools.partial(shards, mesh.shape["dp"], mesh.shape["tensor"]),
        mesh=mesh,
        in_specs=(
            P("dp", "tensor", None),
            P("dp", None),
            P(),
            P(),
            P("dp", None, "tensor"),
            P(None, "tensor"),
            P("tensor", "dp"),
            P(),
            P(),
            P(),
            P("dp", "tensor"),
            P("tensor"),
            P("tensor", "dp"),
            P(),
            P("dp", "tensor", None),
        ),
        out_specs=(
            P("dp", "tensor", None),
            P("dp", "tensor", None),
            P(),
            P(),
            P("dp", None, "tensor"),
            P(None, "tensor"),
            P("tensor", "dp"),
            P(),
            P(),
            P(),
            P("dp", "tensor"),
            P("tensor"),
            P("tensor", "dp"),
            P(),
        ),
        check_vma=False,
    )
```

```python
import functools
import math

import jax
import jax.numpy as jnp
from jax import lax
from jax.experimental import pallas as pl
from jax.experimental.pallas import tpu as pltpu
from jax.sharding import PartitionSpec as P

HD = 72
CHUNK = 768
F32 = jnp.float32
BF16 = jnp.bfloat16
LOG2E = math.log2(math.e)
NN = (((1,), (0,)), ((), ()))
NT = (((1,), (1,)), ((), ()))
TN = (((0,), (0,)), ((), ()))
MESH = pl.DeviceIdType.MESH
ANY = pl.BlockSpec(memory_space=pl.ANY)
VMEM = pl.BlockSpec(memory_space=pltpu.VMEM)
SMEM = pl.BlockSpec(memory_space=pltpu.SMEM)


layer_eps = 1e-06
gelu_root = math.sqrt(2.0 / math.pi)
gelu_cubic = 0.044715


def norm_stats(rows):
    center = rows - jnp.mean(rows, axis=-1, keepdims=True)
    inv_std = lax.rsqrt(jnp.mean(center * center, axis=-1, keepdims=True) + layer_eps)
    return (center * inv_std, inv_std)


def norm_forward(rows, gain, shift):
    unit, _ = norm_stats(rows)
    return (unit * gain + shift).astype(BF16)


def norm_backward(grad_normed, unit, inv_std, gain):
    scaled = grad_normed * gain
    return inv_std * (
        scaled
        - jnp.mean(scaled, axis=-1, keepdims=True)
        - unit * jnp.mean(scaled * unit, axis=-1, keepdims=True)
    )


def gelu_both(pre):
    tangent = jnp.tanh(gelu_root * (pre + gelu_cubic * pre * pre * pre))
    value = 0.5 * pre * (1.0 + tangent)
    slope = 0.5 * (1.0 + tangent) + 0.5 * pre * (1.0 - tangent * tangent) * gelu_root * (
        1.0 + 3.0 * gelu_cubic * pre * pre
    )
    return (value, slope)


def dot(a, b, dims=NN):
    return lax.dot_general(a, b, dims, preferred_element_type=F32)


def soft_columns(keys_in, queries, row_ok, factor):
    raw = jnp.where(row_ok, dot(keys_in, queries, NT), -1e30)
    top = jnp.max(raw, axis=0, keepdims=True)
    grown = jnp.exp2((raw - top) * factor)
    total = jnp.sum(grown, axis=0, keepdims=True)
    return grown * (1.0 / total)


def attend_forward_body(seq, heads, lens_ref, proj_ref, mixed_ref, qh, kh, vh, oh):
    width = heads * HD
    padded = qh.shape[1]
    for h in range(heads):
        qh[h, :seq] = proj_ref[0, :, h * HD : (h + 1) * HD]
        qh[h, seq:] = jnp.zeros((padded - seq, HD), BF16)
        kh[h] = proj_ref[0, :, width + h * HD : width + (h + 1) * HD]
        vh[h] = proj_ref[0, :, 2 * width + h * HD : 2 * width + (h + 1) * HD].T
    length = lens_ref[pl.program_id(0)]
    factor = HD**-0.5 * LOG2E

    def head(h, _):
        def chunk(c, _):
            row_ok = lax.broadcasted_iota(jnp.int32, (seq, CHUNK), 0) < length
            at = pl.ds(pl.multiple_of(c * CHUNK, CHUNK), CHUNK)
            probs = soft_columns(kh[h], qh[h, at], row_ok, factor)
            oh[h, at] = dot(vh[h], probs.astype(BF16)).T.astype(BF16)
            return 0

        return lax.fori_loop(0, padded // CHUNK, chunk, 0)

    lax.fori_loop(0, heads, head, 0)
    for h in range(heads):
        mixed_ref[0, :, h * HD : (h + 1) * HD] = oh[h, :seq]


def attend_forward(lens, proj):
    images, seq, triple = proj.shape
    heads = triple // (3 * HD)
    padded = -(-seq // CHUNK) * CHUNK
    return pl.pallas_call(
        functools.partial(attend_forward_body, seq, heads),
        out_shape=jax.ShapeDtypeStruct((images, seq, heads * HD), BF16),
        grid=(images,),
        in_specs=[SMEM, pl.BlockSpec((1, seq, triple), lambda i: (i, 0, 0))],
        out_specs=pl.BlockSpec((1, seq, heads * HD), lambda i: (i, 0, 0)),
        scratch_shapes=[
            pltpu.VMEM((heads, padded, HD), BF16),
            pltpu.VMEM((heads, seq, HD), BF16),
            pltpu.VMEM((heads, HD, seq), BF16),
            pltpu.VMEM((heads, padded, HD), BF16),
        ],
        name="attend_forward",
    )(lens, proj)


def attend_backward_body(
    seq, heads, lens_ref, proj_ref, gmix_ref, gproj_ref, gbias_ref, qh, kh, kt, vh, gh, gq, gk, gv
):
    width = heads * HD
    padded = qh.shape[1]
    for h in range(heads):
        qh[h, :seq] = proj_ref[0, :, h * HD : (h + 1) * HD]
        qh[h, seq:] = jnp.zeros((padded - seq, HD), BF16)
        gh[h, :seq] = gmix_ref[0, :, h * HD : (h + 1) * HD]
        gh[h, seq:] = jnp.zeros((padded - seq, HD), BF16)
        keys_in = proj_ref[0, :, width + h * HD : width + (h + 1) * HD]
        kh[h] = keys_in
        kt[h] = keys_in.T
        vh[h] = proj_ref[0, :, 2 * width + h * HD : 2 * width + (h + 1) * HD]
    length = lens_ref[pl.program_id(0)]
    scale = HD**-0.5
    factor = scale * LOG2E

    def head(h, _):
        gk[h] = jnp.zeros((seq, HD), F32)
        gv[h] = jnp.zeros((seq, HD), F32)

        def chunk(c, _):
            row_ok = lax.broadcasted_iota(jnp.int32, (seq, CHUNK), 0) < length
            at = pl.ds(pl.multiple_of(c * CHUNK, CHUNK), CHUNK)
            queries = qh[h, at]
            grads = gh[h, at]
            probs = soft_columns(kh[h], queries, row_ok, factor)
            grad_probs = dot(vh[h], grads, NT)
            gv[h] += dot(probs.astype(BF16), grads)
            delta = jnp.sum(probs * grad_probs, axis=0, keepdims=True)
            grad_scores = (probs * (grad_probs - delta) * scale).astype(BF16)
            gk[h] += dot(grad_scores, queries)
            gq[h, at] = dot(kt[h], grad_scores).T
            return 0

        return lax.fori_loop(0, padded // CHUNK, chunk, 0)

    lax.fori_loop(0, heads, head, 0)
    for h in range(heads):
        for c, held in enumerate((gq, gk, gv)):
            value = held[h, :seq]
            at = slice(c * width + h * HD, c * width + (h + 1) * HD)
            gproj_ref[0, :, at] = value.astype(BF16)
            gbias_ref[0, :, at] = jnp.sum(value, axis=0, keepdims=True)


def attend_backward(lens, proj, gmix):
    images, seq, triple = proj.shape
    heads = triple // (3 * HD)
    padded = -(-seq // CHUNK) * CHUNK
    return pl.pallas_call(
        functools.partial(attend_backward_body, seq, heads),
        out_shape=(
            jax.ShapeDtypeStruct((images, seq, triple), BF16),
            jax.ShapeDtypeStruct((images, 1, triple), F32),
        ),
        grid=(images,),
        in_specs=[
            SMEM,
            pl.BlockSpec((1, seq, triple), lambda i: (i, 0, 0)),
            pl.BlockSpec((1, seq, heads * HD), lambda i: (i, 0, 0)),
        ],
        out_specs=(
            pl.BlockSpec((1, seq, triple), lambda i: (i, 0, 0)),
            pl.BlockSpec((1, 1, triple), lambda i: (i, 0, 0)),
        ),
        scratch_shapes=[
            pltpu.VMEM((heads, padded, HD), BF16),
            pltpu.VMEM((heads, seq, HD), BF16),
            pltpu.VMEM((heads, HD, seq), BF16),
            pltpu.VMEM((heads, seq, HD), BF16),
            pltpu.VMEM((heads, padded, HD), BF16),
            pltpu.VMEM((heads, padded, HD), F32),
            pltpu.VMEM((heads, seq, HD), F32),
            pltpu.VMEM((heads, seq, HD), F32),
        ],
        name="attend_backward",
    )(lens, proj, gmix)


def plane():
    me = lax.axis_index("tensor")
    side = me + 1 - 2 * lax.rem(me, 2)
    over = lax.rem(me + 2, 4)
    return (me, side, over, lax.rem(side + 2, 4))


def greet(peers):
    barrier = pltpu.get_barrier_semaphore()
    for peer in peers:
        pl.semaphore_signal(barrier, inc=1, device_id={"tensor": peer}, device_id_type=MESH)
    pl.semaphore_wait(barrier, len(peers))


def greet_all(groups, work):
    row, me = lax.axis_index("dp"), lax.axis_index("tensor")
    barrier = pltpu.get_barrier_semaphore()
    peers = [{"dp": lax.rem(row + k, groups)} for k in range(1, groups)]
    peers += [{"tensor": lax.rem(me + k, 4)} for k in range(1, 4)]
    for peer in peers:
        pl.semaphore_signal(barrier, inc=1, device_id=peer, device_id_type=MESH)
    work()
    pl.semaphore_wait(barrier, len(peers))


def remote(src, dst, send, recv, peer):
    return pltpu.make_async_remote_copy(
        src_ref=src,
        dst_ref=dst,
        send_sem=send,
        recv_sem=recv,
        device_id={"tensor": peer},
        device_id_type=MESH,
    )


def halves_of(rows):
    first = -(-rows // 32) * 16
    return (pl.ds(0, first), pl.ds(first, rows - first))


class Gather:
    def __init__(self, all_ref, rows, send, recv):
        me, side, over, _ = plane()
        low, high = halves_of(rows)
        plan = (
            (me, low, side),
            (me, high, over),
            (me, high, side),
            (me, low, over),
            (side, low, over),
            (over, high, side),
        )
        self.copies = []
        for k, (block, part, peer) in enumerate(plan):
            ref = all_ref.at[block, part]
            self.copies.append(remote(ref, ref, send.at[k], recv.at[k], peer))

    def start(self):
        for made in self.copies[:4]:
            made.start()

    def forward(self):
        for k in range(2):
            self.copies[k].wait_recv()
            self.copies[4 + k].start()

    def arrive(self, first=2, last=6):
        for made in self.copies[first:last]:
            made.wait_recv()

    def finish(self):
        for made in self.copies:
            made.wait_send()


class Scatter:
    def __init__(self, part_ref, rows, slots, send, recv):
        self.me, self.side, self.over, cross = plane()
        self.part_ref = part_ref
        self.own, self.other, self.far, self.passing = slots
        self.halves = low, high = halves_of(rows)
        plan = (
            (part_ref.at[cross, low], self.other.at[low], self.side),
            (part_ref.at[cross, high], self.other.at[high], self.over),
            (part_ref.at[self.side, low], self.own.at[low], self.side),
            (part_ref.at[self.over, high], self.own.at[high], self.over),
            (self.passing.at[low], self.far.at[low], self.over),
            (self.passing.at[high], self.far.at[high], self.side),
        )
        self.copies = [remote(src, dst, send.at[k], recv.at[k], peer) for k, (src, dst, peer) in enumerate(plan)]

    def start(self):
        for made in self.copies[:4]:
            made.start()

    def forward(self):
        for k, (part, block) in enumerate(zip(self.halves, (self.over, self.side))):
            self.copies[k].wait_recv()
            mine = self.part_ref[block, part].astype(F32)
            self.passing[part] = (mine + self.other[part].astype(F32)).astype(BF16)
            self.copies[4 + k].start()

    def arrive(self):
        for made in self.copies[2:]:
            made.wait_recv()

    def total(self, rows):
        return (
            self.part_ref[self.me, rows].astype(F32) + self.own[rows].astype(F32) + self.far[rows].astype(F32)
        )

    def finish(self):
        for made in self.copies:
            made.wait_send()


STEPS = 6


def sems(*shape):
    return [pltpu.SemaphoreType.DMA(shape), pltpu.SemaphoreType.DMA(shape)]


def params(cid):
    return pltpu.CompilerParams(collective_id=cid, has_side_effects=True, vmem_limit_bytes=67043328)


def lanes(width):
    return -(-width // 128) * 128


def pad_rows(rows):
    return -(-rows // 16) * 16


def clear_pads(ref, rows):
    full = ref.shape[1]
    for b in range(ref.shape[0]):
        ref[b, rows:full] = jnp.zeros((full - rows, ref.shape[2]), ref.dtype)


def at_row(ref):
    return ref[...].reshape(1, -1)


def for_image(i, images, act):
    for k in range(images):
        pl.when(i == k)(functools.partial(act, k))


def key_bias(mask, rows, full, seq):
    length = jnp.sum(mask.astype(F32), axis=1, keepdims=True).astype(jnp.int32)
    at = lax.broadcasted_iota(jnp.int32, (seq, 128 - HD), 0)
    lane = lax.broadcasted_iota(jnp.int32, (seq, 128 - HD), 1)
    block = sum((at >= b * full).astype(jnp.int32) for b in range(1, seq // full))
    inner = at - block * full
    good = (inner < rows) & (inner + block * rows < length)
    bias = jnp.where(good, 0.0, -1e30)
    ones = jnp.where(lane == 0, 1.0, 0.0)
    return (jnp.where(lane == 0, bias, 0.0).astype(BF16), ones.astype(BF16))


def soft_open(keys_in, queries, factor):
    raw = dot(keys_in, queries, NT)
    top = jnp.max(raw, axis=0, keepdims=True)
    grown = jnp.exp2((raw - top) * factor)
    total = jnp.sum(grown, axis=0, keepdims=True)
    return grown * (1.0 / total)


def block_of(ref, block, groups):
    if len(ref.shape) == 3:
        return ref.at[block]
    depth = ref.shape[0] // groups
    return ref.at[pl.ds(pl.multiple_of(block * depth, 16), depth)]


def over_dp(src, dst, send, recv, peer):
    return pltpu.make_async_remote_copy(
        src_ref=src, dst_ref=dst, send_sem=send, recv_sem=recv, device_id={"dp": peer}, device_id_type=MESH
    )


class Spread:
    def __init__(self, groups, all_ref, send, recv):
        row = lax.axis_index("dp")
        twin = row + 1 - 2 * lax.rem(row, 2)
        half = groups // 2
        chip = lax.div(row, 2)
        self.relayed = half == 4
        self.out, self.back = [], []
        for k in range(half):
            came = block_of(all_ref, lax.rem(row + groups - 2 * k, groups), groups)
            self.back.append(over_dp(came, came, send.at[half + k], recv.at[half + k], twin))
            if k > 0:
                mine = block_of(all_ref, row, groups)
                self.out.append(over_dp(mine, mine, send.at[k], recv.at[k], lax.rem(row + 2 * k, groups)))
        self.asked = {}
        if self.relayed:
            self.asked = {0: chip != 3, 2: chip != 0}
            self.inner = (chip == 1) | (chip == 2)
            up = lax.div(chip, 2)
            came = block_of(all_ref, lax.rem(row + 4, groups), groups)
            self.relay = over_dp(came, came, send.at[0], recv.at[1 + 2 * up], row + 4 * up - 2)

    def where(self, k, act):
        if k in self.asked:
            pl.when(self.asked[k])(act)
        else:
            act()

    def start(self):
        for k in (1, 0, 2) if self.relayed else range(len(self.out)):
            self.where(k, self.out[k].start)
        self.back[0].start()

    def hop(self):
        if self.relayed:
            self.out[1].wait_recv()
            pl.when(self.inner)(self.relay.start)
            self.back[2].start()

    def forward(self):
        for k, (far, near) in enumerate(zip(self.out, self.back[1:])):
            if k != 1 or not self.relayed:
                far.wait_recv()
                near.start()

    def arrive(self):
        for made in self.back:
            made.wait_recv()

    def finish(self):
        for k, made in enumerate(self.out):
            self.where(k, made.wait_send)
        for made in self.back:
            made.wait_send()
        if self.relayed:
            pl.when(self.inner)(self.relay.wait_send)


class Moves:
    def __init__(self, sem):
        self.sem, self.made = sem, []

    def plan(self, src, dst):
        made = pltpu.make_async_copy(src, dst, self.sem.at[len(self.made)])
        self.made.append(made)
        return made

    def start(self, src, dst):
        made = self.plan(src, dst)
        made.start()
        return made

    def finish(self):
        for made in self.made:
            made.wait()


class Reduce:
    def __init__(self, groups, grad_ref, twin_ref, far_ref, tsend, trecv, fsend, frecv):
        self.grad_ref = grad_ref
        depth = grad_ref.shape[0] // groups
        if far_ref is None:
            near, first = twin_ref, depth * (groups // 2)
            self.twin = lambda slot: near.at[pl.ds(pl.multiple_of(slot * depth, 16), depth)]
            self.far = [near.at[pl.ds(first + k * depth, depth)] for k in range(groups // 2 - 1)]
        else:
            self.twin = lambda slot: twin_ref.at[slot]
            self.far = [far_ref.at[k] for k in range(groups // 2 - 1)]
        rows = lambda block: pl.ds(pl.multiple_of(block * depth, 16), depth)
        row = lax.axis_index("dp")
        core = lax.rem(row, 2)
        self.kept, self.mine = self.twin(lax.div(row, 2)), rows(row)
        self.near, self.away = [], []
        for k in range(groups // 2):
            theirs = grad_ref.at[rows(2 * k + 1 - core)]
            self.near.append(over_dp(theirs, self.twin(k), tsend.at[k], trecv.at[k], row + 1 - 2 * core))
        for k in range(1, groups // 2):
            peer = lax.rem(row + 2 * k, groups)
            slot = lax.div(peer, 2)
            held = self.twin(slot)
            made = over_dp(held, self.far[k - 1], fsend.at[k], frecv.at[k], peer)
            self.away.append((held, rows(peer), made))

    def start(self):
        for made in self.near:
            made.start()

    def pair(self):
        for made in self.near:
            made.wait_recv()
        for held, part, made in self.away:
            held[...] = (held[...].astype(F32) + self.grad_ref[part].astype(F32)).astype(BF16)
            made.start()

    def total(self):
        value = self.kept[...].astype(F32) + self.grad_ref[self.mine].astype(F32)
        for (_, _, made), came in zip(self.away, self.far):
            made.wait_recv()
            value = value + came[...].astype(F32)
        return value

    def finish(self):
        for made in self.near + [made for _, _, made in self.away]:
            made.wait_send()


def reduce_scratch(groups, depth, width):
    half, width = groups // 2, lanes(width)
    return [pltpu.VMEM((half, depth, width), BF16), pltpu.VMEM((half - 1, depth, width), BF16)] + sems(half) * 2


def outer(out_ref, left_ref, right_ref, width, first=0):
    images, blocks, full, model = left_ref.shape
    count = images * blocks * full
    tile = 384

    def part(c, _):
        at = pl.ds(pl.multiple_of(c * tile, tile), tile)
        left = left_ref[:, :, :, at].reshape(count, tile)
        right = right_ref[:, :, :, :width].reshape(count, width)
        out_ref[at, first : first + width] = dot(left, right, TN).astype(BF16)
        return 0

    lax.fori_loop(0, model // tile, part, 0)


def whole_body(
    groups, rows, heads,
    x_ref, grad_ref, mask_ref, gain_one, bias_one, bias_out, gain_two, bias_two, bias_down, qv_ref, hb_ref,
    wq_ref, wo_ref, wh_ref, wd_ref,
    one_out, block_out, gin_out, gwq_ref, gwo_ref, gwh_ref, gwd_ref, both_ref,
    one_ref, full_ref, two_ref, hidden_ref, qh, kh, vh, mixed_ref, wq_all, wo_all, wh_all, wd_all,
    gq, part_ref, ghid_ref, act_ref, gpl_ref, gwh_part, gwd_part, slots, osem,
    dtwin, daway, dtsend, dtrecv, dfsend, dfrecv,
    htwin, haway, htsend, htrecv, hfsend, hfrecv,
    qtsend, qtrecv, qfsend, qfrecv,
    gsend, grecv, wsend, wrecv,
    hsum, bsum, mid, row_in, flat_in, vsend, vrecv,
):
    images = x_ref.shape[0]
    _, _, full, model = one_ref.shape
    units = hb_ref.shape[0]
    seq = 4 * full
    width = heads * HD
    last = images - 1
    me, side, over, _ = plane()
    mine = lax.axis_index("dp")
    wq_all[mine, :, 3 * width :] = jnp.zeros_like(wq_all[mine, :, 3 * width :])
    for c in range(3):
        wq_all[mine, :, c * width : (c + 1) * width] = wq_ref[c]
    weights = [Spread(groups, wq_all, wsend.at[0], wrecv.at[0])]
    for k, (own, everyone) in enumerate(((wo_ref, wo_all), (wh_ref, wh_all), (wd_ref, wd_all))):
        count = own.shape[1]
        place = block_of(everyone, mine, groups)
        place[:, count:] = jnp.zeros((own.shape[0], everyone.shape[-1] - count), BF16)
        place[:, :count] = own[...]
        weights.append(Spread(groups, everyone, wsend.at[k + 1], wrecv.at[k + 1]))
    wq, wo, wh, wd = weights
    ones, sums, twos, grads, turns, lows, outs, backs = [], [], [], [], [], [], [], []
    for i in range(images):
        for ref in (one_ref, two_ref, full_ref):
            clear_pads(ref.at[i], rows)
        pair = lambda k: (gsend.at[k, i], grecv.at[k, i])
        four = [slots.at[i, k] for k in range(4)]
        spare = [act_ref.at[i, k] for k in range(4)]
        ones.append(Gather(one_ref.at[i], rows, *pair(0)))
        grads.append(Gather(full_ref.at[i], rows, *pair(1)))
        sums.append(Scatter(part_ref.at[i], rows, four, *pair(2)))
        twos.append(Gather(two_ref.at[i], rows, *pair(3)))
        turns.append(Scatter(part_ref.at[i], rows, four, *pair(4)))
        lows.append(Gather(one_ref.at[i], rows, *pair(5)))
        outs.append(Scatter(two_ref.at[i], rows, spare, *pair(6)))
        backs.append(Scatter(part_ref.at[i], rows, four, *pair(7)))
    down = Reduce(groups, gwd_part, dtwin, daway, dtsend, dtrecv, dfsend, dfrecv)
    red_h = Reduce(groups, gwh_part, htwin, haway, htsend, htrecv, hfsend, hfrecv)
    red_q = Reduce(groups, gwd_part, wd_all, None, qtsend, qtrecv, qfsend, qfrecv)
    moves = Moves(osem)
    keep_one = [moves.plan(one_ref.at[i], one_out.at[i]) for i in range(images)]
    take_one = [moves.plan(one_out.at[i], full_ref.at[i]) for i in range(images)]
    take_grad = [moves.plan(grad_ref.at[i], full_ref.at[i, me, pl.ds(0, rows)]) for i in range(images)]
    put_out = [moves.plan(two_ref.at[i, me, pl.ds(0, rows)], block_out.at[i]) for i in range(images)]
    put_gin = [moves.plan(ghid_ref.at[i], gin_out.at[i]) for i in range(images)]

    def enter(i):
        one_ref[i, me, :rows] = norm_forward(x_ref[i].astype(F32), at_row(gain_one), at_row(bias_one))

    for made in take_grad:
        made.start()
    greet_all(groups, lambda: enter(0))
    ones[0].start()
    wq.start()
    for i in range(1, images):
        enter(i)
        ones[i].start()
    for step in (wo, wh, wd):
        step.start()
    hsum[...] = jnp.zeros_like(hsum)
    bsum[...] = jnp.zeros_like(bsum)
    mixed_ref[:, :, :, width:] = jnp.zeros_like(mixed_ref[:, :, :, width:])
    for i in range(images):
        bias, tail = key_bias(mask_ref[i : i + 1], rows, full, seq)
        for h in range(heads):
            kh[i, h, :, HD:] = bias
            vh[i, h, :, HD:] = jnp.zeros_like(bias)
            qh[i, h, :, HD:] = tail
    for step in ones:
        step.forward()
    for made in take_grad:
        made.wait()
    for step in grads:
        step.start()
    wq.hop()
    wq.forward()
    scale = HD**-0.5
    shift_q, shift_v = qv_ref[0:1], qv_ref[1:2]

    def project(i):
        weight = wq_all[:, :, : 3 * width].reshape(-1, 3 * width)

        def block(b, _):
            at = pl.ds(pl.multiple_of(b * full, 16), full)
            value = dot(one_ref[i, b], weight)
            queries = (value[:, :width] + shift_q).astype(BF16)
            keys_in = value[:, width : 2 * width].astype(BF16)
            values = (value[:, 2 * width :] + shift_v).astype(BF16)
            for h in range(heads):
                here = slice(h * HD, (h + 1) * HD)
                qh[i, h, at, :HD] = queries[:, here]
                kh[i, h, at, :HD] = keys_in[:, here]
                vh[i, h, at, :HD] = values[:, here]
            return 0

        lax.fori_loop(0, 4, block, 0)

    def attend(i):
        def head(h, _):
            probs = soft_open(kh[i, h], qh[i, h], scale * LOG2E)
            gq[h] = dot(vh[i, h, :, :HD].T, probs.astype(BF16)).T.astype(BF16)
            return 0

        lax.fori_loop(0, heads, head, 0, unroll=2)
        for h in range(heads):
            for b in range(4):
                mixed_ref[i, b, :, h * HD : (h + 1) * HD] = gq[h, b * full : (b + 1) * full]

    def combine(i):
        weight = wo_all[:, :, :width].reshape(-1, width)

        def block(b, _):
            part_ref[i, b] = dot(mixed_ref[i, b, :, :width], weight, NT).astype(BF16)
            return 0

        lax.fori_loop(0, 4, block, 0)

    def ready(k):
        ones[k].arrive()
        keep_one[k].start()
        if k == 0:
            wq.arrive()

    def between(k):
        if k == 0:
            wo.hop()
            wo.forward()
            wh.hop()
            wo.arrive()

    def send(k):
        if k > 0:
            sums[k - 1].forward()
        sums[k].start()
        grads[k].forward()

    def image(i, _):
        for_image(i, images, ready)
        project(i)
        attend(i)
        for_image(i, images, between)
        combine(i)
        for_image(i, images, send)
        return 0

    lax.fori_loop(0, images, image, 0)

    def settle(i):
        sums[i].arrive()
        hidden = x_ref[i].astype(F32) + sums[i].total(pl.ds(0, rows)) + at_row(bias_out)
        hidden_ref[i] = hidden
        two_ref[i, me, :rows] = norm_forward(hidden, at_row(gain_two), at_row(bias_two))
        twos[i].start()

    for i in range(last):
        settle(i)
    sums[-1].forward()
    wd.hop()
    for i in range(last):
        twos[i].forward()
    settle(last)
    twos[-1].forward()
    wh.forward()
    wd.forward()
    for step in sums + ones:
        step.finish()
    for made in keep_one:
        made.wait()
    wide = lambda ref: ref[:, :units]
    shift = at_row(hb_ref)

    def ascend(i):
        def pair(c, _):
            at = pl.ds(2 * c, 2)
            pre = dot(two_ref[i, at].reshape(2 * full, model), wide(wh_all)) + shift
            value, slope = gelu_both(pre)
            act_ref[i, at, :, :units] = value.astype(BF16).reshape(2, full, units)
            grad_pre = dot(full_ref[i, at].reshape(2 * full, model), wide(wd_all)) * slope
            hsum[...] += jnp.sum(grad_pre, axis=0, keepdims=True)
            low = grad_pre.astype(BF16)
            gpl_ref[i, at, :, :units] = low.reshape(2, full, units)
            part_ref[i, at] = dot(low, wide(wh_all), NT).astype(BF16).reshape(2, full, model)
            return 0

        lax.fori_loop(0, 2, pair, 0)

    def descend(k, _):
        at = pl.ds(2 * lax.rem(k, 2), 2)
        i = lax.div(k, 2)
        part = dot(act_ref[i, at, :, :units].reshape(2 * full, units), wide(wd_all), NT)
        two_ref[i, at] = part.astype(BF16).reshape(2, full, model)
        return 0

    totals = [0.0] * 6

    def add_up(first, terms):
        for k, term in enumerate(terms):
            totals[first + k] = totals[first + k] + jnp.sum(term, axis=0, keepdims=True)

    def settle_back(i):
        turns[i].arrive()
        grad_normed = turns[i].total(pl.ds(0, rows))
        unit, inv_std = norm_stats(hidden_ref[i])
        upper = full_ref[i, me, :rows].astype(F32)
        grad_hidden = upper + norm_backward(grad_normed, unit, inv_std, at_row(gain_two))
        ghid_ref[i] = grad_hidden
        one_ref[i, me, :rows] = grad_hidden.astype(BF16)
        lows[i].start()
        add_up(0, (grad_normed * unit, grad_normed, grad_hidden, upper))

    def ready_back(k):
        twos[k].arrive()
        if k == 0:
            wh.arrive()
            wd.arrive()
        grads[k].arrive()

    def send_back(k):
        if k > 0:
            turns[k - 1].forward()
        turns[k].start()

    def image_back(i, _):
        for_image(i, images, ready_back)
        ascend(i)
        for_image(i, images, send_back)
        return 0

    lax.fori_loop(0, images, image_back, 0)
    for step in weights:
        step.finish()
    gwd_part[:, units:] = jnp.zeros((model, lanes(units) - units), BF16)
    outer(gwd_part, full_ref, act_ref, units)
    down.start()
    for i in range(last):
        settle_back(i)
    turns[-1].forward()
    down.pair()
    gwh_part[:, units:] = jnp.zeros((model, lanes(units) - units), BF16)
    outer(gwh_part, two_ref, gpl_ref, units)
    for i in range(last):
        lows[i].forward()
    for step in twos:
        step.finish()
    lax.fori_loop(0, 2 * images, descend, 0)
    red_h.start()
    settle_back(last)
    red_h.pair()
    for step in turns + grads:
        step.finish()
    for made in take_one:
        made.start()

    def mix(i):
        value = dot(one_ref[i].reshape(seq, model), wo_all[:, :, :width].reshape(model, width)).astype(BF16)
        gpl_ref[i, :, :, 3 * width : 4 * width] = value.reshape(4, full, width)

    def midway(k):
        if k < last:
            lows[k + 1].forward()
        if k > 0:
            backs[k - 1].forward()

    def attend_back(i):
        for h in range(heads):
            if h == heads // 2:
                for_image(i, images, midway)
            here = slice(3 * width + h * HD, 3 * width + (h + 1) * HD)
            queries = qh[i, h]
            grads_in = gpl_ref[i, :, :, here].reshape(seq, HD)
            keys_in = kh[i, h]
            probs = soft_open(keys_in, queries, scale * LOG2E)
            grad_probs = dot(vh[i, h, :, :HD], grads_in, NT)
            grad_values = dot(probs.astype(BF16), grads_in)
            delta = jnp.sum(probs * grad_probs, axis=0, keepdims=True)
            grad_scores = (probs * (grad_probs - delta) * scale).astype(BF16)
            grad_keys = dot(grad_scores, queries[:, :HD])
            grad_queries = dot(keys_in[:, :HD].T, grad_scores).T
            for c, value in enumerate((grad_queries, grad_keys, grad_values)):
                here = slice(c * width + h * HD, c * width + (h + 1) * HD)
                gpl_ref[i, :, :, here] = value.astype(BF16).reshape(4, full, HD)
                bsum[h, c : c + 1] += jnp.sum(value, axis=0, keepdims=True)

    def spread(i):
        def pair(c, _):
            at = pl.ds(2 * c, 2)
            left = gpl_ref[i, at, :, : 3 * width].reshape(2 * full, 3 * width)
            part = dot(left, wq_all[:, :, : 3 * width].reshape(model, 3 * width), NT)
            part_ref[i, at] = part.astype(BF16).reshape(2, full, model)
            return 0

        lax.fori_loop(0, 2, pair, 0)

    def ready_last(k):
        lows[k].arrive(4 if k > 0 else 2)

    def send_last(k):
        backs[k].start()
        if k < last:
            lows[k + 1].arrive(2, 4)
            outs[k].start()
        else:
            outs[k - 1].forward()

    def image_last(i, _):
        for_image(i, images, ready_last)
        mix(i)
        attend_back(i)
        spread(i)
        for_image(i, images, send_last)
        return 0

    lax.fori_loop(0, images, image_last, 0)
    gwd_ref[...] = down.total()[:, :units]
    down.finish()
    outer(gwd_part, one_ref, mixed_ref, width, 3 * width)
    for made in take_one:
        made.wait()
    outer(gwd_part, full_ref, gpl_ref, 3 * width)
    red_q.start()

    def settle_last(i):
        backs[i].arrive()
        grad_normed = backs[i].total(pl.ds(0, rows))
        unit, inv_std = norm_stats(x_ref[i].astype(F32))
        ghid_ref[i] = ghid_ref[i] + norm_backward(grad_normed, unit, inv_std, at_row(gain_one))
        put_gin[i].start()
        add_up(4, (grad_normed * unit, grad_normed))

    def finish_out(i):
        outs[i].arrive()
        value = hidden_ref[i] + outs[i].total(pl.ds(0, rows)) + at_row(bias_down)
        two_ref[i, me, :rows] = value.astype(BF16)
        put_out[i].start()

    for i in range(last):
        settle_last(i)
    backs[-1].forward()
    outs[-1].start()
    gwh_ref[...] = red_h.total()[:, :units]
    red_q.pair()
    mid[0] = jnp.zeros_like(mid[0])
    for h in range(heads):
        for c in range(3):
            mid[0, 6:7, c * width + h * HD : c * width + (h + 1) * HD] = bsum[h, c : c + 1]
    mid[0, 7:8, :units] = hsum[...]
    settle_last(last)

    for k in range(6):
        mid[0, k : k + 1] = totals[k]
    row_in[mine] = mid[0]
    aways = []
    for k in range(1, groups):
        aways.append(over_dp(mid.at[0], row_in.at[mine], vsend.at[k], vrecv.at[k], lax.rem(mine + k, groups)))
        aways[-1].start()
    outs[-1].forward()
    for made in aways:
        made.wait()
    held = row_in[0]
    for k in range(1, groups):
        held = held + row_in[k]
    mid[1] = held
    flat_in[me] = mid[1]
    planes = []
    for k in range(1, 4):
        at = groups + k
        planes.append(remote(mid.at[1], flat_in.at[me], vsend.at[at], vrecv.at[at], lax.rem(me + k, 4)))
        planes[-1].start()
    for i in range(last):
        finish_out(i)
    for made in planes:
        made.wait()
    both_ref[0:6] = (flat_in[0] + flat_in[1] + flat_in[2] + flat_in[3])[0:6]
    both_ref[6:8] = mid[1, 6:8]
    finish_out(last)
    total = red_q.total()
    for c in range(3):
        gwq_ref[c] = total[:, c * width : (c + 1) * width]
    gwo_ref[...] = total[:, 3 * width : 4 * width]
    for step in lows + outs + backs + [red_h, red_q]:
        step.finish()
    for made in put_out + put_gin:
        made.wait()


def whole(groups, block_input, grad_out, key_mask, vectors, qv_bias, bias, wq, wo, wh, wd):
    images, rows, model = block_input.shape
    full = pad_rows(rows)
    width = wo.shape[1]
    units = wh.shape[1]
    heads = width // HD
    seq = 4 * full
    depth = wo.shape[0]
    blocks = ((images, 4, full, model), BF16)
    own = ((images, rows, model), F32)
    heads_wide = ((images, heads, seq, 128), BF16)
    piece = ((heads, seq, HD), BF16)
    square = ((model, lanes(units)), BF16)
    weight = lambda count: ((groups, depth, lanes(count)), BF16)
    outs = [blocks, (block_input.shape, BF16), own]
    more = [((3, depth, width), F32), ((depth, width), F32), ((depth, units), F32), ((depth, units), F32), ((8, model), F32)]
    held = [blocks, blocks, blocks, own, heads_wide, heads_wide, heads_wide, ((images, 4, full, lanes(width)), BF16)]
    held += [weight(3 * width), weight(width), square, square]
    held += [piece, blocks, own, blocks, blocks, square, square, blocks]
    return pl.pallas_call(
        functools.partial(whole_body, groups, rows, heads),
        out_shape=tuple(jax.ShapeDtypeStruct(*h) for h in outs + more),
        in_specs=[VMEM, ANY] + [VMEM] * 13,
        out_specs=(ANY,) * len(outs) + (VMEM,) * len(more),
        scratch_shapes=[pltpu.VMEM(*h) for h in held]
        + [pltpu.SemaphoreType.DMA((5 * images,))]
        + reduce_scratch(groups, depth, units) * 2
        + sems(groups // 2) * 2
        + sems(8, images, STEPS)
        + sems(4, groups)
        + [
            pltpu.VMEM((1, units), F32),
            pltpu.VMEM((heads, 3, HD), F32),
            pltpu.VMEM((2, 8, model), F32),
            pltpu.VMEM((groups, 8, model), F32),
            pltpu.VMEM((4, 8, model), F32),
        ]
        + sems(groups + 4),
        compiler_params=params(0),
        name="whole",
    )(block_input, grad_out, key_mask, *vectors, qv_bias, bias, wq, wo, wh, wd)


def deliver_body(width, out, gin, gwq, gwo, gwh, gwd, both, *refs):
    refs, held, lsem, ssem = refs[:14], refs[14:20], refs[20], refs[21]
    loads, stores = Moves(lsem), Moves(ssem)
    sources = (out, gin, gwq, gwo, gwh, gwd)
    got = [loads.start(src, mid) for src, mid in zip(sources, held)]
    qv, unit = refs[6:8]
    qv[0:1] = both[6:7, :width]
    qv[1:2] = both[6:7, 2 * width : 3 * width]
    unit[...] = both[7, : unit.shape[0]]
    for k, dst in enumerate(refs[8:]):
        dst[...] = both[k]
    for made, mid, dst in zip(got, held, refs):
        made.wait()
        stores.start(mid, dst)
    stores.finish()


def deliver(width, units, out, gin, gwq, gwo, gwh, gwd, both):
    model = both.shape[1]
    same = [jax.ShapeDtypeStruct(v.shape, v.dtype) for v in (out, gin, gwq, gwo, gwh, gwd)]
    more = [jax.ShapeDtypeStruct(dims, F32) for dims in ((2, width), (units,)) + ((model,),) * 6]
    return pl.pallas_call(
        functools.partial(deliver_body, width),
        out_shape=tuple(same + more),
        in_specs=[ANY] * 6 + [VMEM],
        out_specs=(ANY,) * 6 + (VMEM,) * 8,
        scratch_shapes=[pltpu.VMEM(v.shape, v.dtype) for v in same]
        + [pltpu.SemaphoreType.DMA((6,)), pltpu.SemaphoreType.DMA((6,))],
        compiler_params=pltpu.CompilerParams(vmem_limit_bytes=60 << 20),
        name="deliver",
    )(out, gin, gwq, gwo, gwh, gwd, both)


def gather_rows(rows):
    return lax.all_gather(rows, "tensor", axis=1, tiled=True)


def scatter_rows(part):
    return lax.psum_scatter(part, "tensor", scatter_dimension=1, tiled=True).astype(F32)


def shards(
    groups,
    ranks,
    block_input,
    key_mask,
    attn_norm_gain,
    attn_norm_bias,
    qkv_weight,
    qv_bias,
    out_weight,
    out_bias,
    mlp_norm_gain,
    mlp_norm_bias,
    hidden_weight,
    hidden_bias,
    down_weight,
    down_bias,
    grad_out,
):
    images, rows, model = block_input.shape
    flat = ranks == 4 and images == 2 and groups > 2 and groups % 2 == 0 and hidden_weight.shape[1] <= model and 4 * qkv_weight.shape[2] == lanes(hidden_weight.shape[1])
    seq = key_mask.shape[1]
    width = qkv_weight.shape[2]
    units = hidden_weight.shape[1]

    def weight(shard):
        return lax.all_gather(shard, "dp", axis=0, tiled=True)

    def owned(grad):
        return lax.psum_scatter(grad.astype(BF16), "dp", scatter_dimension=0, tiled=True).astype(F32)

    out_rows, down_rows = out_weight.T, down_weight.T
    if flat:
        _, block_output, grad_input, grad_qkv_w, grad_out_w, grad_hidden_w, grad_down_w, both = whole(
            groups,
            block_input,
            grad_out,
            key_mask,
            (attn_norm_gain, attn_norm_bias, out_bias, mlp_norm_gain, mlp_norm_bias, down_bias),
            qv_bias,
            hidden_bias,
            qkv_weight.transpose(1, 0, 2),
            out_rows,
            hidden_weight,
            down_rows,
        )
        (
            block_output, grad_input, grad_qkv_w, grad_out_w, grad_hidden_w, grad_down_w, grad_qv, grad_hidden_b, *both
        ) = deliver(
            width, units, block_output, grad_input, grad_qkv_w, grad_out_w, grad_hidden_w, grad_down_w, both
        )
        grad_qkv_w = grad_qkv_w.transpose(1, 0, 2)
        grad_out_w, grad_down_w = grad_out_w.T, grad_down_w.T
    else:
        qkv_rows = qkv_weight.reshape(-1, 3 * width)
        shift = jnp.concatenate([qv_bias[0], jnp.zeros_like(qv_bias[0]), qv_bias[1]])
        hidden_all, down_all = weight(hidden_weight), weight(down_rows)
        qkv_all, out_all = weight(qkv_rows), weight(out_rows)
        lens = jnp.sum(key_mask, axis=1)
        in_float = block_input.astype(F32)
        normed_one = gather_rows(norm_forward(in_float, attn_norm_gain, attn_norm_bias))
        grad_full = gather_rows(grad_out)
        proj = jnp.einsum("isd,df->isf", normed_one, qkv_all, preferred_element_type=F32) + shift
        proj = proj.astype(BF16)
        mixed = attend_forward(lens, proj)
        attn_part = jnp.einsum("isf,df->isd", mixed, out_all, preferred_element_type=F32).astype(BF16)
        hidden_res = in_float + scatter_rows(attn_part) + out_bias
        normed_two = gather_rows(norm_forward(hidden_res, mlp_norm_gain, mlp_norm_bias))
        pre_act = jnp.einsum("isd,df->isf", normed_two, hidden_all, preferred_element_type=F32) + hidden_bias
        value, slope = gelu_both(pre_act)
        activated = value.astype(BF16)
        grad_act = jnp.einsum("isd,df->isf", grad_full, down_all, preferred_element_type=F32)
        grad_pre = grad_act * slope
        grad_hidden_b = jnp.sum(grad_pre, axis=(0, 1))
        grad_pre_low = grad_pre.astype(BF16)
        gpart = jnp.einsum("isf,df->isd", grad_pre_low, hidden_all, preferred_element_type=F32).astype(BF16)
        mpart = jnp.einsum("isf,df->isd", activated, down_all, preferred_element_type=F32).astype(BF16)
        block_output = (hidden_res + scatter_rows(mpart) + down_bias).astype(BF16)
        grad_float = grad_out.astype(F32)
        grad_normed = scatter_rows(gpart)
        unit, inv_std = norm_stats(hidden_res)
        grad_hidden = grad_float + norm_backward(grad_normed, unit, inv_std, mlp_norm_gain)
        hidden_full = gather_rows(grad_hidden.astype(BF16))
        mlp_sums = jnp.stack(
            [jnp.sum(v, axis=(0, 1)) for v in (grad_normed * unit, grad_normed, grad_hidden, grad_float)]
        )
        grad_hidden_w = owned(jnp.einsum("isd,isf->df", normed_two, grad_pre_low, preferred_element_type=F32))
        grad_down_w = owned(jnp.einsum("isd,isf->df", grad_full, activated, preferred_element_type=F32)).T
        grad_mixed = jnp.einsum("isd,df->isf", hidden_full, out_all, preferred_element_type=F32).astype(BF16)
        grad_proj, proj_sums = attend_backward(lens, proj, grad_mixed)
        proj_sums = jnp.sum(proj_sums, axis=(0, 1))
        npart = jnp.einsum("isf,df->isd", grad_proj, qkv_all, preferred_element_type=F32).astype(BF16)
        grad_out_w = owned(jnp.einsum("isd,isf->df", hidden_full, mixed, preferred_element_type=F32)).T
        grad_qkv_w = owned(jnp.einsum("isd,isf->df", normed_one, grad_proj, preferred_element_type=F32))
        grad_normed = scatter_rows(npart)
        unit, inv_std = norm_stats(in_float)
        grad_input = grad_hidden + norm_backward(grad_normed, unit, inv_std, attn_norm_gain)
        attn_sums = jnp.stack([jnp.sum(v, axis=(0, 1)) for v in (grad_normed * unit, grad_normed)])
        both = lax.psum(jnp.concatenate([mlp_sums, attn_sums]), ("dp", "tensor"))
        proj_sums, grad_hidden_b = lax.psum((proj_sums, grad_hidden_b), "dp")
        grad_qv = jnp.stack([proj_sums[:width], proj_sums[2 * width :]])
        grad_qkv_w = grad_qkv_w.reshape(-1, 3, width)
    return (
        block_output,
        grad_input,
        both[4],
        both[5],
        grad_qkv_w,
        grad_qv,
        grad_out_w,
        both[2],
        both[0],
        both[1],
        grad_hidden_w,
        grad_hidden_b,
        grad_down_w,
        both[3],
    )


def solution(mesh):
    return jax.shard_map(
        functools.partial(shards, mesh.shape["dp"], mesh.shape["tensor"]),
        mesh=mesh,
        in_specs=(
            P("dp", "tensor", None),
            P("dp", None),
            P(),
            P(),
            P("dp", None, "tensor"),
            P(None, "tensor"),
            P("tensor", "dp"),
            P(),
            P(),
            P(),
            P("dp", "tensor"),
            P("tensor"),
            P("tensor", "dp"),
            P(),
            P("dp", "tensor", None),
        ),
        out_specs=(
            P("dp", "tensor", None),
            P("dp", "tensor", None),
            P(),
            P(),
            P("dp", None, "tensor"),
            P(None, "tensor"),
            P("tensor", "dp"),
            P(),
            P(),
            P(),
            P("dp", "tensor"),
            P("tensor"),
            P("tensor", "dp"),
            P(),
        ),
        check_vma=False,
    )
```

```python
import functools
import math

import jax
import jax.numpy as jnp
from jax import lax
from jax.experimental import pallas as pl
from jax.experimental.pallas import tpu as pltpu
from jax.sharding import PartitionSpec as P

HD = 72
CHUNK = 768
F32 = jnp.float32
BF16 = jnp.bfloat16
LOG2E = math.log2(math.e)
NN = (((1,), (0,)), ((), ()))
NT = (((1,), (1,)), ((), ()))
TN = (((0,), (0,)), ((), ()))
MESH = pl.DeviceIdType.MESH
ANY = pl.BlockSpec(memory_space=pl.ANY)
VMEM = pl.BlockSpec(memory_space=pltpu.VMEM)
SMEM = pl.BlockSpec(memory_space=pltpu.SMEM)


layer_eps = 1e-06
gelu_root = math.sqrt(2.0 / math.pi)
gelu_cubic = 0.044715


def norm_stats(rows):
    center = rows - jnp.mean(rows, axis=-1, keepdims=True)
    inv_std = lax.rsqrt(jnp.mean(center * center, axis=-1, keepdims=True) + layer_eps)
    return (center * inv_std, inv_std)


def norm_forward(rows, gain, shift):
    unit, _ = norm_stats(rows)
    return (unit * gain + shift).astype(BF16)


def norm_backward(grad_normed, unit, inv_std, gain):
    scaled = grad_normed * gain
    return inv_std * (
        scaled
        - jnp.mean(scaled, axis=-1, keepdims=True)
        - unit * jnp.mean(scaled * unit, axis=-1, keepdims=True)
    )


def gelu_both(pre):
    tangent = jnp.tanh(gelu_root * (pre + gelu_cubic * pre * pre * pre))
    value = 0.5 * pre * (1.0 + tangent)
    slope = 0.5 * (1.0 + tangent) + 0.5 * pre * (1.0 - tangent * tangent) * gelu_root * (
        1.0 + 3.0 * gelu_cubic * pre * pre
    )
    return (value, slope)


def dot(a, b, dims=NN):
    return lax.dot_general(a, b, dims, preferred_element_type=F32)


def soft_columns(keys_in, queries, row_ok, factor):
    raw = jnp.where(row_ok, dot(keys_in, queries, NT), -1e30)
    top = jnp.max(raw, axis=0, keepdims=True)
    grown = jnp.exp2((raw - top) * factor)
    total = jnp.sum(grown, axis=0, keepdims=True)
    return grown * (1.0 / total)


def attend_forward_body(seq, heads, lens_ref, proj_ref, mixed_ref, qh, kh, vh, oh):
    width = heads * HD
    padded = qh.shape[1]
    for h in range(heads):
        qh[h, :seq] = proj_ref[0, :, h * HD : (h + 1) * HD]
        qh[h, seq:] = jnp.zeros((padded - seq, HD), BF16)
        kh[h] = proj_ref[0, :, width + h * HD : width + (h + 1) * HD]
        vh[h] = proj_ref[0, :, 2 * width + h * HD : 2 * width + (h + 1) * HD].T
    length = lens_ref[pl.program_id(0)]
    factor = HD**-0.5 * LOG2E

    def head(h, _):
        def chunk(c, _):
            row_ok = lax.broadcasted_iota(jnp.int32, (seq, CHUNK), 0) < length
            at = pl.ds(pl.multiple_of(c * CHUNK, CHUNK), CHUNK)
            probs = soft_columns(kh[h], qh[h, at], row_ok, factor)
            oh[h, at] = dot(vh[h], probs.astype(BF16)).T.astype(BF16)
            return 0

        return lax.fori_loop(0, padded // CHUNK, chunk, 0)

    lax.fori_loop(0, heads, head, 0)
    for h in range(heads):
        mixed_ref[0, :, h * HD : (h + 1) * HD] = oh[h, :seq]


def attend_forward(lens, proj):
    images, seq, triple = proj.shape
    heads = triple // (3 * HD)
    padded = -(-seq // CHUNK) * CHUNK
    return pl.pallas_call(
        functools.partial(attend_forward_body, seq, heads),
        out_shape=jax.ShapeDtypeStruct((images, seq, heads * HD), BF16),
        grid=(images,),
        in_specs=[SMEM, pl.BlockSpec((1, seq, triple), lambda i: (i, 0, 0))],
        out_specs=pl.BlockSpec((1, seq, heads * HD), lambda i: (i, 0, 0)),
        scratch_shapes=[
            pltpu.VMEM((heads, padded, HD), BF16),
            pltpu.VMEM((heads, seq, HD), BF16),
            pltpu.VMEM((heads, HD, seq), BF16),
            pltpu.VMEM((heads, padded, HD), BF16),
        ],
        name="attend_forward",
    )(lens, proj)


def attend_backward_body(
    seq, heads, lens_ref, proj_ref, gmix_ref, gproj_ref, gbias_ref, qh, kh, kt, vh, gh, gq, gk, gv
):
    width = heads * HD
    padded = qh.shape[1]
    for h in range(heads):
        qh[h, :seq] = proj_ref[0, :, h * HD : (h + 1) * HD]
        qh[h, seq:] = jnp.zeros((padded - seq, HD), BF16)
        gh[h, :seq] = gmix_ref[0, :, h * HD : (h + 1) * HD]
        gh[h, seq:] = jnp.zeros((padded - seq, HD), BF16)
        keys_in = proj_ref[0, :, width + h * HD : width + (h + 1) * HD]
        kh[h] = keys_in
        kt[h] = keys_in.T
        vh[h] = proj_ref[0, :, 2 * width + h * HD : 2 * width + (h + 1) * HD]
    length = lens_ref[pl.program_id(0)]
    scale = HD**-0.5
    factor = scale * LOG2E

    def head(h, _):
        gk[h] = jnp.zeros((seq, HD), F32)
        gv[h] = jnp.zeros((seq, HD), F32)

        def chunk(c, _):
            row_ok = lax.broadcasted_iota(jnp.int32, (seq, CHUNK), 0) < length
            at = pl.ds(pl.multiple_of(c * CHUNK, CHUNK), CHUNK)
            queries = qh[h, at]
            grads = gh[h, at]
            probs = soft_columns(kh[h], queries, row_ok, factor)
            grad_probs = dot(vh[h], grads, NT)
            gv[h] += dot(probs.astype(BF16), grads)
            delta = jnp.sum(probs * grad_probs, axis=0, keepdims=True)
            grad_scores = (probs * (grad_probs - delta) * scale).astype(BF16)
            gk[h] += dot(grad_scores, queries)
            gq[h, at] = dot(kt[h], grad_scores).T
            return 0

        return lax.fori_loop(0, padded // CHUNK, chunk, 0)

    lax.fori_loop(0, heads, head, 0)
    for h in range(heads):
        for c, held in enumerate((gq, gk, gv)):
            value = held[h, :seq]
            at = slice(c * width + h * HD, c * width + (h + 1) * HD)
            gproj_ref[0, :, at] = value.astype(BF16)
            gbias_ref[0, :, at] = jnp.sum(value, axis=0, keepdims=True)


def attend_backward(lens, proj, gmix):
    images, seq, triple = proj.shape
    heads = triple // (3 * HD)
    padded = -(-seq // CHUNK) * CHUNK
    return pl.pallas_call(
        functools.partial(attend_backward_body, seq, heads),
        out_shape=(
            jax.ShapeDtypeStruct((images, seq, triple), BF16),
            jax.ShapeDtypeStruct((images, 1, triple), F32),
        ),
        grid=(images,),
        in_specs=[
            SMEM,
            pl.BlockSpec((1, seq, triple), lambda i: (i, 0, 0)),
            pl.BlockSpec((1, seq, heads * HD), lambda i: (i, 0, 0)),
        ],
        out_specs=(
            pl.BlockSpec((1, seq, triple), lambda i: (i, 0, 0)),
            pl.BlockSpec((1, 1, triple), lambda i: (i, 0, 0)),
        ),
        scratch_shapes=[
            pltpu.VMEM((heads, padded, HD), BF16),
            pltpu.VMEM((heads, seq, HD), BF16),
            pltpu.VMEM((heads, HD, seq), BF16),
            pltpu.VMEM((heads, seq, HD), BF16),
            pltpu.VMEM((heads, padded, HD), BF16),
            pltpu.VMEM((heads, padded, HD), F32),
            pltpu.VMEM((heads, seq, HD), F32),
            pltpu.VMEM((heads, seq, HD), F32),
        ],
        name="attend_backward",
    )(lens, proj, gmix)


def plane():
    me = lax.axis_index("tensor")
    side = me + 1 - 2 * lax.rem(me, 2)
    over = lax.rem(me + 2, 4)
    return (me, side, over, lax.rem(side + 2, 4))


def greet(peers):
    barrier = pltpu.get_barrier_semaphore()
    for peer in peers:
        pl.semaphore_signal(barrier, inc=1, device_id={"tensor": peer}, device_id_type=MESH)
    pl.semaphore_wait(barrier, len(peers))


def greet_all(groups, work):
    row, me = lax.axis_index("dp"), lax.axis_index("tensor")
    barrier = pltpu.get_barrier_semaphore()
    peers = [{"dp": lax.rem(row + k, groups)} for k in range(1, groups)]
    peers += [{"tensor": lax.rem(me + k, 4)} for k in range(1, 4)]
    for peer in peers:
        pl.semaphore_signal(barrier, inc=1, device_id=peer, device_id_type=MESH)
    work()
    pl.semaphore_wait(barrier, len(peers))


def remote(src, dst, send, recv, peer):
    return pltpu.make_async_remote_copy(
        src_ref=src,
        dst_ref=dst,
        send_sem=send,
        recv_sem=recv,
        device_id={"tensor": peer},
        device_id_type=MESH,
    )


def halves_of(rows):
    first = -(-rows // 32) * 16
    return (pl.ds(0, first), pl.ds(first, rows - first))


class Gather:
    def __init__(self, all_ref, rows, send, recv):
        me, side, over, _ = plane()
        low, high = halves_of(rows)
        plan = (
            (me, low, side),
            (me, high, over),
            (me, high, side),
            (me, low, over),
            (side, low, over),
            (over, high, side),
        )
        self.copies = []
        for k, (block, part, peer) in enumerate(plan):
            ref = all_ref.at[block, part]
            self.copies.append(remote(ref, ref, send.at[k], recv.at[k], peer))

    def start(self):
        for made in self.copies[:4]:
            made.start()

    def forward(self):
        for k in range(2):
            self.copies[k].wait_recv()
            self.copies[4 + k].start()

    def arrive(self, first=2, last=6):
        for made in self.copies[first:last]:
            made.wait_recv()

    def finish(self):
        for made in self.copies:
            made.wait_send()


class Scatter:
    def __init__(self, part_ref, rows, slots, send, recv):
        self.me, self.side, self.over, cross = plane()
        self.part_ref = part_ref
        self.own, self.other, self.far, self.passing = slots
        self.halves = low, high = halves_of(rows)
        plan = (
            (part_ref.at[cross, low], self.other.at[low], self.side),
            (part_ref.at[cross, high], self.other.at[high], self.over),
            (part_ref.at[self.side, low], self.own.at[low], self.side),
            (part_ref.at[self.over, high], self.own.at[high], self.over),
            (self.passing.at[low], self.far.at[low], self.over),
            (self.passing.at[high], self.far.at[high], self.side),
        )
        self.copies = [remote(src, dst, send.at[k], recv.at[k], peer) for k, (src, dst, peer) in enumerate(plan)]

    def start(self):
        for made in self.copies[:4]:
            made.start()

    def forward(self):
        for k, (part, block) in enumerate(zip(self.halves, (self.over, self.side))):
            self.copies[k].wait_recv()
            mine = self.part_ref[block, part].astype(F32)
            self.passing[part] = (mine + self.other[part].astype(F32)).astype(BF16)
            self.copies[4 + k].start()

    def arrive(self):
        for made in self.copies[2:]:
            made.wait_recv()

    def total(self, rows):
        return (
            self.part_ref[self.me, rows].astype(F32) + self.own[rows].astype(F32) + self.far[rows].astype(F32)
        )

    def finish(self):
        for made in self.copies:
            made.wait_send()


STEPS = 6


def sems(*shape):
    return [pltpu.SemaphoreType.DMA(shape), pltpu.SemaphoreType.DMA(shape)]


def params(cid):
    return pltpu.CompilerParams(collective_id=cid, has_side_effects=True, vmem_limit_bytes=67043328)


def lanes(width):
    return -(-width // 128) * 128


def pad_rows(rows):
    return -(-rows // 16) * 16


def clear_pads(ref, rows):
    full = ref.shape[1]
    for b in range(ref.shape[0]):
        ref[b, rows:full] = jnp.zeros((full - rows, ref.shape[2]), ref.dtype)


def at_row(ref):
    return ref[...].reshape(1, -1)


def for_image(i, images, act):
    for k in range(images):
        pl.when(i == k)(functools.partial(act, k))


def key_bias(mask, rows, full, seq):
    length = jnp.sum(mask.astype(F32), axis=1, keepdims=True).astype(jnp.int32)
    at = lax.broadcasted_iota(jnp.int32, (seq, 128 - HD), 0)
    lane = lax.broadcasted_iota(jnp.int32, (seq, 128 - HD), 1)
    block = sum((at >= b * full).astype(jnp.int32) for b in range(1, seq // full))
    inner = at - block * full
    good = (inner < rows) & (inner + block * rows < length)
    bias = jnp.where(good, 0.0, -1e30)
    ones = jnp.where(lane == 0, 1.0, 0.0)
    return (jnp.where(lane == 0, bias, 0.0).astype(BF16), ones.astype(BF16))


def soft_open(keys_in, queries, factor):
    raw = dot(keys_in, queries, NT)
    top = jnp.max(raw, axis=0, keepdims=True)
    grown = jnp.exp2((raw - top) * factor)
    total = jnp.sum(grown, axis=0, keepdims=True)
    return grown * (1.0 / total)


def block_of(ref, block, groups):
    if len(ref.shape) == 3:
        return ref.at[block]
    depth = ref.shape[0] // groups
    return ref.at[pl.ds(pl.multiple_of(block * depth, 16), depth)]


def over_dp(src, dst, send, recv, peer):
    return pltpu.make_async_remote_copy(
        src_ref=src, dst_ref=dst, send_sem=send, recv_sem=recv, device_id={"dp": peer}, device_id_type=MESH
    )


class Spread:
    def __init__(self, groups, all_ref, send, recv):
        row = lax.axis_index("dp")
        twin = row + 1 - 2 * lax.rem(row, 2)
        half = groups // 2
        chip = lax.div(row, 2)
        self.relayed = half == 4
        self.out, self.back = [], []
        for k in range(half):
            came = block_of(all_ref, lax.rem(row + groups - 2 * k, groups), groups)
            self.back.append(over_dp(came, came, send.at[half + k], recv.at[half + k], twin))
            if k > 0:
                mine = block_of(all_ref, row, groups)
                self.out.append(over_dp(mine, mine, send.at[k], recv.at[k], lax.rem(row + 2 * k, groups)))
        self.asked = {}
        if self.relayed:
            self.asked = {0: chip != 3, 2: chip != 0}
            self.inner = (chip == 1) | (chip == 2)
            up = lax.div(chip, 2)
            came = block_of(all_ref, lax.rem(row + 4, groups), groups)
            self.relay = over_dp(came, came, send.at[0], recv.at[1 + 2 * up], row + 4 * up - 2)

    def where(self, k, act):
        if k in self.asked:
            pl.when(self.asked[k])(act)
        else:
            act()

    def start(self):
        for k in (1, 0, 2) if self.relayed else range(len(self.out)):
            self.where(k, self.out[k].start)
        self.back[0].start()

    def hop(self):
        if self.relayed:
            self.out[1].wait_recv()
            pl.when(self.inner)(self.relay.start)
            self.back[2].start()

    def forward(self):
        for k, (far, near) in enumerate(zip(self.out, self.back[1:])):
            if k != 1 or not self.relayed:
                far.wait_recv()
                near.start()

    def arrive(self):
        for made in self.back:
            made.wait_recv()

    def finish(self):
        for k, made in enumerate(self.out):
            self.where(k, made.wait_send)
        for made in self.back:
            made.wait_send()
        if self.relayed:
            pl.when(self.inner)(self.relay.wait_send)


class Moves:
    def __init__(self, sem):
        self.sem, self.made = sem, []

    def plan(self, src, dst):
        made = pltpu.make_async_copy(src, dst, self.sem.at[len(self.made)])
        self.made.append(made)
        return made

    def start(self, src, dst):
        made = self.plan(src, dst)
        made.start()
        return made

    def finish(self):
        for made in self.made:
            made.wait()


class Reduce:
    def __init__(self, groups, grad_ref, twin_ref, far_ref, tsend, trecv, fsend, frecv):
        self.grad_ref = grad_ref
        depth = grad_ref.shape[0] // groups
        if far_ref is None:
            near, first = twin_ref, depth * (groups // 2)
            self.twin = lambda slot: near.at[pl.ds(pl.multiple_of(slot * depth, 16), depth)]
            self.far = [near.at[pl.ds(first + k * depth, depth)] for k in range(groups // 2 - 1)]
        else:
            self.twin = lambda slot: twin_ref.at[slot]
            self.far = [far_ref.at[k] for k in range(groups // 2 - 1)]
        rows = lambda block: pl.ds(pl.multiple_of(block * depth, 16), depth)
        row = lax.axis_index("dp")
        core = lax.rem(row, 2)
        self.kept, self.mine = self.twin(lax.div(row, 2)), rows(row)
        self.near, self.away = [], []
        for k in range(groups // 2):
            theirs = grad_ref.at[rows(2 * k + 1 - core)]
            self.near.append(over_dp(theirs, self.twin(k), tsend.at[k], trecv.at[k], row + 1 - 2 * core))
        for k in range(1, groups // 2):
            peer = lax.rem(row + 2 * k, groups)
            slot = lax.div(peer, 2)
            held = self.twin(slot)
            made = over_dp(held, self.far[k - 1], fsend.at[k], frecv.at[k], peer)
            self.away.append((held, rows(peer), made))

    def start(self):
        for made in self.near:
            made.start()

    def pair(self):
        for made in self.near:
            made.wait_recv()
        for held, part, made in self.away:
            held[...] = (held[...].astype(F32) + self.grad_ref[part].astype(F32)).astype(BF16)
            made.start()

    def total(self):
        value = self.kept[...].astype(F32) + self.grad_ref[self.mine].astype(F32)
        for (_, _, made), came in zip(self.away, self.far):
            made.wait_recv()
            value = value + came[...].astype(F32)
        return value

    def finish(self):
        for made in self.near + [made for _, _, made in self.away]:
            made.wait_send()


def reduce_scratch(groups, depth, width):
    half, width = groups // 2, lanes(width)
    return [pltpu.VMEM((half, depth, width), BF16), pltpu.VMEM((half - 1, depth, width), BF16)] + sems(half) * 2


def outer(out_ref, left_ref, right_ref, width, first=0):
    images, blocks, full, model = left_ref.shape
    count = images * blocks * full
    tile = 384

    def part(c, _):
        at = pl.ds(pl.multiple_of(c * tile, tile), tile)
        left = left_ref[:, :, :, at].reshape(count, tile)
        right = right_ref[:, :, :, :width].reshape(count, width)
        out_ref[at, first : first + width] = dot(left, right, TN).astype(BF16)
        return 0

    lax.fori_loop(0, model // tile, part, 0)


def whole_body(
    groups, rows, heads,
    x_ref, grad_ref, mask_ref, gain_one, bias_one, bias_out, gain_two, bias_two, bias_down, qv_ref, hb_ref,
    wq_ref, wo_ref, wh_ref, wd_ref,
    one_out, block_out, gin_out, gwq_ref, gwo_ref, gwh_ref, gwd_ref, both_ref,
    one_ref, full_ref, two_ref, hidden_ref, qh, kh, vh, mixed_ref, wq_all, wo_all, wh_all, wd_all,
    gq, part_ref, ghid_ref, act_ref, gpl_ref, gwh_part, gwd_part, slots, osem,
    dtwin, daway, dtsend, dtrecv, dfsend, dfrecv,
    htwin, haway, htsend, htrecv, hfsend, hfrecv,
    qtsend, qtrecv, qfsend, qfrecv,
    gsend, grecv, wsend, wrecv,
    hsum, bsum, mid, row_in, flat_in, vsend, vrecv,
):
    images = x_ref.shape[0]
    _, _, full, model = one_ref.shape
    units = hb_ref.shape[0]
    seq = 4 * full
    width = heads * HD
    last = images - 1
    me, side, over, _ = plane()
    mine = lax.axis_index("dp")
    wq_all[mine, :, 3 * width :] = jnp.zeros_like(wq_all[mine, :, 3 * width :])
    for c in range(3):
        wq_all[mine, :, c * width : (c + 1) * width] = wq_ref[c]
    weights = [Spread(groups, wq_all, wsend.at[0], wrecv.at[0])]
    for k, (own, everyone) in enumerate(((wo_ref, wo_all), (wh_ref, wh_all), (wd_ref, wd_all))):
        count = own.shape[1]
        place = block_of(everyone, mine, groups)
        place[:, count:] = jnp.zeros((own.shape[0], everyone.shape[-1] - count), BF16)
        place[:, :count] = own[...]
        weights.append(Spread(groups, everyone, wsend.at[k + 1], wrecv.at[k + 1]))
    wq, wo, wh, wd = weights
    ones, sums, twos, grads, turns, lows, outs, backs = [], [], [], [], [], [], [], []
    for i in range(images):
        for ref in (one_ref, two_ref, full_ref):
            clear_pads(ref.at[i], rows)
        pair = lambda k: (gsend.at[k, i], grecv.at[k, i])
        four = [slots.at[i, k] for k in range(4)]
        spare = [act_ref.at[i, k] for k in range(4)]
        ones.append(Gather(one_ref.at[i], rows, *pair(0)))
        grads.append(Gather(full_ref.at[i], rows, *pair(1)))
        sums.append(Scatter(part_ref.at[i], rows, four, *pair(2)))
        twos.append(Gather(two_ref.at[i], rows, *pair(3)))
        turns.append(Scatter(part_ref.at[i], rows, four, *pair(4)))
        lows.append(Gather(one_ref.at[i], rows, *pair(5)))
        outs.append(Scatter(two_ref.at[i], rows, spare, *pair(6)))
        backs.append(Scatter(part_ref.at[i], rows, four, *pair(7)))
    down = Reduce(groups, gwd_part, dtwin, daway, dtsend, dtrecv, dfsend, dfrecv)
    red_h = Reduce(groups, gwh_part, htwin, haway, htsend, htrecv, hfsend, hfrecv)
    red_q = Reduce(groups, gwd_part, wd_all, None, qtsend, qtrecv, qfsend, qfrecv)
    moves = Moves(osem)
    keep_one = [moves.plan(one_ref.at[i], one_out.at[i]) for i in range(images)]
    take_one = [moves.plan(one_out.at[i], full_ref.at[i]) for i in range(images)]
    take_grad = [moves.plan(grad_ref.at[i], full_ref.at[i, me, pl.ds(0, rows)]) for i in range(images)]
    put_out = [moves.plan(two_ref.at[i, me, pl.ds(0, rows)], block_out.at[i]) for i in range(images)]
    put_gin = [moves.plan(ghid_ref.at[i], gin_out.at[i]) for i in range(images)]

    def enter(i):
        one_ref[i, me, :rows] = norm_forward(x_ref[i].astype(F32), at_row(gain_one), at_row(bias_one))

    for made in take_grad:
        made.start()
    greet_all(groups, lambda: enter(0))
    ones[0].start()
    wq.start()
    for i in range(1, images):
        enter(i)
        ones[i].start()
    for step in (wo, wh, wd):
        step.start()
    hsum[...] = jnp.zeros_like(hsum)
    bsum[...] = jnp.zeros_like(bsum)
    mixed_ref[:, :, :, width:] = jnp.zeros_like(mixed_ref[:, :, :, width:])
    for i in range(images):
        bias, tail = key_bias(mask_ref[i : i + 1], rows, full, seq)
        for h in range(heads):
            kh[i, h, :, HD:] = bias
            vh[i, h, :, HD:] = jnp.zeros_like(bias)
            qh[i, h, :, HD:] = tail
    for step in ones:
        step.forward()
    for made in take_grad:
        made.wait()
    for step in grads:
        step.start()
    wq.hop()
    wq.forward()
    scale = HD**-0.5
    shift_q, shift_v = qv_ref[0:1], qv_ref[1:2]

    def project(i):
        weight = wq_all[:, :, : 3 * width].reshape(-1, 3 * width)

        def block(b, _):
            at = pl.ds(pl.multiple_of(b * full, 16), full)
            value = dot(one_ref[i, b], weight)
            queries = (value[:, :width] + shift_q).astype(BF16)
            keys_in = value[:, width : 2 * width].astype(BF16)
            values = (value[:, 2 * width :] + shift_v).astype(BF16)
            for h in range(heads):
                here = slice(h * HD, (h + 1) * HD)
                qh[i, h, at, :HD] = queries[:, here]
                kh[i, h, at, :HD] = keys_in[:, here]
                vh[i, h, at, :HD] = values[:, here]
            return 0

        lax.fori_loop(0, 4, block, 0)

    def attend(i):
        def head(h, _):
            probs = soft_open(kh[i, h], qh[i, h], scale * LOG2E)
            gq[h] = dot(vh[i, h, :, :HD].T, probs.astype(BF16)).T.astype(BF16)
            return 0

        lax.fori_loop(0, heads, head, 0, unroll=2)
        for h in range(heads):
            for b in range(4):
                mixed_ref[i, b, :, h * HD : (h + 1) * HD] = gq[h, b * full : (b + 1) * full]

    def combine(i):
        weight = wo_all[:, :, :width].reshape(-1, width)

        def block(b, _):
            part_ref[i, b] = dot(mixed_ref[i, b, :, :width], weight, NT).astype(BF16)
            return 0

        lax.fori_loop(0, 4, block, 0)

    def ready(k):
        ones[k].arrive()
        keep_one[k].start()
        if k == 0:
            wq.arrive()

    def between(k):
        if k == 0:
            wo.hop()
            wo.forward()
            wh.hop()
            wo.arrive()

    def send(k):
        if k > 0:
            sums[k - 1].forward()
        sums[k].start()
        grads[k].forward()

    def image(i, _):
        for_image(i, images, ready)
        project(i)
        attend(i)
        for_image(i, images, between)
        combine(i)
        for_image(i, images, send)
        return 0

    lax.fori_loop(0, images, image, 0)

    def settle(i):
        sums[i].arrive()
        hidden = x_ref[i].astype(F32) + sums[i].total(pl.ds(0, rows)) + at_row(bias_out)
        hidden_ref[i] = hidden
        two_ref[i, me, :rows] = norm_forward(hidden, at_row(gain_two), at_row(bias_two))
        twos[i].start()

    for i in range(last):
        settle(i)
    sums[-1].forward()
    wd.hop()
    for i in range(last):
        twos[i].forward()
    settle(last)
    twos[-1].forward()
    wh.forward()
    wd.forward()
    for step in sums + ones:
        step.finish()
    for made in keep_one:
        made.wait()
    wide = lambda ref: ref[:, :units]
    shift = at_row(hb_ref)

    def ascend(i):
        def pair(c, _):
            at = pl.ds(2 * c, 2)
            pre = dot(two_ref[i, at].reshape(2 * full, model), wide(wh_all)) + shift
            value, slope = gelu_both(pre)
            act_ref[i, at, :, :units] = value.astype(BF16).reshape(2, full, units)
            grad_pre = dot(full_ref[i, at].reshape(2 * full, model), wide(wd_all)) * slope
            hsum[...] += jnp.sum(grad_pre, axis=0, keepdims=True)
            low = grad_pre.astype(BF16)
            gpl_ref[i, at, :, :units] = low.reshape(2, full, units)
            part_ref[i, at] = dot(low, wide(wh_all), NT).astype(BF16).reshape(2, full, model)
            return 0

        lax.fori_loop(0, 2, pair, 0)

    def descend(k, _):
        at = pl.ds(2 * lax.rem(k, 2), 2)
        i = lax.div(k, 2)
        part = dot(act_ref[i, at, :, :units].reshape(2 * full, units), wide(wd_all), NT)
        two_ref[i, at] = part.astype(BF16).reshape(2, full, model)
        return 0

    totals = [0.0] * 6

    def add_up(first, terms):
        for k, term in enumerate(terms):
            totals[first + k] = totals[first + k] + jnp.sum(term, axis=0, keepdims=True)

    def settle_back(i):
        turns[i].arrive()
        grad_normed = turns[i].total(pl.ds(0, rows))
        unit, inv_std = norm_stats(hidden_ref[i])
        upper = full_ref[i, me, :rows].astype(F32)
        grad_hidden = upper + norm_backward(grad_normed, unit, inv_std, at_row(gain_two))
        ghid_ref[i] = grad_hidden
        one_ref[i, me, :rows] = grad_hidden.astype(BF16)
        lows[i].start()
        add_up(0, (grad_normed * unit, grad_normed, grad_hidden, upper))

    def ready_back(k):
        twos[k].arrive()
        if k == 0:
            wh.arrive()
            wd.arrive()
        grads[k].arrive()

    def send_back(k):
        if k > 0:
            turns[k - 1].forward()
        turns[k].start()

    def image_back(i, _):
        for_image(i, images, ready_back)
        ascend(i)
        for_image(i, images, send_back)
        return 0

    lax.fori_loop(0, images, image_back, 0)
    for step in weights:
        step.finish()
    gwd_part[:, units:] = jnp.zeros((model, lanes(units) - units), BF16)
    outer(gwd_part, full_ref, act_ref, units)
    down.start()
    for i in range(last):
        settle_back(i)
    turns[-1].forward()
    down.pair()
    gwh_part[:, units:] = jnp.zeros((model, lanes(units) - units), BF16)
    outer(gwh_part, two_ref, gpl_ref, units)
    for i in range(last):
        lows[i].forward()
    for step in twos:
        step.finish()
    lax.fori_loop(0, 2 * images, descend, 0)
    red_h.start()
    settle_back(last)
    red_h.pair()
    for step in turns + grads:
        step.finish()
    for made in take_one:
        made.start()

    def mix(i):
        value = dot(one_ref[i].reshape(seq, model), wo_all[:, :, :width].reshape(model, width)).astype(BF16)
        gpl_ref[i, :, :, 3 * width : 4 * width] = value.reshape(4, full, width)

    def midway(k):
        if k < last:
            lows[k + 1].forward()
        if k > 0:
            backs[k - 1].forward()

    def attend_back(i):
        for h in range(heads):
            if h == heads // 2:
                for_image(i, images, midway)
            here = slice(3 * width + h * HD, 3 * width + (h + 1) * HD)
            queries = qh[i, h]
            grads_in = gpl_ref[i, :, :, here].reshape(seq, HD)
            keys_in = kh[i, h]
            probs = soft_open(keys_in, queries, scale * LOG2E)
            grad_probs = dot(vh[i, h, :, :HD], grads_in, NT)
            grad_values = dot(probs.astype(BF16), grads_in)
            delta = jnp.sum(probs * grad_probs, axis=0, keepdims=True)
            grad_scores = (probs * (grad_probs - delta) * scale).astype(BF16)
            grad_keys = dot(grad_scores, queries[:, :HD])
            grad_queries = dot(keys_in[:, :HD].T, grad_scores).T
            for c, value in enumerate((grad_queries, grad_keys, grad_values)):
                here = slice(c * width + h * HD, c * width + (h + 1) * HD)
                gpl_ref[i, :, :, here] = value.astype(BF16).reshape(4, full, HD)
                bsum[h, c : c + 1] += jnp.sum(value, axis=0, keepdims=True)

    def spread(i):
        def pair(c, _):
            at = pl.ds(2 * c, 2)
            left = gpl_ref[i, at, :, : 3 * width].reshape(2 * full, 3 * width)
            part = dot(left, wq_all[:, :, : 3 * width].reshape(model, 3 * width), NT)
            part_ref[i, at] = part.astype(BF16).reshape(2, full, model)
            return 0

        lax.fori_loop(0, 2, pair, 0)

    def ready_last(k):
        lows[k].arrive(4 if k > 0 else 2)

    def send_last(k):
        backs[k].start()
        if k < last:
            lows[k + 1].arrive(2, 4)
            outs[k].start()
        else:
            outs[k].start()
            outs[k - 1].forward()

    def image_last(i, _):
        for_image(i, images, ready_last)
        mix(i)
        attend_back(i)
        spread(i)
        for_image(i, images, send_last)
        return 0

    lax.fori_loop(0, images, image_last, 0)
    gwd_ref[...] = down.total()[:, :units]
    down.finish()
    outer(gwd_part, one_ref, mixed_ref, width, 3 * width)
    for made in take_one:
        made.wait()
    outer(gwd_part, full_ref, gpl_ref, 3 * width)
    red_q.start()

    def settle_last(i):
        backs[i].arrive()
        grad_normed = backs[i].total(pl.ds(0, rows))
        unit, inv_std = norm_stats(x_ref[i].astype(F32))
        ghid_ref[i] = ghid_ref[i] + norm_backward(grad_normed, unit, inv_std, at_row(gain_one))
        put_gin[i].start()
        add_up(4, (grad_normed * unit, grad_normed))

    def finish_out(i):
        outs[i].arrive()
        value = hidden_ref[i] + outs[i].total(pl.ds(0, rows)) + at_row(bias_down)
        two_ref[i, me, :rows] = value.astype(BF16)
        put_out[i].start()

    for i in range(last):
        settle_last(i)
    backs[-1].forward()
    gwh_ref[...] = red_h.total()[:, :units]
    red_q.pair()
    mid[0] = jnp.zeros_like(mid[0])
    for h in range(heads):
        for c in range(3):
            mid[0, 6:7, c * width + h * HD : c * width + (h + 1) * HD] = bsum[h, c : c + 1]
    mid[0, 7:8, :units] = hsum[...]
    settle_last(last)

    for k in range(6):
        mid[0, k : k + 1] = totals[k]
    row_in[mine] = mid[0]
    aways = []
    for k in range(1, groups):
        aways.append(over_dp(mid.at[0], row_in.at[mine], vsend.at[k], vrecv.at[k], lax.rem(mine + k, groups)))
        aways[-1].start()
    outs[-1].forward()
    for made in aways:
        made.wait()
    held = row_in[0]
    for k in range(1, groups):
        held = held + row_in[k]
    mid[1] = held
    flat_in[me] = mid[1]
    planes = []
    for k in range(1, 4):
        at = groups + k
        planes.append(remote(mid.at[1], flat_in.at[me], vsend.at[at], vrecv.at[at], lax.rem(me + k, 4)))
        planes[-1].start()
    for i in range(last):
        finish_out(i)
    for made in planes:
        made.wait()
    both_ref[0:6] = (flat_in[0] + flat_in[1] + flat_in[2] + flat_in[3])[0:6]
    both_ref[6:8] = mid[1, 6:8]
    finish_out(last)
    total = red_q.total()
    for c in range(3):
        gwq_ref[c] = total[:, c * width : (c + 1) * width]
    gwo_ref[...] = total[:, 3 * width : 4 * width]
    for step in lows + outs + backs + [red_h, red_q]:
        step.finish()
    for made in put_out + put_gin:
        made.wait()


def whole(groups, block_input, grad_out, key_mask, vectors, qv_bias, bias, wq, wo, wh, wd):
    images, rows, model = block_input.shape
    full = pad_rows(rows)
    width = wo.shape[1]
    units = wh.shape[1]
    heads = width // HD
    seq = 4 * full
    depth = wo.shape[0]
    blocks = ((images, 4, full, model), BF16)
    own = ((images, rows, model), F32)
    heads_wide = ((images, heads, seq, 128), BF16)
    piece = ((heads, seq, HD), BF16)
    square = ((model, lanes(units)), BF16)
    weight = lambda count: ((groups, depth, lanes(count)), BF16)
    outs = [blocks, (block_input.shape, BF16), own]
    more = [((3, depth, width), F32), ((depth, width), F32), ((depth, units), F32), ((depth, units), F32), ((8, model), F32)]
    held = [blocks, blocks, blocks, own, heads_wide, heads_wide, heads_wide, ((images, 4, full, lanes(width)), BF16)]
    held += [weight(3 * width), weight(width), square, square]
    held += [piece, blocks, own, blocks, blocks, square, square, blocks]
    return pl.pallas_call(
        functools.partial(whole_body, groups, rows, heads),
        out_shape=tuple(jax.ShapeDtypeStruct(*h) for h in outs + more),
        in_specs=[VMEM, ANY] + [VMEM] * 13,
        out_specs=(ANY,) * len(outs) + (VMEM,) * len(more),
        scratch_shapes=[pltpu.VMEM(*h) for h in held]
        + [pltpu.SemaphoreType.DMA((5 * images,))]
        + reduce_scratch(groups, depth, units) * 2
        + sems(groups // 2) * 2
        + sems(8, images, STEPS)
        + sems(4, groups)
        + [
            pltpu.VMEM((1, units), F32),
            pltpu.VMEM((heads, 3, HD), F32),
            pltpu.VMEM((2, 8, model), F32),
            pltpu.VMEM((groups, 8, model), F32),
            pltpu.VMEM((4, 8, model), F32),
        ]
        + sems(groups + 4),
        compiler_params=params(0),
        name="whole",
    )(block_input, grad_out, key_mask, *vectors, qv_bias, bias, wq, wo, wh, wd)


def deliver_body(width, out, gin, gwq, gwo, gwh, gwd, both, *refs):
    refs, held, lsem, ssem = refs[:14], refs[14:20], refs[20], refs[21]
    loads, stores = Moves(lsem), Moves(ssem)
    sources = (out, gin, gwq, gwo, gwh, gwd)
    got = [loads.start(src, mid) for src, mid in zip(sources, held)]
    qv, unit = refs[6:8]
    qv[0:1] = both[6:7, :width]
    qv[1:2] = both[6:7, 2 * width : 3 * width]
    unit[...] = both[7, : unit.shape[0]]
    for k, dst in enumerate(refs[8:]):
        dst[...] = both[k]
    for made, mid, dst in zip(got, held, refs):
        made.wait()
        stores.start(mid, dst)
    stores.finish()


def deliver(width, units, out, gin, gwq, gwo, gwh, gwd, both):
    model = both.shape[1]
    same = [jax.ShapeDtypeStruct(v.shape, v.dtype) for v in (out, gin, gwq, gwo, gwh, gwd)]
    more = [jax.ShapeDtypeStruct(dims, F32) for dims in ((2, width), (units,)) + ((model,),) * 6]
    return pl.pallas_call(
        functools.partial(deliver_body, width),
        out_shape=tuple(same + more),
        in_specs=[ANY] * 6 + [VMEM],
        out_specs=(ANY,) * 6 + (VMEM,) * 8,
        scratch_shapes=[pltpu.VMEM(v.shape, v.dtype) for v in same]
        + [pltpu.SemaphoreType.DMA((6,)), pltpu.SemaphoreType.DMA((6,))],
        compiler_params=pltpu.CompilerParams(vmem_limit_bytes=60 << 20),
        name="deliver",
    )(out, gin, gwq, gwo, gwh, gwd, both)


def gather_rows(rows):
    return lax.all_gather(rows, "tensor", axis=1, tiled=True)


def scatter_rows(part):
    return lax.psum_scatter(part, "tensor", scatter_dimension=1, tiled=True).astype(F32)


def shards(
    groups,
    ranks,
    block_input,
    key_mask,
    attn_norm_gain,
    attn_norm_bias,
    qkv_weight,
    qv_bias,
    out_weight,
    out_bias,
    mlp_norm_gain,
    mlp_norm_bias,
    hidden_weight,
    hidden_bias,
    down_weight,
    down_bias,
    grad_out,
):
    images, rows, model = block_input.shape
    flat = ranks == 4 and images == 2 and groups > 2 and groups % 2 == 0 and hidden_weight.shape[1] <= model and 4 * qkv_weight.shape[2] == lanes(hidden_weight.shape[1])
    seq = key_mask.shape[1]
    width = qkv_weight.shape[2]
    units = hidden_weight.shape[1]

    def weight(shard):
        return lax.all_gather(shard, "dp", axis=0, tiled=True)

    def owned(grad):
        return lax.psum_scatter(grad.astype(BF16), "dp", scatter_dimension=0, tiled=True).astype(F32)

    out_rows, down_rows = out_weight.T, down_weight.T
    if flat:
        _, block_output, grad_input, grad_qkv_w, grad_out_w, grad_hidden_w, grad_down_w, both = whole(
            groups,
            block_input,
            grad_out,
            key_mask,
            (attn_norm_gain, attn_norm_bias, out_bias, mlp_norm_gain, mlp_norm_bias, down_bias),
            qv_bias,
            hidden_bias,
            qkv_weight.transpose(1, 0, 2),
            out_rows,
            hidden_weight,
            down_rows,
        )
        (
            block_output, grad_input, grad_qkv_w, grad_out_w, grad_hidden_w, grad_down_w, grad_qv, grad_hidden_b, *both
        ) = deliver(
            width, units, block_output, grad_input, grad_qkv_w, grad_out_w, grad_hidden_w, grad_down_w, both
        )
        grad_qkv_w = grad_qkv_w.transpose(1, 0, 2)
        grad_out_w, grad_down_w = grad_out_w.T, grad_down_w.T
    else:
        qkv_rows = qkv_weight.reshape(-1, 3 * width)
        shift = jnp.concatenate([qv_bias[0], jnp.zeros_like(qv_bias[0]), qv_bias[1]])
        hidden_all, down_all = weight(hidden_weight), weight(down_rows)
        qkv_all, out_all = weight(qkv_rows), weight(out_rows)
        lens = jnp.sum(key_mask, axis=1)
        in_float = block_input.astype(F32)
        normed_one = gather_rows(norm_forward(in_float, attn_norm_gain, attn_norm_bias))
        grad_full = gather_rows(grad_out)
        proj = jnp.einsum("isd,df->isf", normed_one, qkv_all, preferred_element_type=F32) + shift
        proj = proj.astype(BF16)
        mixed = attend_forward(lens, proj)
        attn_part = jnp.einsum("isf,df->isd", mixed, out_all, preferred_element_type=F32).astype(BF16)
        hidden_res = in_float + scatter_rows(attn_part) + out_bias
        normed_two = gather_rows(norm_forward(hidden_res, mlp_norm_gain, mlp_norm_bias))
        pre_act = jnp.einsum("isd,df->isf", normed_two, hidden_all, preferred_element_type=F32) + hidden_bias
        value, slope = gelu_both(pre_act)
        activated = value.astype(BF16)
        grad_act = jnp.einsum("isd,df->isf", grad_full, down_all, preferred_element_type=F32)
        grad_pre = grad_act * slope
        grad_hidden_b = jnp.sum(grad_pre, axis=(0, 1))
        grad_pre_low = grad_pre.astype(BF16)
        gpart = jnp.einsum("isf,df->isd", grad_pre_low, hidden_all, preferred_element_type=F32).astype(BF16)
        mpart = jnp.einsum("isf,df->isd", activated, down_all, preferred_element_type=F32).astype(BF16)
        block_output = (hidden_res + scatter_rows(mpart) + down_bias).astype(BF16)
        grad_float = grad_out.astype(F32)
        grad_normed = scatter_rows(gpart)
        unit, inv_std = norm_stats(hidden_res)
        grad_hidden = grad_float + norm_backward(grad_normed, unit, inv_std, mlp_norm_gain)
        hidden_full = gather_rows(grad_hidden.astype(BF16))
        mlp_sums = jnp.stack(
            [jnp.sum(v, axis=(0, 1)) for v in (grad_normed * unit, grad_normed, grad_hidden, grad_float)]
        )
        grad_hidden_w = owned(jnp.einsum("isd,isf->df", normed_two, grad_pre_low, preferred_element_type=F32))
        grad_down_w = owned(jnp.einsum("isd,isf->df", grad_full, activated, preferred_element_type=F32)).T
        grad_mixed = jnp.einsum("isd,df->isf", hidden_full, out_all, preferred_element_type=F32).astype(BF16)
        grad_proj, proj_sums = attend_backward(lens, proj, grad_mixed)
        proj_sums = jnp.sum(proj_sums, axis=(0, 1))
        npart = jnp.einsum("isf,df->isd", grad_proj, qkv_all, preferred_element_type=F32).astype(BF16)
        grad_out_w = owned(jnp.einsum("isd,isf->df", hidden_full, mixed, preferred_element_type=F32)).T
        grad_qkv_w = owned(jnp.einsum("isd,isf->df", normed_one, grad_proj, preferred_element_type=F32))
        grad_normed = scatter_rows(npart)
        unit, inv_std = norm_stats(in_float)
        grad_input = grad_hidden + norm_backward(grad_normed, unit, inv_std, attn_norm_gain)
        attn_sums = jnp.stack([jnp.sum(v, axis=(0, 1)) for v in (grad_normed * unit, grad_normed)])
        both = lax.psum(jnp.concatenate([mlp_sums, attn_sums]), ("dp", "tensor"))
        proj_sums, grad_hidden_b = lax.psum((proj_sums, grad_hidden_b), "dp")
        grad_qv = jnp.stack([proj_sums[:width], proj_sums[2 * width :]])
        grad_qkv_w = grad_qkv_w.reshape(-1, 3, width)
    return (
        block_output,
        grad_input,
        both[4],
        both[5],
        grad_qkv_w,
        grad_qv,
        grad_out_w,
        both[2],
        both[0],
        both[1],
        grad_hidden_w,
        grad_hidden_b,
        grad_down_w,
        both[3],
    )


def solution(mesh):
    return jax.shard_map(
        functools.partial(shards, mesh.shape["dp"], mesh.shape["tensor"]),
        mesh=mesh,
        in_specs=(
            P("dp", "tensor", None),
            P("dp", None),
            P(),
            P(),
            P("dp", None, "tensor"),
            P(None, "tensor"),
            P("tensor", "dp"),
            P(),
            P(),
            P(),
            P("dp", "tensor"),
            P("tensor"),
            P("tensor", "dp"),
            P(),
            P("dp", "tensor", None),
        ),
        out_specs=(
            P("dp", "tensor", None),
            P("dp", "tensor", None),
            P(),
            P(),
            P("dp", None, "tensor"),
            P(None, "tensor"),
            P("tensor", "dp"),
            P(),
            P(),
            P(),
            P("dp", "tensor"),
            P("tensor"),
            P("tensor", "dp"),
            P(),
        ),
        check_vma=False,
    )
```
